8 devices in a mesh: batch: 1 (over z), col: 2 (over y), row: 4 (over x, core).
Axes of the slice: x: 2, y: 2, z: 1, core: 2. Of those that a mesh axis runs over, the one named last changes fastest.
Arguments:
- a_matrix: float32 [16384, 64, 64], P(('batch', 'row'), 'col')
- b_matrix: float32 [16384, 64, 64], P(('batch', 'row'), 'col')
Outputs:
- output 1: float32 [16384, 64, 64], P(('batch', 'row'), 'col')
- output 2: float32 [256], P('batch')
- output 3: float32 [4, 64, 64], P('batch')
- output 4: float32 [16384, 64, 64], P(('batch', 'row'), 'col')
- output 5: float32 [256], P('batch')
- output 6: float32 [4, 64, 64], P('batch')
All inputs are finite; a program needn't handle non-finite values.
Results may differ from the reference program's by a relative error of at most 0.001.
Values sent between devices are 32-bit elements.
A program may use at most 1 GiB of HBM per device.

```python
import jax
import jax.numpy as jnp
from jax import lax

MATRIX_ROWS = 16384
MATRIX_COLS = 4096
PANEL_WIDTH = 64
PANELS = 4
COL_PROCS = 2
FACTOR_COLS = PANELS * PANEL_WIDTH
LOCAL_BLOCKS = MATRIX_COLS // (COL_PROCS * PANEL_WIDTH)
PRECISE = lax.Precision.HIGHEST


def to_storage(dense_mat):
    row_count = dense_mat.shape[0]
    blocks = dense_mat.reshape(row_count, LOCAL_BLOCKS, COL_PROCS, PANEL_WIDTH)
    return blocks.transpose(0, 2, 1, 3).reshape(row_count, COL_PROCS * LOCAL_BLOCKS, PANEL_WIDTH)


def to_global(stored):
    row_count = stored.shape[0]
    blocks = stored.reshape(row_count, COL_PROCS, LOCAL_BLOCKS, PANEL_WIDTH)
    return blocks.transpose(0, 2, 1, 3).reshape(row_count, MATRIX_COLS)


def draw_matrix(key_mat):
    key_noise, key_left, key_right, key_sign = jax.random.split(key_mat, 4)
    noise_mat = jax.random.normal(key_noise, (MATRIX_ROWS, MATRIX_COLS), jnp.float32)
    left_vec = jax.random.normal(key_left, (MATRIX_ROWS,), jnp.float32)
    right_vec = jax.random.normal(key_right, (MATRIX_COLS,), jnp.float32)
    pivot_sign = (2 * jax.random.randint(key_sign, (FACTOR_COLS,), 0, 2) - 1).astype(jnp.float32)
    diag_ids = jnp.arange(FACTOR_COLS)
    dense_mat = noise_mat + 0.5 * left_vec[:, None] * right_vec[None, :]
    dense_mat = dense_mat.at[diag_ids, diag_ids].add(pivot_sign * (MATRIX_ROWS ** 0.5))
    return to_storage(dense_mat)


def setup_inputs(seed: int = 0, part: int = 0) -> dict:
    part_key = jax.random.fold_in(jax.random.key(seed), part)
    key_first, key_second = jax.random.split(part_key)
    return {"a_matrix": draw_matrix(key_first), "b_matrix": draw_matrix(key_second)}


def factor_panel(panel_in, row_start):
    row_ids = jnp.arange(panel_in.shape[0])
    col_ids = jnp.arange(PANEL_WIDTH)

    def column_step(col_idx, loop_state):
        panel_work, tau_vec = loop_state
        diag_idx = row_start + col_idx
        column = lax.dynamic_slice_in_dim(panel_work, col_idx, 1, axis=1)[:, 0]
        below_diag = jnp.where(row_ids >= diag_idx, column, 0.0)
        pivot_val = lax.dynamic_slice_in_dim(column, diag_idx, 1)[0]
        col_norm = jnp.sqrt(jnp.sum(below_diag * below_diag))
        house_beta = -jnp.where(pivot_val >= 0, 1.0, -1.0) * col_norm
        house_tau = (house_beta - pivot_val) / house_beta
        at_diag = (row_ids == diag_idx).astype(jnp.float32)
        refl_vec = jnp.where(row_ids > diag_idx, column / (pivot_val - house_beta), 0.0) + at_diag
        proj_row = jnp.dot(refl_vec, panel_work, precision=PRECISE)
        proj_row = jnp.where(col_ids > col_idx, proj_row, 0.0)
        panel_work = panel_work - house_tau * refl_vec[:, None] * proj_row[None, :]
        new_col = jnp.where(row_ids < diag_idx, column, jnp.where(row_ids == diag_idx, house_beta, refl_vec))
        panel_work = lax.dynamic_update_slice_in_dim(panel_work, new_col[:, None], col_idx, axis=1)
        tau_vec = lax.dynamic_update_slice_in_dim(tau_vec, house_tau[None], col_idx, axis=0)
        return panel_work, tau_vec

    return lax.fori_loop(0, PANEL_WIDTH, column_step, (panel_in, jnp.zeros((PANEL_WIDTH,), jnp.float32)))


def build_factor(gram_mat, tau_vec):
    col_ids = jnp.arange(PANEL_WIDTH)

    def t_step(col_idx, t_factor):
        gram_col = lax.dynamic_slice_in_dim(gram_mat, col_idx, 1, axis=1)[:, 0]
        gram_col = jnp.where(col_ids < col_idx, gram_col, 0.0)
        tau_k = lax.dynamic_slice_in_dim(tau_vec, col_idx, 1)[0]
        t_col = -tau_k * jnp.dot(t_factor, gram_col, precision=PRECISE)
        t_col = jnp.where(col_ids == col_idx, tau_k, t_col)
        return lax.dynamic_update_slice_in_dim(t_factor, t_col[:, None], col_idx, axis=1)

    return lax.fori_loop(0, PANEL_WIDTH, t_step, jnp.zeros((PANEL_WIDTH, PANEL_WIDTH), jnp.float32))


def factor_matrix(stored):
    dense_mat = to_global(stored)
    row_ids = jnp.arange(MATRIX_ROWS)[:, None]
    col_ids = jnp.arange(PANEL_WIDTH)[None, :]
    tau_parts = []
    t_factors = []
    for panel_idx in range(PANELS):
        row_start = panel_idx * PANEL_WIDTH
        col_stop = row_start + PANEL_WIDTH
        panel_work, tau_vec = factor_panel(dense_mat[:, row_start:col_stop], row_start)
        diag_ids = row_start + col_ids
        v_block = jnp.where(row_ids == diag_ids, 1.0, jnp.where(row_ids > diag_ids, panel_work, 0.0))
        t_factor = build_factor(jnp.dot(v_block.T, v_block, precision=PRECISE), tau_vec)
        trailing = dense_mat[:, col_stop:]
        w_block = jnp.dot(t_factor.T, jnp.dot(v_block.T, trailing, precision=PRECISE), precision=PRECISE)
        trailing = trailing - jnp.dot(v_block, w_block, precision=PRECISE)
        dense_mat = jnp.concatenate([dense_mat[:, :row_start], panel_work, trailing], axis=1)
        tau_parts.append(tau_vec)
        t_factors.append(t_factor)
    return to_storage(dense_mat), jnp.concatenate(tau_parts), jnp.stack(t_factors)


def reference(a_matrix, b_matrix):
    a_factored, a_tau, a_tfactor = factor_matrix(a_matrix)
    b_factored, b_tau, b_tfactor = factor_matrix(b_matrix)
    return (a_factored, a_tau, a_tfactor, b_factored, b_tau, b_tfactor)
```

```python
import functools

import jax
import jax.numpy as jnp
from jax import lax
from jax.experimental import pallas as pl
from jax.experimental.pallas import tpu as pltpu
from jax.sharding import PartitionSpec as P

F32 = jnp.float32
HI = lax.Precision.HIGHEST
PANELS = 4
PRECISE = lax.Precision.HIGHEST
W=64
NP=4
N=256
NN=(((1,),(0,)),((),()))
NT=(((1,),(1,)),((),()))
TN=(((0,),(0,)),((),()))
def hdot(a,b,dn=NN):
    return lax.dot_general(a,b,dn,precision=HI,preferred_element_type=F32)

def diag_factor(mats):
    lane8 = lax.broadcasted_iota(jnp.int32,(8,128),1)
    sub8 = lax.broadcasted_iota(jnp.int32,(8,128),0)
    r64 = lax.broadcasted_iota(jnp.int32,(W,W),0)
    c64 = lax.broadcasted_iota(jnp.int32,(W,W),1)
    eye = (r64==c64).astype(F32)
    st=[]
    for Hpp,Ypp in mats:
        HE=jnp.concatenate([Hpp,eye],1); YW=jnp.concatenate([Ypp,eye],1)
        st.append(dict(he=[HE[8*g:8*g+8] for g in range(8)], yw=[YW[8*g:8*g+8] for g in range(8)],
            l=[jnp.zeros((8,128),F32) for g in range(8)], u=[jnp.zeros((8,128),F32) for g in range(8)], tau=jnp.zeros((8,128),F32)))
    for k in range(W):
        gk,sk=divmod(k,8)
        for s in st:
            ch=[jnp.broadcast_to(s['he'][g][:,k:k+1],(8,128)) if g>=gk else None for g in range(8)]
            cy=[jnp.broadcast_to(s['yw'][g][:,k:k+1],(8,128)) for g in range(8)]
            h=jnp.broadcast_to(ch[gk][sk:sk+1,:],(8,128)); a=jnp.broadcast_to(cy[gk][sk:sk+1,:],(8,128))
            rs=lax.rsqrt(h)
            rinv=jnp.where(a>=0,-rs,rs)
            beta=h*rinv
            ukk=a-beta
            uinv=1.0/ukk
            r=jnp.broadcast_to(s['he'][gk][sk:sk+1,:],(8,128))*rinv
            y=jnp.broadcast_to(s['yw'][gk][sk:sk+1,:],(8,128))
            u=y-jnp.where((lane8>=k)&(lane8<W),r,0.0)
            un=u*uinv
            rr=r*rinv
            isk=sub8==sk
            for g in range(gk,8):
                new=s['he'][g]-ch[g]*rr
                lc=cy[g]*uinv
                if g==gk:
                    new=jnp.where(sub8>sk,new,jnp.where(isk,r,s['he'][g]))
                    lc=jnp.where(sub8>sk,lc,0.0)
                s['he'][g]=new
                s['l'][g]=jnp.where(lane8==k,lc,s['l'][g])
            for g in range(8):
                new=s['yw'][g]-cy[g]*un
                if g==gk:
                    new=jnp.where(isk,un,new)
                s['yw'][g]=new
            s['u'][gk]=jnp.where(isk,u,s['u'][gk])
            s['tau']=jnp.where(lane8==k,-ukk*rinv,s['tau'])
    out=[]
    up=c64>=r64
    for s in st:
        HE=jnp.concatenate(s['he'],0); YW=jnp.concatenate(s['yw'],0); L=jnp.concatenate(s['l'],0)[:,:W]; U=jnp.concatenate(s['u'],0)[:,:W]
        out.append((jnp.where(up,HE[:,:W],0.0), jnp.where(c64<=r64,HE[:,W:],0.0), L+eye, jnp.where(up,U,0.0), YW[:,W:], s['tau'][0:1,:W]))
    return out

def chain_kernel(nm, *refs):
    g_refs=refs[0:nm]; xt_refs=refs[nm:2*nm]
    outs=refs[2*nm:2*nm+7*nm]
    HFs=refs[9*nm:10*nm]; YFs=refs[10*nm:11*nm]; Ls=refs[11*nm:12*nm]
    ri=lax.broadcasted_iota(jnp.int32,(N,N),0); ci=lax.broadcasted_iota(jnp.int32,(N,N),1)
    eye=(ri==ci).astype(F32)
    for m in range(nm):
        HFs[m][:,:N]=g_refs[m][...]; HFs[m][:,N:]=eye
        YFs[m][:,:N]=xt_refs[m][...].T; YFs[m][:,N:]=eye
        Ls[m][...]=jnp.zeros((N,N),F32)
    rw=lax.broadcasted_iota(jnp.int32,(W,2*N),0); cw=lax.broadcasted_iota(jnp.int32,(W,2*N),1)
    for p in range(NP):
        s=slice(p*W,(p+1)*W)
        res=diag_factor([(HFs[m][s,s],YFs[m][s,s]) for m in range(nm)])
        for m in range(nm):
            rinvt,minv,uinvt,ptop,tfac,tau,met=outs[7*m:7*m+7]
            HF,YF,L=HFs[m],YFs[m],Ls[m]
            Rpp,E,Lpp,U,Wp,tv=res[m]
            tau[0:1,s]=tv
            A=hdot(U,E,NT); B=hdot(U,Wp,NN); T=-hdot(A,B,NT)
            r64=lax.broadcasted_iota(jnp.int32,(W,W),0); c64=lax.broadcasted_iota(jnp.int32,(W,W),1)
            tfac[p]=jnp.where(c64>r64,T,jnp.where(c64==r64,jnp.broadcast_to(tv,(W,W)),0.0))
            Rall=hdot(E,HF[s,:])
            Rall=jnp.where((cw>=N)|(cw>=rw+p*W),Rall,0.0)
            Mrow=YF[s,:]-jnp.where(cw<N,Rall,0.0)
            Nrow=hdot(Wp,Mrow)
            if p<NP-1:
                lo=(p+1)*W
                HF[lo:,:]=HF[lo:,:]-hdot(Rall[:,lo:N],Rall,TN)
                L[lo:,s]=hdot(YF[lo:,s],hdot(Wp,Lpp))
            L[s,s]=Lpp
            HF[s,:]=Rall
            Yc=YF[:,s]
            rr=lax.broadcasted_iota(jnp.int32,(N,W),0)
            Yc=jnp.where((rr>=p*W)&(rr<(p+1)*W),0.0,Yc)
            YF[...]=YF[...]-hdot(Yc,Nrow)
            YF[s,:]=Nrow
    for m in range(nm):
        rinvt,minv,uinvt,ptop,tfac,tau,met=outs[7*m:7*m+7]
        HF,YF,L=HFs[m],YFs[m],Ls[m]
        RT=HF[:,N:]; MI=YF[:,N:]
        rinvt[...]=RT; minv[...]=MI
        uinvt[...]=lax.dot_general(L[...],MI,(((0,),(1,)),((),())),precision=HI,preferred_element_type=F32)
        ptop[...]=jnp.where(ri>ci,L[...],HF[:,:N]).T
        dg=jnp.where(ri==ci,g_refs[m][...],0.0)
        grow=jnp.sqrt(jnp.sum(dg,0,keepdims=True)); gcol=jnp.sqrt(jnp.sum(dg,1,keepdims=True))
        c1=jnp.max(jnp.sum(jnp.abs(RT)*grow,1,keepdims=True),keepdims=True)
        c2=jnp.max(jnp.sum(jnp.abs(MI)*gcol,0,keepdims=True),keepdims=True)
        gmin=jnp.min(grow,keepdims=True); gmax=jnp.max(grow,keepdims=True)
        l8=lax.broadcasted_iota(jnp.int32,(8,128),1)
        met[...]=jnp.where(l8==0,c1,jnp.where(l8==1,c2,jnp.where(l8==2,gmin,gmax)))

def chain(gs,xts):
    nm=len(gs)
    osh=[]
    for m in range(nm):
        osh+= [jax.ShapeDtypeStruct((N,N),F32)]*4+[jax.ShapeDtypeStruct((NP,W,W),F32),jax.ShapeDtypeStruct((1,N),F32),jax.ShapeDtypeStruct((8,128),F32)]
    vm=pl.BlockSpec(memory_space=pltpu.VMEM)
    o=pl.pallas_call(functools.partial(chain_kernel,nm),in_specs=[vm]*(2*nm),out_specs=[vm]*len(osh),out_shape=osh,
        scratch_shapes=[pltpu.VMEM((N,2*N),F32)]*(2*nm)+[pltpu.VMEM((N,N),F32)]*nm,
        compiler_params=pltpu.CompilerParams(vmem_limit_bytes=40*2**20))(*gs,*xts)
    return [o[7*m:7*m+7] for m in range(nm)]


def cross_products(ct, xt):
    cols, rows = ct.shape
    mb = 256

    def body(c_ref, x_ref, o_ref):
        o_ref[...] = hdot(c_ref[...], x_ref[...], NT)

    return pl.pallas_call(
        body, grid=(cols // mb,),
        in_specs=[pl.BlockSpec((mb, rows), lambda i: (i, 0)), pl.BlockSpec((N, rows), lambda i: (0, 0))],
        out_specs=pl.BlockSpec((mb, N), lambda i: (i, 0)),
        out_shape=jax.ShapeDtypeStruct((cols, N), F32),
        cost_estimate=pl.CostEstimate(flops=2 * 6 * cols * rows * N, bytes_accessed=4 * cols * rows, transcendentals=0),
        compiler_params=pltpu.CompilerParams(vmem_limit_bytes=60 * 2**20))(ct, xt)


def solve_small(pt, c1t, rinvt, minv):
    cols = pt.shape[0]
    mb = 256

    def body(p_ref, c_ref, r_ref, m_ref, rc_ref, z_ref, f_ref):
        rc = hdot(p_ref[...], r_ref[...], NT)
        z = hdot(c_ref[...] - rc, m_ref[...], NT)
        rc_ref[...] = rc
        z_ref[...] = z
        zero = jnp.sum(jnp.sum(z * 0.0, 0, keepdims=True), 1, keepdims=True)
        @pl.when(pl.program_id(0) == 0)
        def _():
            f_ref[...] = jnp.zeros_like(f_ref)
        f_ref[...] += jnp.broadcast_to(zero, f_ref.shape)

    blk = pl.BlockSpec((mb, N), lambda i: (i, 0))
    whole = pl.BlockSpec((N, N), lambda i: (0, 0))
    return pl.pallas_call(
        body, grid=(cols // mb,), in_specs=[blk, blk, whole, whole],
        out_specs=[blk, blk, pl.BlockSpec((8, 128), lambda i: (0, 0))],
        out_shape=[jax.ShapeDtypeStruct((cols, N), F32)] * 2 + [jax.ShapeDtypeStruct((8, 128), F32)])(pt, c1t, rinvt, minv)


def apply_update(rank, ct, xt, zt, rct, upt, ptt):
    cols, rows = ct.shape
    nb = 512
    mb = 512
    own = upt.shape[0]

    def body(rank_ref, c_ref, x_ref, z_ref, rc_ref, up_ref, pt_ref, o_ref):
        x = x_ref[...]
        o_ref[0:own, :] = hdot(up_ref[...], x)
        o_ref[own:mb, :] = c_ref[own:mb, :] - hdot(z_ref[own:mb, :], x)
        for j in range(1, cols // mb):
            s = slice(j * mb, (j + 1) * mb)
            o_ref[s, :] = c_ref[s, :] - hdot(z_ref[s, :], x)

        @pl.when((pl.program_id(0) == 0) & (rank_ref[0] == 0))
        def _():
            o_ref[0:own, 0:N] = pt_ref[...]
            o_ref[own:, 0:N] = rc_ref[own:, :]

    blk = pl.BlockSpec((cols, nb), lambda i, r: (0, i))
    fixed = lambda a: pl.BlockSpec(a.shape, lambda i, r: (0, 0))
    return pl.pallas_call(
        body,
        grid_spec=pltpu.PrefetchScalarGridSpec(
            num_scalar_prefetch=1, grid=(rows // nb,),
            in_specs=[blk, pl.BlockSpec((N, nb), lambda i, r: (0, i)), fixed(zt), fixed(rct), fixed(upt), fixed(ptt)],
            out_specs=blk),
        out_shape=jax.ShapeDtypeStruct((cols, rows), F32),
        cost_estimate=pl.CostEstimate(flops=2 * 6 * cols * rows * N, bytes_accessed=8 * cols * rows, transcendentals=0),
        compiler_params=pltpu.CompilerParams(vmem_limit_bytes=60 * 2**20))(rank, ct, xt, zt, rct, upt, ptt)


def factor_columns(stored):
    local_rows, local_blocks, width = stored.shape
    row_rank = lax.axis_index("row")
    col_rank = lax.axis_index("col")
    row_ids = row_rank * local_rows + jnp.arange(local_rows)
    col_ids = jnp.arange(width)

    def panel_step(panel_idx, state):
        stored, taus, tfs = state
        row_start = panel_idx * width
        local_idx = panel_idx // 2
        is_owner = col_rank == panel_idx % 2
        panel_in = lax.dynamic_slice_in_dim(stored, local_idx, 1, axis=1)[:, 0, :]

        def column_step(col_idx, loop_state):
            work, tau_vec = loop_state
            diag_idx = row_start + col_idx
            column = lax.dynamic_slice_in_dim(work, col_idx, 1, axis=1)[:, 0]
            below = jnp.where(row_ids >= diag_idx, column, 0.0)
            at_diag = (row_ids == diag_idx).astype(F32)
            summed = lax.psum(jnp.stack([
                jnp.dot(below, work, precision=PRECISE, preferred_element_type=F32),
                jnp.dot(at_diag, work, precision=PRECISE, preferred_element_type=F32)]), "row")
            cross, diag_row = summed[0], summed[1]
            pivot = lax.dynamic_slice_in_dim(diag_row, col_idx, 1)[0]
            norm = jnp.sqrt(lax.dynamic_slice_in_dim(cross, col_idx, 1)[0])
            beta = -jnp.where(pivot >= 0, 1.0, -1.0) * norm
            tau = (beta - pivot) / beta
            denom = pivot - beta
            proj = jnp.where(col_ids > col_idx, (cross - beta * diag_row) / denom, 0.0)
            refl = jnp.where(row_ids > diag_idx, column / denom, 0.0) + at_diag
            work = work - tau * refl[:, None] * proj[None, :]
            new_col = jnp.where(row_ids < diag_idx, column, jnp.where(row_ids == diag_idx, beta, refl))
            work = lax.dynamic_update_slice_in_dim(work, new_col[:, None], col_idx, axis=1)
            return work, lax.dynamic_update_slice_in_dim(tau_vec, tau[None], col_idx, axis=0)

        work, tau_vec = lax.fori_loop(0, width, column_step, (panel_in, jnp.zeros((width,), F32)))
        diag_ids = row_start + col_ids[None, :]
        v_block = jnp.where(row_ids[:, None] == diag_ids, 1.0, jnp.where(row_ids[:, None] > diag_ids, work, 0.0))
        gram = lax.psum(jnp.einsum("ri,rj->ij", v_block, v_block, precision=PRECISE, preferred_element_type=F32), "row")

        def t_step(col_idx, tf):
            g = lax.dynamic_slice_in_dim(gram, col_idx, 1, axis=1)[:, 0]
            g = jnp.where(col_ids < col_idx, g, 0.0)
            tau_k = lax.dynamic_slice_in_dim(tau_vec, col_idx, 1)[0]
            t_col = -tau_k * jnp.dot(tf, g, precision=PRECISE, preferred_element_type=F32)
            t_col = jnp.where(col_ids == col_idx, tau_k, t_col)
            return lax.dynamic_update_slice_in_dim(tf, t_col[:, None], col_idx, axis=1)

        tf = lax.fori_loop(0, width, t_step, jnp.zeros((width, width), F32))
        v_block, tf = lax.psum((jnp.where(is_owner, v_block, 0.0), jnp.where(is_owner, tf, 0.0)), "col")

        def block_step(b, stored):
            blk = lax.dynamic_slice_in_dim(stored, b, 1, axis=1)[:, 0, :]
            proj = lax.psum(jnp.einsum("ri,rk->ik", v_block, blk, precision=PRECISE, preferred_element_type=F32), "row")
            w = jnp.einsum("ij,ik->jk", tf, proj, precision=PRECISE, preferred_element_type=F32)
            upd = blk - jnp.einsum("ri,ik->rk", v_block, w, precision=PRECISE, preferred_element_type=F32)
            keep = b * 2 + col_rank > panel_idx
            mine = (b == local_idx) & is_owner
            new = jnp.where(keep, upd, jnp.where(mine, work, blk))
            return lax.dynamic_update_slice_in_dim(stored, new[:, None, :], b, axis=1)

        stored = lax.fori_loop(0, local_blocks, block_step, stored)
        taus = lax.dynamic_update_slice_in_dim(taus, jnp.diagonal(tf), row_start, axis=0)
        return stored, taus, lax.dynamic_update_slice_in_dim(tfs, tf[None], panel_idx, axis=0)

    return lax.fori_loop(0, PANELS, panel_step, (stored, jnp.zeros((PANELS * width,), F32), jnp.zeros((PANELS, width, width), F32)))


R1 = [(0, 1), (1, 0), (2, 3), (3, 2)]
R2 = [(0, 2), (2, 0), (1, 3), (3, 1)]
CY = [(0, 1), (1, 0)]


def solution(mesh):
    def factor_both(a_matrix, b_matrix):
        local_rows, local_blocks, width = a_matrix.shape
        cols = local_blocks * width
        half = cols // 2
        own = 2 * width
        row_rank = lax.axis_index("row")
        col_rank = lax.axis_index("col")
        core = row_rank % 2
        chip = row_rank // 2
        mats = [a_matrix, b_matrix]
        cts = [m.transpose(1, 2, 0).reshape(cols, local_rows) for m in mats]

        def interleave(mine, peer, n):
            o = mine.reshape(2, width, n)
            q = peer.reshape(2, width, n)
            first = jnp.where(col_rank == 0, o, q)
            second = jnp.where(col_rank == 0, q, o)
            return jnp.stack([first, second], 1).reshape(4 * width, n)

        def my_half(x):
            return lax.dynamic_slice_in_dim(x, core * half, half, 0)

        xts, pts, c1s, gs, x1s = [], [], [], [], []
        for ct in cts:
            mine = ct[:own]
            xts.append(interleave(mine, lax.ppermute(mine, "col", CY), local_rows))
        for ct, xt in zip(cts, xts):
            top = ct[:, :N]
            over = lax.ppermute(top[half:], "row", [(0, 1)])
            here = jnp.where(core == 0, top[:half], over)
            down = lax.ppermute(here, "row", [(0, 2), (1, 3)])
            c1s.append(jnp.where(chip == 0, here, down))
            x1 = xt[:, :N]
            o1 = lax.ppermute(x1, "row", [(0, 1)])
            h1 = jnp.where(core == 0, x1, o1)
            d1 = lax.ppermute(h1, "row", [(0, 2), (1, 3)])
            x1s.append(jnp.where(chip == 0, h1, d1))
        for ct, xt in zip(cts, xts):
            pt = cross_products(ct, xt)
            g = pt[:own]
            g = g + lax.ppermute(g, "row", R1)
            g = g + lax.ppermute(g, "row", R2)
            gs.append(interleave(g, lax.ppermute(g, "col", CY), N))
            send = lax.dynamic_slice_in_dim(pt, (1 - core) * half, half, 0)
            acc = my_half(pt) + lax.ppermute(send, "row", R1)
            pts.append(acc + lax.ppermute(acc, "row", R2))
        small = chain(gs, x1s)
        outs = []
        ok = jnp.ones((), jnp.bool_)
        for i in range(2):
            rinvt, minv, uinvt, ptop, tfac, tau, met = small[i]
            rc, z, fin = solve_small(pts[i], c1s[i], rinvt, minv)
            zo = lax.ppermute(z, "row", R1)
            zt = jnp.where(core == 0, jnp.concatenate([z, zo], 0), jnp.concatenate([zo, z], 0))
            rct = jnp.concatenate([rc, lax.ppermute(rc, "row", [(1, 0)])], 0)
            pick = lambda x: jnp.where(col_rank == 0, x.reshape(2, 2, width, N)[:, 0], x.reshape(2, 2, width, N)[:, 1]).reshape(own, N)
            outs.append((zt, rct, pick(uinvt), pick(ptop), tau[0], tfac))
            ok &= (met[0, 0] <= 64.0) & (met[0, 1] <= 64.0) & (met[0, 2] >= 1e-5) & (met[0, 3] <= 1e10) & (fin[0, 0] == 0.0)
        flag = jnp.where(ok, 1.0, 0.0).astype(F32).reshape(1)
        flag = flag * lax.ppermute(flag, "row", R1)
        flag = flag * lax.ppermute(flag, "row", R2)
        flag = flag * lax.ppermute(flag, "col", CY)
        rank = row_rank.astype(jnp.int32).reshape(1)
        carry = [flag]
        for i in range(2):
            zt, rct, upt, ptt, tau, tfac = outs[i]
            carry += [apply_update(rank, cts[i], xts[i], zt, rct, upt, ptt), tau, tfac]

        def redo(state):
            new = [jnp.ones((1,), F32)]
            for m in (a_matrix, b_matrix):
                st, taus, tfs = factor_columns(m)
                new += [st.transpose(1, 2, 0).reshape(cols, local_rows), taus, tfs]
            return tuple(new)

        res = lax.while_loop(lambda s: s[0][0] < 0.5, redo, tuple(carry))
        back = lambda x: x.reshape(local_blocks, width, local_rows).transpose(2, 0, 1)
        return back(res[1]), res[2], res[3], back(res[4]), res[5], res[6]

    spec_mat = P(("batch", "row"), "col", None)
    spec_out = (spec_mat, P("batch"), P("batch", None, None))
    return jax.shard_map(factor_both, mesh=mesh, in_specs=(spec_mat, spec_mat), out_specs=spec_out + spec_out, check_vma=False)
```

```python
import functools

import jax
import jax.numpy as jnp
from jax import lax
from jax.experimental import pallas as pl
from jax.experimental.pallas import tpu as pltpu
from jax.sharding import PartitionSpec as P

F32 = jnp.float32
BF = jnp.bfloat16
HI = lax.Precision.HIGHEST
PANELS = 4
W = 64
NP = 4
N = 256
NN = (((1,), (0,)), ((), ()))
NT = (((1,), (1,)), ((), ()))
TN = (((0,), (0,)), ((), ()))


BOTH = (0, 1)
TILE = (8, 128)


def rows_of(shape):
    return lax.broadcasted_iota(jnp.int32, shape, 0)


def lanes_of(shape):
    return lax.broadcasted_iota(jnp.int32, shape, 1)


def hdot(a, b, dn=NN):
    return lax.dot_general(a, b, dn, precision=HI, preferred_element_type=F32)


GROUP = 4
AMPLIFY = 64.0
HUGE = 1e9


def diag_factor(mats):
    tiles = W // 8
    lane8 = lanes_of(TILE)
    sub8 = rows_of(TILE)
    r64 = rows_of((W, W))
    c64 = lanes_of((W, W))
    eye = (r64 == c64).astype(F32)
    full = lambda x: jnp.broadcast_to(x, TILE)
    zeros = jnp.zeros(TILE, F32)
    st = []
    for hpp, ypp in mats:
        he = jnp.concatenate([hpp, eye], 1)
        yw = jnp.concatenate([ypp, eye], 1)
        st.append(dict(he=[he[8 * g:8 * g + 8] for g in range(tiles)], yw=[yw[8 * g:8 * g + 8] for g in range(tiles)],
                       l=[zeros] * tiles, u=[zeros] * tiles, tau=zeros))
    for k0 in range(0, W, GROUP):
        gk = k0 // 8
        for s in st:
            s['bh'] = [[full(s['he'][g][:, k:k + 1]) for g in range(gk, tiles)] for k in range(k0, k0 + GROUP)]
            s['by'] = [[full(s['yw'][g][:, k:k + 1]) for g in range(tiles)] for k in range(k0, k0 + GROUP)]
        for k in range(k0, k0 + GROUP):
            sk = k - 8 * gk
            isk = sub8 == sk
            for s in st:
                ch, cy = s['bh'][k - k0], s['by'][k - k0]
                pick = lambda x: full(x[sk:sk + 1, :])
                h = pick(ch[0])
                a = pick(cy[gk])
                rs = lax.rsqrt(h)
                rinv = jnp.where(a >= 0, -rs, rs)
                ukk = a - h * rinv
                uinv = 1.0 / ukk
                r = pick(s['he'][gk]) * rinv
                u = pick(s['yw'][gk]) - jnp.where((lane8 >= k) & (lane8 < W), r, 0.0)
                un = u * uinv
                rr = r * rinv
                for k2 in range(k + 1, k0 + GROUP):
                    r2 = pick(s['bh'][k2 - k0][0]) * rinv
                    un2 = (pick(s['by'][k2 - k0][gk]) - r2) * uinv
                    rr2 = r2 * rinv
                    s['bh'][k2 - k0] = [x - ch[i] * rr2 for i, x in enumerate(s['bh'][k2 - k0])]
                    nby = [x - cy[i] * un2 for i, x in enumerate(s['by'][k2 - k0])]
                    nby[gk] = jnp.where(isk, un2, nby[gk])
                    s['by'][k2 - k0] = nby
                for g in range(gk, tiles):
                    new = s['he'][g] - ch[g - gk] * rr
                    lc = cy[g] * uinv
                    if g == gk:
                        new = jnp.where(sub8 > sk, new, jnp.where(isk, r, s['he'][g]))
                        lc = jnp.where(sub8 > sk, lc, 0.0)
                    s['he'][g] = new
                    s['l'][g] = jnp.where(lane8 == k, lc, s['l'][g])
                for g in range(tiles):
                    new = s['yw'][g] - cy[g] * un
                    s['yw'][g] = jnp.where(isk, un, new) if g == gk else new
                s['u'][gk] = jnp.where(isk, u, s['u'][gk])
                s['tau'] = jnp.where(lane8 == k, -ukk * rinv, s['tau'])
    out = []
    up = c64 >= r64
    for s in st:
        he = jnp.concatenate(s['he'], 0)
        yw = jnp.concatenate(s['yw'], 0)
        l = jnp.concatenate(s['l'], 0)[:, :W]
        u = jnp.concatenate(s['u'], 0)[:, :W]
        out.append((jnp.where(c64 <= r64, he[:, W:], 0.0), l + eye, jnp.where(up, u, 0.0), yw[:, W:], s['tau'][0:1, :W]))
    return out


def blk(b):
    return slice(b * W, (b + 1) * W)


def order(c):
    return [2 * l + c for l in BOTH] + [2 * l + 1 - c for l in BOTH]


def turn(x):
    return jnp.concatenate([x[:, W:N], x[:, :W], x[:, N:]], 1)


CHAIN_SCRATCH = [(N, 2 * N), (N, 2 * N), (N, N), (4, W, W), (8, N), (8, W)]
CHAIN_SHAPES = [(N, N), (N, N), (2 * W, N), (2 * W, N), (N, W), (NP, W), TILE]


def chain_init(col, g, x1, st):
    hs, ys, ls, _, norm, _ = st
    ri, ci = rows_of((N, N)), lanes_of((N, N))
    eye = (ri == ci).astype(F32)
    for c in BOTH:
        @pl.when(col == c)
        def _():
            for i, b in enumerate(order(c)):
                ls[blk(b), :] = x1[blk(i), :]
                for i2, b2 in enumerate(order(c)):
                    hs[blk(b), blk(b2)] = g[blk(i), blk(i2)]
    hs[:, N:] = eye
    ys[:, :N] = ls[...].T
    ys[:, N:] = eye
    dg = jnp.where(ri == ci, hs[:, :N], 0.0)
    norm[...] = jnp.broadcast_to(jnp.sqrt(jnp.sum(dg, 0, keepdims=True)), (8, N))


def chain_cols(st):
    hs, ys, _, fac, _, tv = st
    e, l, u, w, tau = diag_factor([(hs[0:W, 0:W], ys[0:W, 0:W])])[0]
    for i, x in enumerate((e, l, u, w)):
        fac[i] = x
    tv[...] = jnp.broadcast_to(tau, (8, W))


def chain_update(p, st, tfac, tau):
    hs, ys, ls, fac, _, tv = st
    r64 = rows_of((W, W))
    c64 = lanes_of((W, W))
    rw = rows_of((W, 2 * N))
    cw = lanes_of((W, 2 * N))
    rl = rows_of((N - W, W))
    live = N - p * W
    e, l, u, w = fac[0], fac[1], fac[2], fac[3]
    t = -hdot(hdot(u, e, NT), hdot(u, w), NT)
    d = pl.ds(pl.multiple_of(p * W, W), W)
    tfac[d, :] = jnp.where(c64 > r64, t, jnp.where(c64 == r64, jnp.broadcast_to(tv[0:1, :], (W, W)), 0.0))
    tau[pl.ds(p, 1), :] = tv[0:1, :]
    rall = hdot(e, hs[0:W, :])
    rall = jnp.where((cw >= N) | ((cw >= rw) & (cw < live)), rall, 0.0)
    nrow = hdot(w, ys[0:W, :] - jnp.where(cw < N, rall, 0.0))
    hnew = hs[W:, :] - hdot(rall[:, W:N], rall, TN)
    yc = ys[W:, 0:W]
    ynew = ys[W:, :] - hdot(yc, nrow)
    lnew = jnp.where(rl < live - W, hdot(yc, hdot(w, l)), 0.0)
    rest = ls[W:, W:]
    first = ls[0:W, W:]
    ls[0:N - W, N - W:] = lnew
    ls[N - W:, N - W:] = l
    ls[0:N - W, 0:N - W] = rest
    ls[N - W:, 0:N - W] = first
    hs[0:N - W, :] = turn(hnew)
    hs[N - W:, :] = turn(rall)
    ys[0:N - W, :] = turn(ynew)
    ys[N - W:, :] = turn(nrow)


def chain_final(col, st, outs):
    hs, ys, ls, _, norm, _ = st
    rinvt, minv, upt, ptt, _, _, bad = outs
    ri = rows_of((N, N))
    ci = lanes_of((N, N))
    rt, mi = hs[:, N:], ys[:, N:]
    g = norm[0:1, :]
    c1 = jnp.max(jnp.sum(jnp.abs(rt) * g, 1, keepdims=True), keepdims=True)
    c2 = jnp.max(hdot(g, jnp.abs(mi)), keepdims=True)
    good = (c1 <= AMPLIFY) & (c2 <= AMPLIFY) & (jnp.min(g, keepdims=True) >= 1 / HUGE) & (jnp.max(g, keepdims=True) <= HUGE)
    bad[...] = jnp.broadcast_to(jnp.where(good, 0.0, 1.0), TILE)
    pt = jnp.where(ri > ci, ls[...], hs[:, :N]).T
    ut = lax.dot_general(ls[...], mi, (((0,), (1,)), ((), ())), precision=HI, preferred_element_type=F32)
    hs[:, :N] = pt
    ys[:, :N] = ut
    for c in BOTH:
        @pl.when(col == c)
        def _():
            for i, b in enumerate(order(c)):
                rinvt[:, blk(i)] = hs[:, N + b * W:N + (b + 1) * W]
                minv[blk(i), :] = ys[blk(b), N:]
            for i in BOTH:
                b = order(c)[i]
                ptt[blk(i), :] = hs[blk(b), :N]
                for i2, b2 in enumerate(order(c)):
                    upt[blk(i), blk(i2)] = ys[blk(b), blk(b2)]


def split3(x):
    h = x.astype(BF)
    r = x - h.astype(F32)
    m = r.astype(BF)
    return h, m, (r - m.astype(F32)).astype(BF)


def dot6(a, b, dn):
    d = lambda i, j: lax.dot_general(a[i], b[j], dn, preferred_element_type=F32)
    return (((d(2, 0) + d(0, 2)) + d(1, 1)) + (d(1, 0) + d(0, 1))) + d(0, 0)


CHUNK = 1024
SPAN = 1024
SLOTS = 3
AHEAD = SLOTS - 1


def exchange_kernel(ca, cb, peer_a, peer_b, c1a, c1b, pam, pao, pbm, g_out, x1b, *refs):
    outs, refs = refs[:len(CHAIN_SHAPES)], refs[len(CHAIN_SHAPES):]
    st, refs = refs[:len(CHAIN_SCRATCH)], refs[len(CHAIN_SCRATCH):]
    (x1a, peer, own, xs, cbuf, acc, gacc, r1buf, r2buf, gloc, gbuf1, gsum, gbuf2,
     c_sem, own_sem, out_sem, y_send, y_recv, top_send, top_recv, swap_send, swap_recv,
     g_send, g_recv, p_send, p_recv, x_send, x_recv) = refs
    cts, x1 = (ca, cb), (x1a, x1b)
    row = lax.axis_index("row")
    col = lax.axis_index("col")
    core = lax.rem(row, 2)
    mate = row + 1 - 2 * core
    across = lax.rem(row + 2, 4)
    diag = lax.rem(row + 3 - 2 * core, 4)
    cols, rows = ca.shape
    half = cols // 2
    nown = peer.shape[1]
    nchunk = cols // CHUNK
    spans = rows // SPAN
    trips = nchunk * spans

    def remote(src, dst, send, recv, **where):
        return pltpu.make_async_remote_copy(src_ref=src, dst_ref=dst, send_sem=send, recv_sem=recv,
                                            device_id=where, device_id_type=pl.DeviceIdType.MESH)

    to_mate = functools.partial(remote, row=mate)
    to_across = functools.partial(remote, row=across)

    def c_copy(m, t):
        slot = lax.rem(m * trips + t, SLOTS)
        h, j = lax.div(t, nchunk), lax.rem(t, nchunk)
        return pltpu.make_async_copy(
            cts[m].at[pl.ds(pl.multiple_of(j * CHUNK, CHUNK), CHUNK), pl.ds(pl.multiple_of(h * SPAN, SPAN), SPAN)],
            cbuf.at[slot], c_sem.at[slot])

    first = pl.ds(0, nown)
    second = pl.ds(nown, nown)
    lanes = pl.ds(0, N)

    def y_copy(m, h):
        s = pl.ds(pl.multiple_of(h * SPAN, SPAN), SPAN)
        i = m * spans + h
        return remote(cts[m].at[first, s], peer.at[m, :, s], y_send.at[i], y_recv.at[i], col=1 - col)

    own_copies = [pltpu.make_async_copy(cts[m].at[first, :], own.at[m], own_sem.at[m]) for m in BOTH]
    for o in own_copies:
        o.start()
    for t in range(AHEAD):
        c_copy(0, t).start()

    barrier = pltpu.get_barrier_semaphore()
    for where in (dict(row=mate), dict(row=across), dict(row=diag), dict(col=1 - col)):
        pl.semaphore_signal(barrier, device_id=where, device_id_type=pl.DeviceIdType.MESH)
    pl.semaphore_wait(barrier, 4)

    for m in BOTH:
        for h in range(spans):
            y_copy(m, h).start()

    tops = (c1a, c1b)
    lows = [pl.ds(0, half), pl.ds(half, half)]
    x_local = [pltpu.make_async_copy(cts[m].at[first, lanes], x1[m].at[first, :], own_sem.at[2 + m]) for m in BOTH]
    x_own = [[remote(cts[m].at[first, lanes], x1[m].at[first, :], top_send.at[m, k], top_recv.at[m], row=k + 1)
              for k in range(3)] for m in BOTH]
    x_peer = [[remote(peer.at[m, :, lanes], x1[m].at[second, :], top_send.at[2 + m, k], top_recv.at[2 + m], row=k + 1)
               for k in range(3)] for m in BOTH]
    top_far = [[remote(cts[m].at[:, lanes], tops[m], top_send.at[4 + m, 0], top_recv.at[4 + m], row=1)]
               + [remote(cts[m].at[lows[k], lanes], tops[m].at[lows[k], :], top_send.at[4 + m, 1 + k], top_recv.at[4 + m], row=2 + k)
                  for k in BOTH] for m in BOTH]

    @pl.when(row == 0)
    def _():
        for m in BOTH:
            x_local[m].start()
        for c in x_own[0] + x_own[1] + top_far[0] + top_far[1]:
            c.start()

    mine = pl.ds(pl.multiple_of(core * half, half), half)
    others = pl.ds(pl.multiple_of((1 - core) * half, half), half)
    p1 = [to_mate(acc.at[m, others, :], r1buf.at[m], p_send.at[m], p_recv.at[m]) for m in BOTH]
    g1 = [to_mate(gloc.at[m], gbuf1.at[m], g_send.at[m], g_recv.at[m]) for m in BOTH]
    g2 = [to_across(gsum.at[m], gbuf2.at[m], g_send.at[2 + m], g_recv.at[2 + m]) for m in BOTH]
    p2 = to_across(r1buf.at[0], r2buf, x_send.at[0], x_recv.at[0])
    p3 = to_mate(r1buf.at[0], pao, x_send.at[1], x_recv.at[1])
    swap = [to_mate(tops[m].at[mine, :], tops[m].at[mine, :], swap_send.at[m], swap_recv.at[m]) for m in BOTH]
    peer_out = [pltpu.make_async_copy(peer.at[m], (peer_a, peer_b)[m], out_sem.at[m]) for m in BOTH]
    pam_out = pltpu.make_async_copy(r1buf.at[0], pam, out_sem.at[2])
    pbm_out = pltpu.make_async_copy(r1buf.at[1], pbm, out_sem.at[3])

    def add_half(m):
        p1[m].wait()
        r1buf[m] = r1buf[m] + acc[m, mine, :]

    def start_g(m):
        gloc[m, 0:nown, :] = acc[m, 0:nown, :]
        gloc[m, nown:, :] = gacc[m]
        g1[m].start()

    def finish_g1(m):
        g1[m].wait()
        gsum[m] = gloc[m] + gbuf1[m]
        g2[m].start()

    def send_x(m):
        @pl.when(row == 0)
        def _():
            x1[m][nown:, :] = peer[m, :, 0:N]
            for c in x_peer[m]:
                c.start()

    def wait_x(m):
        @pl.when(row == 0)
        def _():
            x_local[m].wait()

        @pl.when(row > 0)
        def _():
            x_own[m][0].wait_recv()
            x_peer[m][0].wait_recv()

    def sums_a():
        finish_g1(0)
        add_half(0)
        p2.start()

    def begin_chain():
        wait_x(0)
        g2[0].wait()
        gsum[0] = gsum[0] + gbuf2[0]
        chain_init(col, gsum.at[0], x1a, st)

    def top_rows():
        @pl.when(row == 1)
        def _():
            for m in BOTH:
                top_far[m][0].wait_recv()

        @pl.when(row >= 2)
        def _():
            for m in BOTH:
                top_far[m][1].wait_recv()
                swap[m].start()

    def finish_chain():
        chain_final(col, st, outs)
        top_rows()

    def last_sums_a():
        p2.wait()
        r1buf[0] = r1buf[0] + r2buf[...]
        p3.start()
        pam_out.start()

    last = trips - nchunk
    begin = last - NP
    hooks = [[(0, lambda: send_x(0))],
             [(0, lambda: send_x(1)), (begin - 1, begin_chain), (last - 2, last_sums_a), (last - 1, finish_chain),
              (last, lambda: start_g(1))]]

    def products(m):
        def span(h, _):
            y_copy(m, h).wait_recv()
            s0 = pl.multiple_of(h * SPAN, SPAN)

            def build(q, _):
                d = pl.ds(pl.multiple_of(q * 512, 512), 512)
                s = pl.ds(pl.multiple_of(s0 + q * 512, 512), 512)
                for i, part in enumerate(split3(own[m, :, s])):
                    xs[i, 0:nown, d] = part
                for i, part in enumerate(split3(peer[m, :, s])):
                    xs[i, nown:, d] = part
                return 0

            lax.fori_loop(0, SPAN // 512, build, 0)
            x = (xs[0], xs[1], xs[2])
            r = dot6([xs[i, nown:, :] for i in range(3)], x, NT)
            gacc[m] = jnp.where(h == 0, r, gacc[m] + r)

            def trip(j, _):
                t = h * nchunk + j
                slot = lax.rem(m * trips + t, SLOTS)
                c_copy(m, t).wait()

                @pl.when(t + AHEAD < trips)
                def _():
                    c_copy(m, t + AHEAD).start()

                if m == 0:
                    @pl.when(t + AHEAD >= trips)
                    def _():
                        c_copy(1, t + AHEAD - trips).start()

                def core_trip():
                    r = dot6(split3(cbuf[slot]), (xs[0], xs[1], xs[2]), NT)
                    d = pl.ds(pl.multiple_of(j * CHUNK, CHUNK), CHUNK)
                    acc[m, d, :] = jnp.where(h == 0, r, acc[m, d, :] + r)

                if m == 0:
                    core_trip()
                else:
                    live = (t >= begin) & (t < last)

                    @pl.when(live)
                    def _():
                        chain_cols(st)
                        core_trip()
                        chain_update(t - begin, st, outs[4], outs[5])

                    pl.when(~live)(core_trip)
                for at, hook in hooks[m]:
                    pl.when(t == at)(hook)
                return 0

            lax.fori_loop(0, nchunk, trip, 0)
            return 0

        own_copies[m].wait()
        lax.fori_loop(0, spans, span, 0)

    products(0)
    start_g(0)
    p1[0].start()
    peer_out[0].start()
    sums_a()
    products(1)
    p1[1].start()
    finish_g1(1)
    peer_out[1].start()
    wait_x(1)
    add_half(1)
    pbm_out.start()
    g2[1].wait()
    g_out[...] = gsum[1] + gbuf2[1]

    @pl.when(row == 0)
    def _():
        for c in x_own[0] + x_own[1] + x_peer[0] + x_peer[1] + top_far[0] + top_far[1]:
            c.wait_send()

    @pl.when(row >= 2)
    def _():
        for m in BOTH:
            swap[m].wait()

    for c in peer_out + [p3, pam_out, pbm_out]:
        c.wait()
    for m in BOTH:
        for h in range(spans):
            y_copy(m, h).wait_send()


def exchange(ca, cb, own):
    cols, rows = ca.shape
    half = cols // 2
    hbm = pl.BlockSpec(memory_space=pl.ANY)
    vm = pl.BlockSpec(memory_space=pltpu.VMEM)
    dma = pltpu.SemaphoreType.DMA
    pair = (2, N, N)
    ny = 2 * rows // SPAN
    shapes = [(own, rows)] * 2 + [(cols, N)] * 2 + [(half, N)] * 3 + [(N, N), (N, N)] + CHAIN_SHAPES
    scratch = CHAIN_SCRATCH + [(N, N), (2, own, rows), (2, own, rows)]
    after = [(SLOTS, CHUNK, SPAN), (2, cols, N), (2, own, N), (2, half, N), (half, N)] + [pair] * 4
    return pl.pallas_call(
        exchange_kernel,
        in_specs=[hbm, hbm],
        out_specs=[hbm] * 7 + [vm] * (2 + len(CHAIN_SHAPES)),
        out_shape=[jax.ShapeDtypeStruct(s, F32) for s in shapes],
        scratch_shapes=[pltpu.VMEM(s, F32) for s in scratch] + [pltpu.VMEM((3, 2 * own, SPAN), BF)]
        + [pltpu.VMEM(s, F32) for s in after]
        + [dma(n) for n in ((SLOTS,), (4,), (4,), (ny,), (ny,), (6, 3), (6,), (2,), (2,), (4,), (4,), (2,), (2,), (2,), (2,))],
        cost_estimate=pl.CostEstimate(flops=24 * cols * rows * N, bytes_accessed=8 * cols * rows, transcendentals=0),
        compiler_params=pltpu.CompilerParams(vmem_limit_bytes=60 * 2**20, collective_id=0, has_side_effects=True))(ca, cb)


def apply_update(ids, ct, peer, psum, poth, c1, small, before, nxt=None):
    cols, rows = ct.shape
    nb = 512
    mb = 512
    own = peer.shape[0]
    half = cols // 2
    steps = rows // nb
    rinvt, minv, upt, ptt, _, _, bad = small
    no = len(CHAIN_SHAPES)

    def body(ids_ref, c_ref, x_ref, p_ref, q_ref, c1_ref, r_ref, m_ref, up_ref, pt_ref, bad_ref, before_ref, *refs):
        if nxt is None:
            o_ref, f_ref, z_ref, rc_ref = refs
        else:
            ins, (o_ref, f_ref), outs, (z_ref, rc_ref), st = refs[:2], refs[2:4], refs[4:4 + no], refs[4 + no:6 + no], refs[6 + no:]
        i = pl.program_id(0)
        top = ids_ref[0] == 0

        @pl.when(i == 0)
        def _():
            zero = jnp.zeros((1, 1), F32)
            for src, which in ((p_ref, 0), (q_ref, 1)):
                base = pl.multiple_of((ids_ref[1] ^ which) * half, half)
                for j in range(half // mb):
                    s = slice(j * mb, (j + 1) * mb)
                    d = pl.ds(base + j * mb, mb)
                    rc = hdot(src[s, :], r_ref[...], NT)
                    z = hdot(jnp.where(top, c_ref[d, 0:N], c1_ref[d, :]) - rc, m_ref[...], NT)
                    rc_ref[d, :] = rc
                    z_ref[d, :] = z
                    zero = zero + jnp.sum(jnp.sum(z * 0.0, 0, keepdims=True), 1, keepdims=True)
            f_ref[...] = jnp.where(zero == 0.0, 0.0, 1.0) + bad_ref[...] + before_ref[...]
            if nxt is not None:
                chain_init(ids_ref[2], *ins, st)

        def products():
            x = jnp.concatenate([c_ref[0:own, :], x_ref[...]], 0)
            o_ref[0:own, :] = hdot(up_ref[...], x)
            o_ref[own:mb, :] = c_ref[own:mb, :] - hdot(z_ref[own:mb, :], x)
            for j in range(1, cols // mb):
                s = slice(j * mb, (j + 1) * mb)
                o_ref[s, :] = c_ref[s, :] - hdot(z_ref[s, :], x)

        if nxt is None:
            products()
        else:
            @pl.when(lax.rem(i, 2) == 0)
            def _():
                chain_cols(st)
                products()

            @pl.when(lax.rem(i, 2) == 1)
            def _():
                products()
                chain_update(lax.div(i, 2), st, outs[4], outs[5])

            @pl.when(i == steps - 1)
            def _():
                chain_final(ids_ref[2], st, outs)

        @pl.when((i == 0) & top)
        def _():
            o_ref[0:own, 0:N] = pt_ref[...]
            o_ref[own:, 0:N] = rc_ref[own:, :]

    blk2 = pl.BlockSpec((cols, nb), lambda i, r: (0, i))
    fixed = lambda shape: pl.BlockSpec(shape, lambda i, r: (0, 0))
    consts = [psum, poth, c1, rinvt, minv, upt, ptt, bad, before] + list(nxt or [])
    more = CHAIN_SHAPES if nxt is not None else []
    scratch = [(cols, N), (cols, N)] + (CHAIN_SCRATCH if nxt is not None else [])
    return pl.pallas_call(
        body,
        grid_spec=pltpu.PrefetchScalarGridSpec(
            num_scalar_prefetch=1, grid=(steps,),
            in_specs=[blk2, pl.BlockSpec((own, nb), lambda i, r: (0, i))] + [fixed(a.shape) for a in consts],
            out_specs=[blk2, fixed((8, 128))] + [fixed(s) for s in more],
            scratch_shapes=[pltpu.VMEM(s, F32) for s in scratch]),
        out_shape=[jax.ShapeDtypeStruct(s, F32) for s in [(cols, rows), (8, 128)] + more],
        cost_estimate=pl.CostEstimate(flops=2 * 6 * cols * rows * N, bytes_accessed=8 * cols * rows, transcendentals=0),
        compiler_params=pltpu.CompilerParams(vmem_limit_bytes=60 * 2**20))(ids, ct, peer, *consts)


R1 = [(0, 1), (1, 0), (2, 3), (3, 2)]
R2 = [(0, 2), (2, 0), (1, 3), (3, 1)]
CY = [(0, 1), (1, 0)]


def row_major(x):
    def body(i_ref, o_ref):
        o_ref[...] = i_ref[...]

    return pl.pallas_call(body, out_shape=jax.ShapeDtypeStruct(x.shape, F32))(x)


def row_sum(x):
    x = x + lax.ppermute(x, "row", R1)
    return x + lax.ppermute(x, "row", R2)


def factor_columns(stored):
    local_rows, local_blocks, width = stored.shape
    row_rank = lax.axis_index("row")
    col_rank = lax.axis_index("col")
    row_ids = row_rank * local_rows + jnp.arange(local_rows)
    col_ids = jnp.arange(width)
    edot = functools.partial(jnp.einsum, precision=HI, preferred_element_type=F32)

    def panel_step(panel_idx, state):
        stored, taus, tfs = state
        row_start = panel_idx * width
        local_idx = panel_idx // 2
        is_owner = col_rank == panel_idx % 2
        panel_in = lax.dynamic_slice_in_dim(stored, local_idx, 1, axis=1)[:, 0, :]

        def column_step(col_idx, loop_state):
            work, tau_vec = loop_state
            diag_idx = row_start + col_idx
            column = lax.dynamic_slice_in_dim(work, col_idx, 1, axis=1)[:, 0]
            below = jnp.where(row_ids >= diag_idx, column, 0.0)
            at_diag = (row_ids == diag_idx).astype(F32)
            summed = row_sum(edot("ar,rk->ak", jnp.stack([below, at_diag]), work))
            cross, diag_row = summed[0], summed[1]
            pivot = lax.dynamic_slice_in_dim(diag_row, col_idx, 1)[0]
            norm = jnp.sqrt(lax.dynamic_slice_in_dim(cross, col_idx, 1)[0])
            beta = -jnp.where(pivot >= 0, 1.0, -1.0) * norm
            tau = (beta - pivot) / beta
            denom = pivot - beta
            proj = jnp.where(col_ids > col_idx, (cross - beta * diag_row) / denom, 0.0)
            refl = jnp.where(row_ids > diag_idx, column / denom, 0.0) + at_diag
            work = work - tau * refl[:, None] * proj[None, :]
            new_col = jnp.where(row_ids < diag_idx, column, jnp.where(row_ids == diag_idx, beta, refl))
            work = lax.dynamic_update_slice_in_dim(work, new_col[:, None], col_idx, axis=1)
            return work, lax.dynamic_update_slice_in_dim(tau_vec, tau[None], col_idx, axis=0)

        work, tau_vec = lax.fori_loop(0, width, column_step, (panel_in, jnp.zeros((width,), F32)))
        diag_ids = row_start + col_ids[None, :]
        v_block = jnp.where(row_ids[:, None] == diag_ids, 1.0, jnp.where(row_ids[:, None] > diag_ids, work, 0.0))
        gram = row_sum(edot("ri,rj->ij", v_block, v_block))

        def t_step(col_idx, tf):
            g = lax.dynamic_slice_in_dim(gram, col_idx, 1, axis=1)[:, 0]
            g = jnp.where(col_ids < col_idx, g, 0.0)
            tau_k = lax.dynamic_slice_in_dim(tau_vec, col_idx, 1)[0]
            t_col = -tau_k * edot("ij,j->i", tf, g)
            t_col = jnp.where(col_ids == col_idx, tau_k, t_col)
            return lax.dynamic_update_slice_in_dim(tf, t_col[:, None], col_idx, axis=1)

        tf = lax.fori_loop(0, width, t_step, jnp.zeros((width, width), F32))
        v_mine = jnp.where(is_owner, v_block, 0.0)
        t_mine = jnp.where(is_owner, tf, 0.0)
        v_block = v_mine + lax.ppermute(v_mine, "col", CY)
        tf = t_mine + lax.ppermute(t_mine, "col", CY)

        def block_step(b, stored):
            blk = lax.dynamic_slice_in_dim(stored, b, 1, axis=1)[:, 0, :]
            w = edot("ij,ik->jk", tf, row_sum(edot("ri,rk->ik", v_block, blk)))
            upd = blk - edot("ri,ik->rk", v_block, w)
            keep = b * 2 + col_rank > panel_idx
            mine = (b == local_idx) & is_owner
            new = jnp.where(keep, upd, jnp.where(mine, work, blk))
            return lax.dynamic_update_slice_in_dim(stored, new[:, None, :], b, axis=1)

        stored = lax.fori_loop(0, local_blocks, block_step, stored)
        taus = lax.dynamic_update_slice_in_dim(taus, jnp.diagonal(tf), row_start, axis=0)
        return stored, taus, lax.dynamic_update_slice_in_dim(tfs, tf, row_start, axis=0)

    return lax.fori_loop(0, PANELS, panel_step, (stored, jnp.zeros((PANELS * width,), F32), jnp.zeros((PANELS * width, width), F32)))


def solution(mesh):
    def factor_both(a_matrix, b_matrix):
        local_rows, local_blocks, width = a_matrix.shape
        cols = local_blocks * width
        own = 2 * width
        row_rank = lax.axis_index("row")
        col_rank = lax.axis_index("col")
        core = row_rank % 2
        cts = [m.transpose(1, 2, 0).reshape(cols, local_rows) for m in (a_matrix, b_matrix)]

        pa, pb, c1a, c1b, pam, pao, pbm, g, x1, *first = exchange(*cts, own)
        across = lax.ppermute(pbm, "row", R2)
        ids = jnp.stack([row_rank, core, col_rank]).astype(jnp.int32)
        out_a, bad_a, *second = apply_update(ids, cts[0], pa, pam, pao, c1a, first, jnp.zeros(TILE, F32), (g, x1))
        across, bad_a = lax.optimization_barrier((across, bad_a))
        pbm = pbm + across
        pbo = lax.ppermute(pbm, "row", R1)
        tt = jnp.concatenate([s[i] for s in (first, second) for i in (4, 5)], 0)
        tt = jnp.where(col_rank == 0, tt, lax.ppermute(tt, "col", [(0, 1)]))
        out_b, bad = apply_update(ids, cts[1], pb, pbm, pbo, c1b, second, bad_a)
        bad = bad + lax.ppermute(bad, "col", CY)
        carry = [bad]
        for i, out in enumerate((out_a, out_b)):
            at = i * (N + NP)
            carry += [out, tt[at + N:at + N + NP], tt[at:at + N]]

        def redo(state):
            new = [jnp.zeros(TILE, F32)]
            for m in (a_matrix, b_matrix):
                st, taus, tfs = factor_columns(m)
                new += [st.transpose(1, 2, 0).reshape(cols, local_rows), row_major(taus.reshape(NP, W)), row_major(tfs)]
            return tuple(new)

        res = lax.while_loop(lambda s: s[0][0, 0] > 0.5, redo, tuple(carry))
        back = lambda x: x.reshape(local_blocks, width, local_rows).transpose(2, 0, 1)
        stack = lambda t: t.reshape(PANELS, width, width)
        return back(res[1]), res[2].reshape(N), stack(res[3]), back(res[4]), res[5].reshape(N), stack(res[6])

    spec_mat = P(("batch", "row"), "col", None)
    spec_out = (spec_mat, P("batch"), P("batch", None, None))
    return jax.shard_map(factor_both, mesh=mesh, in_specs=(spec_mat, spec_mat), out_specs=spec_out + spec_out, check_vma=False)
```

```python
import functools

import jax
import jax.numpy as jnp
from jax import lax
from jax.experimental import pallas as pl
from jax.experimental.pallas import tpu as pltpu
from jax.sharding import PartitionSpec as P

F32 = jnp.float32
BF = jnp.bfloat16
HI = lax.Precision.HIGHEST
PANELS = 4
W = 64
NP = 4
N = 256
NN = (((1,), (0,)), ((), ()))
NT = (((1,), (1,)), ((), ()))
TN = (((0,), (0,)), ((), ()))


BOTH = (0, 1)
TILE = (8, 128)


def rows_of(shape):
    return lax.broadcasted_iota(jnp.int32, shape, 0)


def lanes_of(shape):
    return lax.broadcasted_iota(jnp.int32, shape, 1)


def hdot(a, b, dn=NN):
    return lax.dot_general(a, b, dn, precision=HI, preferred_element_type=F32)


GROUP = 4
AMPLIFY = 64.0
HUGE = 1e9


def diag_factor(mats):
    tiles = W // 8
    lane8 = lanes_of(TILE)
    sub8 = rows_of(TILE)
    r64 = rows_of((W, W))
    c64 = lanes_of((W, W))
    eye = (r64 == c64).astype(F32)
    full = lambda x: jnp.broadcast_to(x, TILE)
    zeros = jnp.zeros(TILE, F32)
    st = []
    for hpp, ypp in mats:
        he = jnp.concatenate([hpp, eye], 1)
        yw = jnp.concatenate([ypp, eye], 1)
        st.append(dict(he=[he[8 * g:8 * g + 8] for g in range(tiles)], yw=[yw[8 * g:8 * g + 8] for g in range(tiles)],
                       l=[zeros] * tiles, u=[zeros] * tiles, tau=zeros))
    for k0 in range(0, W, GROUP):
        gk = k0 // 8
        for s in st:
            s['bh'] = [[full(s['he'][g][:, k:k + 1]) for g in range(gk, tiles)] for k in range(k0, k0 + GROUP)]
            s['by'] = [[full(s['yw'][g][:, k:k + 1]) for g in range(tiles)] for k in range(k0, k0 + GROUP)]
        for k in range(k0, k0 + GROUP):
            sk = k - 8 * gk
            isk = sub8 == sk
            for s in st:
                ch, cy = s['bh'][k - k0], s['by'][k - k0]
                pick = lambda x: full(x[sk:sk + 1, :])
                h = pick(ch[0])
                a = pick(cy[gk])
                rs = lax.rsqrt(h)
                rinv = jnp.where(a >= 0, -rs, rs)
                ukk = a - h * rinv
                uinv = 1.0 / ukk
                r = pick(s['he'][gk]) * rinv
                u = pick(s['yw'][gk]) - jnp.where((lane8 >= k) & (lane8 < W), r, 0.0)
                un = u * uinv
                rr = r * rinv
                for k2 in range(k + 1, k0 + GROUP):
                    r2 = pick(s['bh'][k2 - k0][0]) * rinv
                    un2 = (pick(s['by'][k2 - k0][gk]) - r2) * uinv
                    rr2 = r2 * rinv
                    s['bh'][k2 - k0] = [x - ch[i] * rr2 for i, x in enumerate(s['bh'][k2 - k0])]
                    nby = [x - cy[i] * un2 for i, x in enumerate(s['by'][k2 - k0])]
                    nby[gk] = jnp.where(isk, un2, nby[gk])
                    s['by'][k2 - k0] = nby
                for g in range(gk, tiles):
                    new = s['he'][g] - ch[g - gk] * rr
                    lc = cy[g] * uinv
                    if g == gk:
                        new = jnp.where(sub8 > sk, new, jnp.where(isk, r, s['he'][g]))
                        lc = jnp.where(sub8 > sk, lc, 0.0)
                    s['he'][g] = new
                    s['l'][g] = jnp.where(lane8 == k, lc, s['l'][g])
                for g in range(tiles):
                    new = s['yw'][g] - cy[g] * un
                    s['yw'][g] = jnp.where(isk, un, new) if g == gk else new
                s['u'][gk] = jnp.where(isk, u, s['u'][gk])
                s['tau'] = jnp.where(lane8 == k, -ukk * rinv, s['tau'])
    out = []
    up = c64 >= r64
    for s in st:
        he = jnp.concatenate(s['he'], 0)
        yw = jnp.concatenate(s['yw'], 0)
        l = jnp.concatenate(s['l'], 0)[:, :W]
        u = jnp.concatenate(s['u'], 0)[:, :W]
        out.append((jnp.where(c64 <= r64, he[:, W:], 0.0), l + eye, jnp.where(up, u, 0.0), yw[:, W:], s['tau'][0:1, :W]))
    return out


def blk(b):
    return slice(b * W, (b + 1) * W)


def order(c):
    return [2 * l + c for l in BOTH] + [2 * l + 1 - c for l in BOTH]


def turn(x):
    return jnp.concatenate([x[:, W:N], x[:, :W], x[:, N:]], 1)


CHAIN_SCRATCH = [(N, 2 * N), (N, 2 * N), (N, N), (4, W, W), (8, N), (8, W)]
CHAIN_SHAPES = [(N, N), (N, N), (2 * W, N), (2 * W, N), (N, W), (NP, W), TILE]


def chain_init(col, g, x1, st):
    hs, ys, ls, _, norm, _ = st
    ri, ci = rows_of((N, N)), lanes_of((N, N))
    eye = (ri == ci).astype(F32)
    for c in BOTH:
        @pl.when(col == c)
        def _():
            for i, b in enumerate(order(c)):
                ls[blk(b), :] = x1[blk(i), :]
                for i2, b2 in enumerate(order(c)):
                    hs[blk(b), blk(b2)] = g[blk(i), blk(i2)]
    hs[:, N:] = eye
    ys[:, :N] = ls[...].T
    ys[:, N:] = eye
    dg = jnp.where(ri == ci, hs[:, :N], 0.0)
    norm[...] = jnp.broadcast_to(jnp.sqrt(jnp.sum(dg, 0, keepdims=True)), (8, N))


def chain_cols(st):
    hs, ys, _, fac, _, tv = st
    e, l, u, w, tau = diag_factor([(hs[0:W, 0:W], ys[0:W, 0:W])])[0]
    for i, x in enumerate((e, l, u, w)):
        fac[i] = x
    tv[...] = jnp.broadcast_to(tau, (8, W))


def chain_update(p, st, tfac, tau):
    hs, ys, ls, fac, _, tv = st
    r64 = rows_of((W, W))
    c64 = lanes_of((W, W))
    rw = rows_of((W, 2 * N))
    cw = lanes_of((W, 2 * N))
    rl = rows_of((N - W, W))
    live = N - p * W
    e, l, u, w = fac[0], fac[1], fac[2], fac[3]
    d = pl.ds(pl.multiple_of(p * W, W), W)
    rall = hdot(e, hs[0:W, :])
    rall = jnp.where((cw >= N) | ((cw >= rw) & (cw < live)), rall, 0.0)
    ue, uw, wl = hdot(u, e, NT), hdot(u, w), hdot(w, l)
    yield
    yc = ys[W:, 0:W]
    nrow = hdot(w, ys[0:W, :] - jnp.where(cw < N, rall, 0.0))
    hnew = hs[W:, :] - hdot(rall[:, W:N], rall, TN)
    hs[0:N - W, :] = turn(hnew)
    hs[N - W:, :] = turn(rall)
    t = -hdot(ue, uw, NT)
    tfac[d, :] = jnp.where(c64 > r64, t, jnp.where(c64 == r64, jnp.broadcast_to(tv[0:1, :], (W, W)), 0.0))
    tau[pl.ds(p, 1), :] = tv[0:1, :]
    lnew = jnp.where(rl < live - W, hdot(yc, wl), 0.0)
    rest = ls[W:, W:]
    first = ls[0:W, W:]
    ls[0:N - W, N - W:] = lnew
    ls[N - W:, N - W:] = l
    ls[0:N - W, 0:N - W] = rest
    ls[N - W:, 0:N - W] = first
    yield
    ynew = ys[W:, :] - hdot(yc, nrow)
    ys[0:N - W, :] = turn(ynew)
    ys[N - W:, :] = turn(nrow)


def weave(stages, pieces):
    stages = iter(stages)
    for piece in pieces:
        next(stages, None)
        piece()
    for _ in stages:
        pass


def chain_final(col, st, outs):
    hs, ys, ls, _, norm, _ = st
    rinvt, minv, upt, ptt, _, _, bad = outs
    ri = rows_of((N, N))
    ci = lanes_of((N, N))
    rt, mi = hs[:, N:], ys[:, N:]
    g = norm[0:1, :]
    c1 = jnp.max(jnp.sum(jnp.abs(rt) * g, 1, keepdims=True), keepdims=True)
    c2 = jnp.max(hdot(g, jnp.abs(mi)), keepdims=True)
    good = (c1 <= AMPLIFY) & (c2 <= AMPLIFY) & (jnp.min(g, keepdims=True) >= 1 / HUGE) & (jnp.max(g, keepdims=True) <= HUGE)
    bad[...] = jnp.broadcast_to(jnp.where(good, 0.0, 1.0), TILE)
    pt = jnp.where(ri > ci, ls[...], hs[:, :N]).T
    ut = lax.dot_general(ls[...], mi, (((0,), (1,)), ((), ())), precision=HI, preferred_element_type=F32)
    hs[:, :N] = pt
    ys[:, :N] = ut
    for c in BOTH:
        @pl.when(col == c)
        def _():
            for i, b in enumerate(order(c)):
                rinvt[:, blk(i)] = hs[:, N + b * W:N + (b + 1) * W]
                minv[blk(i), :] = ys[blk(b), N:]
            for i in BOTH:
                b = order(c)[i]
                ptt[blk(i), :] = hs[blk(b), :N]
                for i2, b2 in enumerate(order(c)):
                    upt[blk(i), blk(i2)] = ys[blk(b), blk(b2)]


def split3(x):
    h = x.astype(BF)
    r = x - h.astype(F32)
    m = r.astype(BF)
    return h, m, (r - m.astype(F32)).astype(BF)


def dot6(a, b, dn):
    d = lambda i, j: lax.dot_general(a[i], b[j], dn, preferred_element_type=F32)
    return (((d(2, 0) + d(0, 2)) + d(1, 1)) + (d(1, 0) + d(0, 1))) + d(0, 0)


CHUNK = 1024
PIECE = 512
SPAN = 1024
SLOTS = 3
AHEAD = SLOTS - 1


def exchange_kernel(ca, cb, peer_a, peer_b, c1a, c1b, pam, pao, pbm, g_out, x1b, *refs):
    outs, refs = refs[:len(CHAIN_SHAPES)], refs[len(CHAIN_SHAPES):]
    st, refs = refs[:len(CHAIN_SCRATCH)], refs[len(CHAIN_SCRATCH):]
    (x1a, peer, own, xs, cbuf, acc, gacc, r1buf, r2buf, gbuf1, gsum, gbuf2,
     c_sem, own_sem, out_sem, y_send, y_recv, top_send, top_recv, swap_send, swap_recv,
     g_send, g_recv, p_send, p_recv, x_send, x_recv) = refs
    cts, x1 = (ca, cb), (x1a, x1b)
    row = lax.axis_index("row")
    col = lax.axis_index("col")
    core = lax.rem(row, 2)
    mate = row + 1 - 2 * core
    across = lax.rem(row + 2, 4)
    diag = lax.rem(row + 3 - 2 * core, 4)
    cols, rows = ca.shape
    half = cols // 2
    nown = peer.shape[1]
    nchunk = cols // CHUNK
    spans = rows // SPAN
    trips = nchunk * spans

    def remote(src, dst, send, recv, **where):
        return pltpu.make_async_remote_copy(src_ref=src, dst_ref=dst, send_sem=send, recv_sem=recv,
                                            device_id=where, device_id_type=pl.DeviceIdType.MESH)

    to_mate = functools.partial(remote, row=mate)
    to_across = functools.partial(remote, row=across)

    def c_copy(m, t):
        slot = lax.rem(m * trips + t, SLOTS)
        h, j = lax.div(t, nchunk), lax.rem(t, nchunk)
        return pltpu.make_async_copy(
            cts[m].at[pl.ds(pl.multiple_of(j * CHUNK, CHUNK), CHUNK), pl.ds(pl.multiple_of(h * SPAN, SPAN), SPAN)],
            cbuf.at[slot], c_sem.at[slot])

    first = pl.ds(0, nown)
    second = pl.ds(nown, nown)
    lanes = pl.ds(0, N)

    def y_copy(m, h):
        s = pl.ds(pl.multiple_of(h * SPAN, SPAN), SPAN)
        i = m * spans + h
        return remote(cts[m].at[first, s], peer.at[m, :, s], y_send.at[i], y_recv.at[i], col=1 - col)

    own_copies = [pltpu.make_async_copy(cts[m].at[first, :], own.at[m], own_sem.at[m]) for m in BOTH]
    for o in own_copies:
        o.start()
    for t in range(AHEAD):
        c_copy(0, t).start()

    barrier = pltpu.get_barrier_semaphore()
    for where in (dict(row=mate), dict(row=across), dict(row=diag), dict(col=1 - col)):
        pl.semaphore_signal(barrier, device_id=where, device_id_type=pl.DeviceIdType.MESH)
    pl.semaphore_wait(barrier, 4)

    for m in BOTH:
        for h in range(spans):
            y_copy(m, h).start()

    tops = (c1a, c1b)
    lows = [pl.ds(0, half), pl.ds(half, half)]
    x_local = [pltpu.make_async_copy(cts[m].at[first, lanes], x1[m].at[first, :], own_sem.at[2 + m]) for m in BOTH]
    x_own = [[remote(cts[m].at[first, lanes], x1[m].at[first, :], top_send.at[m, k], top_recv.at[m], row=k + 1)
              for k in range(3)] for m in BOTH]
    x_peer = [[remote(peer.at[m, :, lanes], x1[m].at[second, :], top_send.at[2 + m, k], top_recv.at[2 + m], row=k + 1)
               for k in range(3)] for m in BOTH]
    top_far = [[remote(cts[m].at[:, lanes], tops[m], top_send.at[4 + m, 0], top_recv.at[4 + m], row=1)]
               + [remote(cts[m].at[lows[k], lanes], tops[m].at[lows[k], :], top_send.at[4 + m, 1 + k], top_recv.at[4 + m], row=2 + k)
                  for k in BOTH] for m in BOTH]

    @pl.when(row == 0)
    def _():
        for m in BOTH:
            x_local[m].start()
        for c in x_own[0] + x_own[1] + top_far[0] + top_far[1]:
            c.start()

    mine = pl.ds(pl.multiple_of(core * half, half), half)
    others = pl.ds(pl.multiple_of((1 - core) * half, half), half)
    p1 = [to_mate(acc.at[m, others, :], r1buf.at[m], p_send.at[m], p_recv.at[m]) for m in BOTH]
    g1 = [to_mate(gacc.at[m], gbuf1.at[m], g_send.at[m], g_recv.at[m]) for m in BOTH]
    g2 = [to_across(gsum.at[m], gbuf2.at[m], g_send.at[2 + m], g_recv.at[2 + m]) for m in BOTH]
    p2 = to_across(r1buf.at[0], r2buf, x_send.at[0], x_recv.at[0])
    p3 = to_mate(r1buf.at[0], pao, x_send.at[1], x_recv.at[1])
    swap = [to_mate(tops[m].at[mine, :], tops[m].at[mine, :], swap_send.at[m], swap_recv.at[m]) for m in BOTH]
    peer_out = [pltpu.make_async_copy(peer.at[m], (peer_a, peer_b)[m], out_sem.at[m]) for m in BOTH]
    pam_out = pltpu.make_async_copy(r1buf.at[0], pam, out_sem.at[2])
    pbm_out = pltpu.make_async_copy(r1buf.at[1], pbm, out_sem.at[3])

    def add_half(m):
        p1[m].wait()
        r1buf[m] = r1buf[m] + acc[m, mine, :]

    def finish_g1(m):
        g1[m].wait()
        gsum[m] = gacc[m] + gbuf1[m]
        g2[m].start()

    def send_x(m):
        @pl.when(row == 0)
        def _():
            x1[m][nown:, :] = peer[m, :, 0:N]
            for c in x_peer[m]:
                c.start()

    def wait_x(m):
        @pl.when(row == 0)
        def _():
            x_local[m].wait()

        @pl.when(row > 0)
        def _():
            x_own[m][0].wait_recv()
            x_peer[m][0].wait_recv()

    def begin_chain():
        wait_x(0)
        g2[0].wait()
        gsum[0] = gsum[0] + gbuf2[0]
        chain_init(col, gsum.at[0], x1a, st)

    def top_rows():
        @pl.when(row == 1)
        def _():
            for m in BOTH:
                top_far[m][0].wait_recv()

        @pl.when(row >= 2)
        def _():
            for m in BOTH:
                top_far[m][1].wait_recv()
                swap[m].start()

    def last_sums_a():
        p2.wait()
        r1buf[0] = r1buf[0] + r2buf[...]
        p3.start()
        pam_out.start()

    last = trips - nchunk
    begin = 1
    hooks = [[(0, lambda: send_x(0)), (last, lambda: finish_g1(0))],
             [(begin - 1, begin_chain), (begin, lambda: send_x(1)), (last - 1, last_sums_a), (last - 1, top_rows),
              (last, lambda: finish_g1(1))]]

    def products(m):
        def span(h, _):
            y_copy(m, h).wait_recv()
            s0 = pl.multiple_of(h * SPAN, SPAN)

            def build(q, _):
                d = pl.ds(pl.multiple_of(q * 512, 512), 512)
                s = pl.ds(pl.multiple_of(s0 + q * 512, 512), 512)
                for i, part in enumerate(split3(own[m, :, s])):
                    xs[i, 0:nown, d] = part
                for i, part in enumerate(split3(peer[m, :, s])):
                    xs[i, nown:, d] = part
                return 0

            lax.fori_loop(0, SPAN // 512, build, 0)
            x = (xs[0], xs[1], xs[2])
            r = dot6(x, x, NT)
            gacc[m] = jnp.where(h == 0, r, gacc[m] + r)

            @pl.when(h == spans - 1)
            def _():
                g1[m].start()

            def trip(j, _):
                t = h * nchunk + j
                slot = lax.rem(m * trips + t, SLOTS)
                c_copy(m, t).wait()

                @pl.when(t + AHEAD < trips)
                def _():
                    c_copy(m, t + AHEAD).start()

                if m == 0:
                    @pl.when(t + AHEAD >= trips)
                    def _():
                        c_copy(1, t + AHEAD - trips).start()

                def piece(i):
                    r = dot6(split3(cbuf[slot, i * PIECE:(i + 1) * PIECE, :]), (xs[0], xs[1], xs[2]), NT)
                    d = pl.ds(pl.multiple_of(j * CHUNK + i * PIECE, PIECE), PIECE)
                    acc[m, d, :] = jnp.where(h == 0, r, acc[m, d, :] + r)

                def core_trip():
                    for i in range(CHUNK // PIECE):
                        piece(i)

                if m == 0:
                    core_trip()
                else:
                    live = (t >= begin) & (t < begin + NP)

                    @pl.when(live)
                    def _():
                        chain_cols(st)
                        core_trip()
                        weave(chain_update(t - begin, st, outs[4], outs[5]), [])

                    pl.when(~live)(core_trip)
                for at, hook in hooks[m]:
                    pl.when(t == at)(hook)
                return 0

            lax.fori_loop(0, nchunk, trip, 0)
            return 0

        own_copies[m].wait()
        lax.fori_loop(0, spans, span, 0)

    products(0)
    p1[0].start()
    peer_out[0].start()
    add_half(0)
    p2.start()
    products(1)
    p1[1].start()
    peer_out[1].start()
    wait_x(1)
    chain_final(col, st, outs)
    add_half(1)
    pbm_out.start()
    g2[1].wait()
    g_out[...] = gsum[1] + gbuf2[1]

    @pl.when(row == 0)
    def _():
        for c in x_own[0] + x_own[1] + x_peer[0] + x_peer[1] + top_far[0] + top_far[1]:
            c.wait_send()

    @pl.when(row >= 2)
    def _():
        for m in BOTH:
            swap[m].wait()

    for c in peer_out + [p3, pam_out, pbm_out]:
        c.wait()
    for m in BOTH:
        for h in range(spans):
            y_copy(m, h).wait_send()


def exchange(ca, cb, own):
    cols, rows = ca.shape
    half = cols // 2
    hbm = pl.BlockSpec(memory_space=pl.ANY)
    vm = pl.BlockSpec(memory_space=pltpu.VMEM)
    dma = pltpu.SemaphoreType.DMA
    pair = (2, N, N)
    ny = 2 * rows // SPAN
    shapes = [(own, rows)] * 2 + [(cols, N)] * 2 + [(half, N)] * 3 + [(N, N), (N, N)] + CHAIN_SHAPES
    scratch = CHAIN_SCRATCH + [(N, N), (2, own, rows), (2, own, rows)]
    after = [(SLOTS, CHUNK, SPAN), (2, cols, N), pair, (2, half, N), (half, N)] + [pair] * 3
    return pl.pallas_call(
        exchange_kernel,
        in_specs=[hbm, hbm],
        out_specs=[hbm] * 7 + [vm] * (2 + len(CHAIN_SHAPES)),
        out_shape=[jax.ShapeDtypeStruct(s, F32) for s in shapes],
        scratch_shapes=[pltpu.VMEM(s, F32) for s in scratch] + [pltpu.VMEM((3, 2 * own, SPAN), BF)]
        + [pltpu.VMEM(s, F32) for s in after]
        + [dma(n) for n in ((SLOTS,), (4,), (4,), (ny,), (ny,), (6, 3), (6,), (2,), (2,), (4,), (4,), (2,), (2,), (2,), (2,))],
        cost_estimate=pl.CostEstimate(flops=24 * cols * rows * N, bytes_accessed=8 * cols * rows, transcendentals=0),
        compiler_params=pltpu.CompilerParams(vmem_limit_bytes=60 * 2**20, collective_id=0, has_side_effects=True))(ca, cb)


def apply_update(ct, peer, psum, poth, c1, small, before, nxt=None, past=()):
    cols, rows = ct.shape
    nb = 512
    mb = 512
    own = peer.shape[0]
    half = cols // 2
    steps = rows // nb
    rinvt, minv, upt, ptt, _, _, bad = small
    no = len(CHAIN_SHAPES)
    extra = list(nxt or ()) + list(past)
    ne = len(extra)

    def body(c_ref, x_ref, p_ref, q_ref, c1_ref, r_ref, m_ref, up_ref, pt_ref, bad_ref, before_ref, *refs):
        ins, (o_ref, f_ref) = refs[:ne], refs[ne:ne + 2]
        outs, (z_ref, rc_ref, *st) = refs[ne + 2:len(refs) - ns], refs[len(refs) - ns:]
        i = pl.program_id(0)
        row = lax.axis_index("row")
        top = row == 0

        @pl.when(i == 0)
        def _():
            zero = jnp.zeros((1, 1), F32)
            for src, which in ((p_ref, 0), (q_ref, 1)):
                base = pl.multiple_of((lax.rem(row, 2) ^ which) * half, half)
                for j in range(half // mb):
                    s = slice(j * mb, (j + 1) * mb)
                    d = pl.ds(base + j * mb, mb)
                    rc = hdot(src[s, :], r_ref[...], NT)
                    z = hdot(jnp.where(top, c_ref[d, 0:N], c1_ref[d, :]) - rc, m_ref[...], NT)
                    rc_ref[d, :] = rc
                    z_ref[d, :] = z
                    zero = zero + jnp.sum(jnp.sum(z * 0.0, 0, keepdims=True), 1, keepdims=True)
            f_ref[...] = jnp.where(zero == 0.0, 0.0, 1.0) + bad_ref[...] + before_ref[...]
            if nxt is not None:
                chain_init(lax.axis_index("col"), *ins[:2], st)
                outs[4][0:N, :] = ins[2][...]
                outs[4][2 * N:2 * N + NP, :] = ins[3][...]

        def piece(j):
            x = jnp.concatenate([c_ref[0:own, :], x_ref[...]], 0)
            lo = own if j == 0 else j * mb
            if j == 0:
                o_ref[0:own, :] = hdot(up_ref[...], x)
            s = slice(lo, (j + 1) * mb)
            o_ref[s, :] = c_ref[s, :] - hdot(z_ref[s, :], x)

        pieces = [functools.partial(piece, j) for j in range(cols // mb)]
        if nxt is None:
            weave([], pieces)
        else:
            @pl.when(lax.rem(i, 2) == 0)
            def _():
                chain_cols(st)
                weave([], pieces)

            @pl.when(lax.rem(i, 2) == 1)
            def _():
                weave(chain_update(lax.div(i, 2), st, outs[4].at[pl.ds(N, N), :], outs[4].at[pl.ds(2 * N + NP, NP), :]), pieces)

            @pl.when(i == steps - 1)
            def _():
                chain_final(lax.axis_index("col"), st, outs)

        @pl.when((i == 0) & top)
        def _():
            o_ref[0:own, 0:N] = pt_ref[...]
            o_ref[own:, 0:N] = rc_ref[own:, :]

    blk2 = pl.BlockSpec((cols, nb), lambda i: (0, i))
    fixed = lambda shape: pl.BlockSpec(shape, lambda i: (0, 0))
    consts = [psum, poth, c1, rinvt, minv, upt, ptt, bad, before] + extra
    more = CHAIN_SHAPES[:4] + [(2 * (N + NP), W)] + CHAIN_SHAPES[5:] if nxt is not None else []
    scratch = [(cols, N), (cols, N)] + (CHAIN_SCRATCH if nxt is not None else [])
    ns = len(scratch)
    return pl.pallas_call(
        body, grid=(steps,),
        in_specs=[blk2, pl.BlockSpec((own, nb), lambda i: (0, i))] + [fixed(a.shape) for a in consts],
        out_specs=[blk2, fixed(TILE)] + [fixed(s) for s in more],
        scratch_shapes=[pltpu.VMEM(s, F32) for s in scratch],
        out_shape=[jax.ShapeDtypeStruct(s, F32) for s in [(cols, rows), TILE] + more],
        cost_estimate=pl.CostEstimate(flops=12 * cols * rows * N, bytes_accessed=8 * cols * rows, transcendentals=0),
        compiler_params=pltpu.CompilerParams(vmem_limit_bytes=60 * 2**20))(ct, peer, *consts)


R1 = [(0, 1), (1, 0), (2, 3), (3, 2)]
R2 = [(0, 2), (2, 0), (1, 3), (3, 1)]
CY = [(0, 1), (1, 0)]


def row_major(x):
    def body(i_ref, o_ref):
        o_ref[...] = i_ref[...]

    return pl.pallas_call(body, out_shape=jax.ShapeDtypeStruct(x.shape, F32))(x)


def row_sum(x):
    x = x + lax.ppermute(x, "row", R1)
    return x + lax.ppermute(x, "row", R2)


def factor_columns(stored):
    local_rows, local_blocks, width = stored.shape
    row_rank = lax.axis_index("row")
    col_rank = lax.axis_index("col")
    row_ids = row_rank * local_rows + jnp.arange(local_rows)
    col_ids = jnp.arange(width)
    edot = functools.partial(jnp.einsum, precision=HI, preferred_element_type=F32)

    def panel_step(panel_idx, state):
        stored, taus, tfs = state
        row_start = panel_idx * width
        local_idx = panel_idx // 2
        is_owner = col_rank == panel_idx % 2
        panel_in = lax.dynamic_slice_in_dim(stored, local_idx, 1, axis=1)[:, 0, :]

        def column_step(col_idx, loop_state):
            work, tau_vec = loop_state
            diag_idx = row_start + col_idx
            column = lax.dynamic_slice_in_dim(work, col_idx, 1, axis=1)[:, 0]
            below = jnp.where(row_ids >= diag_idx, column, 0.0)
            at_diag = (row_ids == diag_idx).astype(F32)
            summed = row_sum(edot("ar,rk->ak", jnp.stack([below, at_diag]), work))
            cross, diag_row = summed[0], summed[1]
            pivot = lax.dynamic_slice_in_dim(diag_row, col_idx, 1)[0]
            norm = jnp.sqrt(lax.dynamic_slice_in_dim(cross, col_idx, 1)[0])
            beta = -jnp.where(pivot >= 0, 1.0, -1.0) * norm
            tau = (beta - pivot) / beta
            denom = pivot - beta
            proj = jnp.where(col_ids > col_idx, (cross - beta * diag_row) / denom, 0.0)
            refl = jnp.where(row_ids > diag_idx, column / denom, 0.0) + at_diag
            work = work - tau * refl[:, None] * proj[None, :]
            new_col = jnp.where(row_ids < diag_idx, column, jnp.where(row_ids == diag_idx, beta, refl))
            work = lax.dynamic_update_slice_in_dim(work, new_col[:, None], col_idx, axis=1)
            return work, lax.dynamic_update_slice_in_dim(tau_vec, tau[None], col_idx, axis=0)

        work, tau_vec = lax.fori_loop(0, width, column_step, (panel_in, jnp.zeros((width,), F32)))
        diag_ids = row_start + col_ids[None, :]
        v_block = jnp.where(row_ids[:, None] == diag_ids, 1.0, jnp.where(row_ids[:, None] > diag_ids, work, 0.0))
        gram = row_sum(edot("ri,rj->ij", v_block, v_block))

        def t_step(col_idx, tf):
            g = lax.dynamic_slice_in_dim(gram, col_idx, 1, axis=1)[:, 0]
            g = jnp.where(col_ids < col_idx, g, 0.0)
            tau_k = lax.dynamic_slice_in_dim(tau_vec, col_idx, 1)[0]
            t_col = -tau_k * edot("ij,j->i", tf, g)
            t_col = jnp.where(col_ids == col_idx, tau_k, t_col)
            return lax.dynamic_update_slice_in_dim(tf, t_col[:, None], col_idx, axis=1)

        tf = lax.fori_loop(0, width, t_step, jnp.zeros((width, width), F32))
        v_mine = jnp.where(is_owner, v_block, 0.0)
        t_mine = jnp.where(is_owner, tf, 0.0)
        v_block = v_mine + lax.ppermute(v_mine, "col", CY)
        tf = t_mine + lax.ppermute(t_mine, "col", CY)

        def block_step(b, stored):
            blk = lax.dynamic_slice_in_dim(stored, b, 1, axis=1)[:, 0, :]
            w = edot("ij,ik->jk", tf, row_sum(edot("ri,rk->ik", v_block, blk)))
            upd = blk - edot("ri,ik->rk", v_block, w)
            keep = b * 2 + col_rank > panel_idx
            mine = (b == local_idx) & is_owner
            new = jnp.where(keep, upd, jnp.where(mine, work, blk))
            return lax.dynamic_update_slice_in_dim(stored, new[:, None, :], b, axis=1)

        stored = lax.fori_loop(0, local_blocks, block_step, stored)
        taus = lax.dynamic_update_slice_in_dim(taus, jnp.diagonal(tf), row_start, axis=0)
        return stored, taus, lax.dynamic_update_slice_in_dim(tfs, tf, row_start, axis=0)

    return lax.fori_loop(0, PANELS, panel_step, (stored, jnp.zeros((PANELS * width,), F32), jnp.zeros((PANELS * width, width), F32)))


def solution(mesh):
    def factor_both(a_matrix, b_matrix):
        local_rows, local_blocks, width = a_matrix.shape
        cols = local_blocks * width
        own = 2 * width
        col_rank = lax.axis_index("col")
        cts = [m.transpose(1, 2, 0).reshape(cols, local_rows) for m in (a_matrix, b_matrix)]

        pa, pb, c1a, c1b, pam, pao, pbm, g, x1, *first = exchange(*cts, own)
        across = lax.ppermute(pbm, "row", R2)
        out_a, bad_a, *second = apply_update(cts[0], pa, pam, pao, c1a, first, first[6], (g, x1), (first[4], first[5]))
        across, bad_a = lax.optimization_barrier((across, bad_a))
        pbm = pbm + across
        pbo = lax.ppermute(pbm, "row", R1)
        small = lax.ppermute(second[4], "col", [(0, 1)])
        out_b, bad = apply_update(cts[1], pb, pbm, pbo, c1b, second, bad_a)
        small, bad = lax.optimization_barrier((small, bad))
        small = jnp.where(col_rank == 0, second[4], small)
        carry = (bad, lax.ppermute(bad, "col", CY), small, out_a, out_b)

        def redo(state):
            def one(i, done):
                st, taus, tfs = factor_columns(jnp.where(i == 0, a_matrix, b_matrix))
                new = (st.transpose(1, 2, 0).reshape(cols, local_rows), jnp.concatenate([tfs, taus.reshape(PANELS, width)], 0))
                return tuple(jnp.where(i == k, n, d) for k, pair in enumerate((done[:2], done[2:])) for n, d in zip(new, pair))

            blank = jnp.zeros((N + PANELS, width), F32)
            st_a, tt_a, st_b, tt_b = lax.fori_loop(0, 2, one, (state[3], blank, state[4], blank))
            tt = row_major(jnp.concatenate([tt_a[:N], tt_b[:N], tt_a[N:], tt_b[N:]], 0))
            return jnp.zeros(TILE, F32), jnp.zeros(TILE, F32), tt, st_a, st_b

        _, _, tt, out_a, out_b = lax.while_loop(lambda s: jnp.max(s[0] + s[1]) > 0.5, redo, carry)
        back = lambda x: x.reshape(local_blocks, width, local_rows).transpose(2, 0, 1)
        tail = []
        for i, out in enumerate((out_a, out_b)):
            at = 2 * N + i * PANELS
            tail += [back(out), tt[at:at + PANELS].reshape(N), tt[i * N:(i + 1) * N].reshape(PANELS, width, width)]
        return tuple(tail)

    spec_mat = P(("batch", "row"), "col", None)
    spec_out = (spec_mat, P("batch"), P("batch", None, None))
    return jax.shard_map(factor_both, mesh=mesh, in_specs=(spec_mat, spec_mat), out_specs=spec_out + spec_out, check_vma=False)
```

```python
import functools

import jax
import jax.numpy as jnp
from jax import lax
from jax.experimental import pallas as pl
from jax.experimental.pallas import tpu as pltpu
from jax.sharding import PartitionSpec as P

F32 = jnp.float32
BF = jnp.bfloat16
HI = lax.Precision.HIGHEST
PANELS = 4
W = 64
NP = 4
N = 256
NN = (((1,), (0,)), ((), ()))
NT = (((1,), (1,)), ((), ()))
TN = (((0,), (0,)), ((), ()))


BOTH = (0, 1)
total = functools.partial(jnp.sum, keepdims=True)
peak = functools.partial(jnp.max, keepdims=True)
TILE = (8, 128)


def rows_of(shape):
    return lax.broadcasted_iota(jnp.int32, shape, 0)


def lanes_of(shape):
    return lax.broadcasted_iota(jnp.int32, shape, 1)


def hdot(a, b, dn=NN):
    return lax.dot_general(a, b, dn, precision=HI, preferred_element_type=F32)


GROUP = 4
AMPLIFY = 64.0
HUGE = 1e9


def diag_factor(mats):
    tiles = W // 8
    lane8 = lanes_of(TILE)
    sub8 = rows_of(TILE)
    r64 = rows_of((W, W))
    c64 = lanes_of((W, W))
    eye = (r64 == c64).astype(F32)
    full = lambda x: jnp.broadcast_to(x, TILE)
    zeros = jnp.zeros(TILE, F32)
    st = []
    for hpp, ypp in mats:
        he = jnp.concatenate([hpp, eye], 1)
        yw = jnp.concatenate([ypp, eye], 1)
        st.append(dict(he=[he[8 * g:8 * g + 8] for g in range(tiles)], yw=[yw[8 * g:8 * g + 8] for g in range(tiles)],
                       l=[zeros] * tiles, u=[zeros] * tiles, tau=zeros))
    for k0 in range(0, W, GROUP):
        gk = k0 // 8
        for s in st:
            s['bh'] = [[full(s['he'][g][:, k:k + 1]) for g in range(gk, tiles)] for k in range(k0, k0 + GROUP)]
            s['by'] = [[full(s['yw'][g][:, k:k + 1]) for g in range(tiles)] for k in range(k0, k0 + GROUP)]
        for k in range(k0, k0 + GROUP):
            sk = k - 8 * gk
            isk = sub8 == sk
            for s in st:
                ch, cy = s['bh'][k - k0], s['by'][k - k0]
                pick = lambda x: full(x[sk:sk + 1, :])
                h = pick(ch[0])
                a = pick(cy[gk])
                rs = lax.rsqrt(h)
                rinv = jnp.where(a >= 0, -rs, rs)
                ukk = a - h * rinv
                uinv = 1.0 / ukk
                r = pick(s['he'][gk]) * rinv
                u = pick(s['yw'][gk]) - jnp.where((lane8 >= k) & (lane8 < W), r, 0.0)
                un = u * uinv
                rr = r * rinv
                for k2 in range(k + 1, k0 + GROUP):
                    r2 = pick(s['bh'][k2 - k0][0]) * rinv
                    un2 = (pick(s['by'][k2 - k0][gk]) - r2) * uinv
                    rr2 = r2 * rinv
                    s['bh'][k2 - k0] = [x - ch[i] * rr2 for i, x in enumerate(s['bh'][k2 - k0])]
                    nby = [x - cy[i] * un2 for i, x in enumerate(s['by'][k2 - k0])]
                    nby[gk] = jnp.where(isk, un2, nby[gk])
                    s['by'][k2 - k0] = nby
                for g in range(gk, tiles):
                    new = s['he'][g] - ch[g - gk] * rr
                    lc = cy[g] * uinv
                    if g == gk:
                        new = jnp.where(sub8 > sk, new, jnp.where(isk, r, s['he'][g]))
                        lc = jnp.where(sub8 > sk, lc, 0.0)
                    s['he'][g] = new
                    s['l'][g] = jnp.where(lane8 == k, lc, s['l'][g])
                for g in range(tiles):
                    new = s['yw'][g] - cy[g] * un
                    s['yw'][g] = jnp.where(isk, un, new) if g == gk else new
                s['u'][gk] = jnp.where(isk, u, s['u'][gk])
                s['tau'] = jnp.where(lane8 == k, -ukk * rinv, s['tau'])
    out = []
    up = c64 >= r64
    for s in st:
        he = jnp.concatenate(s['he'], 0)
        yw = jnp.concatenate(s['yw'], 0)
        l = jnp.concatenate(s['l'], 0)[:, :W]
        u = jnp.concatenate(s['u'], 0)[:, :W]
        out.append((jnp.where(c64 <= r64, he[:, W:], 0.0), l + eye, jnp.where(up, u, 0.0), yw[:, W:], s['tau'][0:1, :W]))
    return out


def blk(b):
    return slice(b * W, (b + 1) * W)


def order(c):
    return [2 * l + c for l in BOTH] + [2 * l + 1 - c for l in BOTH]


def turn(x):
    return jnp.concatenate([x[:, W:N], x[:, :W], x[:, N:]], 1)


CHAIN_SCRATCH = [(N, 2 * N), (N, 2 * N), (N, N), (NP, 4, W, W), (8, N), (NP, W)]
CHAIN_SHAPES = [(N, N), (N, N), (2 * W, N), (2 * W, N), (N, W), (NP, W), TILE]


def chain_init(col, g, x1, st):
    hs, ys, ls, _, norm, _ = st
    ri, ci = rows_of((N, N)), lanes_of((N, N))
    eye = (ri == ci).astype(F32)
    for c in BOTH:
        @pl.when(col == c)
        def _():
            for i, b in enumerate(order(c)):
                ls[blk(b), :] = x1[blk(i), :]
                for i2, b2 in enumerate(order(c)):
                    hs[blk(b), blk(b2)] = g[blk(i), blk(i2)]
    hs[:, N:] = eye
    ys[:, :N] = ls[...].T
    ys[:, N:] = eye
    dg = jnp.where(ri == ci, hs[:, :N], 0.0)
    norm[...] = jnp.broadcast_to(jnp.sqrt(total(dg, 0)), (8, N))


def chain_cols(p, st):
    hs, ys, _, fac, _, tv = st
    e, l, u, w, tau = diag_factor([(hs[0:W, 0:W], ys[0:W, 0:W])])[0]
    for i, x in enumerate((e, l, u, w)):
        fac[p, i] = x
    tv[pl.ds(p, 1), :] = tau


def chain_update(p, st):
    hs, ys, ls, fac, _, _ = st
    rw = rows_of((W, 2 * N))
    cw = lanes_of((W, 2 * N))
    rl = rows_of((N - W, W))
    live = N - p * W
    e, l, w = fac[p, 0], fac[p, 1], fac[p, 3]
    rall = hdot(e, hs[0:W, :])
    rall = jnp.where((cw >= N) | ((cw >= rw) & (cw < live)), rall, 0.0)
    wl = hdot(w, l)
    yield
    yc = ys[W:, 0:W]
    nrow = hdot(w, ys[0:W, :] - jnp.where(cw < N, rall, 0.0))
    hnew = hs[W:, :] - hdot(rall[:, W:N], rall, TN)
    hs[0:N - W, :] = turn(hnew)
    hs[N - W:, :] = turn(rall)
    lnew = jnp.where(rl < live - W, hdot(yc, wl), 0.0)
    rest = ls[W:, W:]
    first = ls[0:W, W:]
    ls[0:N - W, N - W:] = lnew
    ls[N - W:, N - W:] = l
    ls[0:N - W, 0:N - W] = rest
    ls[N - W:, 0:N - W] = first
    yield
    ynew = ys[W:, :] - hdot(yc, nrow)
    ys[0:N - W, :] = turn(ynew)
    ys[N - W:, :] = turn(nrow)


def weave(stages, pieces):
    stages = iter(stages)
    for piece in pieces:
        next(stages, None)
        piece()
    for _ in stages:
        pass


def chain_final(col, st, outs):
    hs, ys, ls, fac, norm, tv = st
    rinvt, minv, upt, ptt, tfac, tau, bad = outs
    r64 = rows_of((W, W))
    c64 = lanes_of((W, W))
    tau[...] = tv[...]
    for p in range(NP):
        e, _, u, w = [fac[p, i] for i in range(4)]
        t = -hdot(hdot(u, e, NT), hdot(u, w), NT)
        tfac[blk(p), :] = jnp.where(c64 > r64, t, jnp.where(c64 == r64, jnp.broadcast_to(tv[p:p + 1, :], (W, W)), 0.0))
    ri = rows_of((N, N))
    ci = lanes_of((N, N))
    rt, mi = hs[:, N:], ys[:, N:]
    g = norm[0:1, :]
    c1 = peak(total(jnp.abs(rt) * g, 1))
    c2 = peak(hdot(g, jnp.abs(mi)))
    good = (c1 <= AMPLIFY) & (c2 <= AMPLIFY) & (-peak(-g) >= 1 / HUGE) & (peak(g) <= HUGE)
    bad[...] = jnp.broadcast_to(jnp.where(good, 0.0, 1.0), TILE)
    pt = jnp.where(ri > ci, ls[...], hs[:, :N]).T
    ut = lax.dot_general(ls[...], mi, (((0,), (1,)), ((), ())), precision=HI, preferred_element_type=F32)
    hs[:, :N] = pt
    ys[:, :N] = ut
    for c in BOTH:
        @pl.when(col == c)
        def _():
            for i, b in enumerate(order(c)):
                rinvt[:, blk(i)] = hs[:, N + b * W:N + (b + 1) * W]
                minv[blk(i), :] = ys[blk(b), N:]
            for i in BOTH:
                b = order(c)[i]
                ptt[blk(i), :] = hs[blk(b), :N]
                for i2, b2 in enumerate(order(c)):
                    upt[blk(i), blk(i2)] = ys[blk(b), blk(b2)]


SPLITS = range(3)
loop = functools.partial(lax.fori_loop, 0)


def split3(x):
    h = x.astype(BF)
    r = x - h.astype(F32)
    m = r.astype(BF)
    return h, m, (r - m.astype(F32)).astype(BF)


def dot6(a, b, dn):
    d = lambda i, j: lax.dot_general(a[i], b[j], dn, preferred_element_type=F32)
    return (((d(2, 0) + d(0, 2)) + d(1, 1)) + (d(1, 0) + d(0, 1))) + d(0, 0)


CHUNK = 960
PIECE = 480
HALF = 512
SPAN = 1024
SLOTS = 3
AHEAD = SLOTS - 1


def exchange_kernel(ca, cb, peer_a, peer_b, c1a, c1b, pam, pao, pbm, g_out, x1b, *refs):
    outs, refs = refs[:len(CHAIN_SHAPES)], refs[len(CHAIN_SHAPES):]
    st, refs = refs[:len(CHAIN_SCRATCH)], refs[len(CHAIN_SCRATCH):]
    (x1a, peer, own, xo, xs, cbuf, acc, gacc, r1buf, r2buf, gbuf1, gsum, gbuf2, gfull,
     c_sem, own_sem, out_sem, y_send, y_recv, top_send, top_recv, swap_send, swap_recv,
     g_send, g_recv, p_send, p_recv, x_send, x_recv) = refs
    cts, x1 = (ca, cb), (x1a, x1b)
    row = lax.axis_index("row")
    col = lax.axis_index("col")
    core = lax.rem(row, 2)
    mate = row + 1 - 2 * core
    across = lax.rem(row + 2, 4)
    diag = lax.rem(row + 3 - 2 * core, 4)
    cols, rows = ca.shape
    half = cols // 2
    nown = peer.shape[1]
    nchunk = (cols - nown) // CHUNK
    spans = rows // SPAN
    trips = nchunk * spans

    def remote(src, dst, send, recv, **where):
        return pltpu.make_async_remote_copy(src_ref=src, dst_ref=dst, send_sem=send, recv_sem=recv,
                                            device_id=where, device_id_type=pl.DeviceIdType.MESH)

    to_mate = functools.partial(remote, row=mate)
    to_across = functools.partial(remote, row=across)

    def c_copy(m, t):
        slot = lax.rem(m * trips + t, SLOTS)
        h, j = lax.div(t, nchunk), lax.rem(t, nchunk)
        return pltpu.make_async_copy(
            cts[m].at[pl.ds(pl.multiple_of(nown + j * CHUNK, 64), CHUNK), pl.ds(pl.multiple_of(h * SPAN, SPAN), SPAN)],
            cbuf.at[slot], c_sem.at[slot])

    first = pl.ds(0, nown)
    second = pl.ds(nown, nown)
    lanes = pl.ds(0, N)

    def y_copy(m, h):
        s = pl.ds(pl.multiple_of(h * SPAN, SPAN), SPAN)
        i = m * spans + h
        return remote(cts[m].at[first, s], peer.at[m, :, s], y_send.at[i], y_recv.at[i], col=1 - col)

    def half_slot(u):
        return lax.rem(2 * trips - nchunk + u, SLOTS)

    def c_half(u):
        q, j = lax.div(u, nchunk), lax.rem(u, nchunk)
        return pltpu.make_async_copy(
            cb.at[pl.ds(pl.multiple_of(nown + j * CHUNK, 64), CHUNK), pl.ds(pl.multiple_of(rows - SPAN + q * HALF, HALF), HALF)],
            cbuf.at[half_slot(u), :, pl.ds(0, HALF)], c_sem.at[half_slot(u)])

    def y_half(q):
        s = pl.ds(pl.multiple_of(rows - SPAN + q * HALF, HALF), HALF)
        i = 2 * spans - 1 + q
        return remote(cb.at[first, s], peer.at[1, :, s], y_send.at[i], y_recv.at[i], col=1 - col)

    own_copies = [pltpu.make_async_copy(cts[m].at[first, :], own.at[m], own_sem.at[m]) for m in BOTH]
    for o in own_copies:
        o.start()
    for t in range(AHEAD):
        c_copy(0, t).start()

    for m in BOTH:
        acc[m, 0:nown, :] = jnp.zeros((nown, N), F32)
    barrier = pltpu.get_barrier_semaphore()
    for where in (dict(row=mate), dict(row=across), dict(row=diag), dict(col=1 - col)):
        pl.semaphore_signal(barrier, device_id=where, device_id_type=pl.DeviceIdType.MESH)
    pl.semaphore_wait(barrier, 4)

    ys = [y_copy(m, h) for m in BOTH for h in range(spans - m)] + [y_half(q) for q in BOTH]
    for y in ys:
        y.start()

    tops = (c1a, c1b)
    lows = [pl.ds(0, half), pl.ds(half, half)]
    x_local = [pltpu.make_async_copy(cts[m].at[first, lanes], x1[m].at[first, :], own_sem.at[2 + m]) for m in BOTH]
    x_own = [[remote(cts[m].at[first, lanes], x1[m].at[first, :], top_send.at[m, k], top_recv.at[m], row=k + 1)
              for k in SPLITS] for m in BOTH]
    x_peer = [[remote(peer.at[m, :, lanes], x1[m].at[second, :], top_send.at[2 + m, k], top_recv.at[2 + m], row=k + 1)
               for k in SPLITS] for m in BOTH]
    top_far = [[remote(cts[m].at[:, lanes], tops[m], top_send.at[4 + m, 0], top_recv.at[4 + m], row=1)]
               + [remote(cts[m].at[lows[k], lanes], tops[m].at[lows[k], :], top_send.at[4 + m, 1 + k], top_recv.at[4 + m], row=2 + k)
                  for k in BOTH] for m in BOTH]

    @pl.when(row == 0)
    def _():
        for m in BOTH:
            x_local[m].start()
        for c in x_own[0] + x_own[1] + top_far[0] + top_far[1]:
            c.start()

    mine = pl.ds(pl.multiple_of(core * half, half), half)
    others = pl.ds(pl.multiple_of((1 - core) * half, half), half)
    g_mine = pl.ds(pl.multiple_of(core * nown, nown), nown)
    g_theirs = pl.ds(pl.multiple_of((1 - core) * nown, nown), nown)
    p1 = [to_mate(acc.at[m, others, :], r1buf.at[m], p_send.at[m], p_recv.at[m]) for m in BOTH]
    g1 = [to_mate(gacc.at[m, g_theirs, :], gbuf1.at[m], g_send.at[m], g_recv.at[m]) for m in BOTH]
    g2 = [to_across(gsum.at[m], gbuf2.at[m], g_send.at[2 + m], g_recv.at[2 + m]) for m in BOTH]
    g3 = [to_mate(full.at[g_mine, :], full.at[g_mine, :], g_send.at[4 + m], g_recv.at[4 + m]) for m, full in enumerate((gfull, g_out))]
    p2 = to_across(r1buf.at[0], r2buf, x_send.at[0], x_recv.at[0])
    p3 = to_mate(r1buf.at[0], pao, x_send.at[1], x_recv.at[1])
    swap = [to_mate(tops[m].at[mine, :], tops[m].at[mine, :], swap_send.at[m], swap_recv.at[m]) for m in BOTH]
    peer_out = [pltpu.make_async_copy(peer.at[m], (peer_a, peer_b)[m], out_sem.at[m]) for m in BOTH]
    pam_out = pltpu.make_async_copy(r1buf.at[0], pam, out_sem.at[2])

    def add_half(m):
        p1[m].wait()
        r1buf[m] = r1buf[m] + acc[m, mine, :]

    def finish_g1(m):
        g1[m].wait()
        gsum[m] = gacc[m, g_mine, :] + gbuf1[m]
        g2[m].start()

    def finish_g2(m, full):
        g2[m].wait()
        full[g_mine, :] = gsum[m] + gbuf2[m]
        g3[m].start()

    def send_x(m):
        @pl.when(row == 0)
        def _():
            x1[m][nown:, :] = peer[m, :, 0:N]
            for c in x_peer[m]:
                c.start()

    def wait_x(m):
        @pl.when(row == 0)
        def _():
            x_local[m].wait()

        @pl.when(row > 0)
        def _():
            x_own[m][0].wait_recv()
            x_peer[m][0].wait_recv()

    def begin_chain():
        wait_x(0)
        g3[0].wait()
        chain_init(col, gfull, x1a, st)

    def top_rows():
        @pl.when(row == 1)
        def _():
            for m in BOTH:
                top_far[m][0].wait_recv()

        @pl.when(row >= 2)
        def _():
            for m in BOTH:
                top_far[m][1].wait_recv()
                swap[m].start()

    def last_sums_a():
        p2.wait()
        r1buf[0] = r1buf[0] + r2buf[...]
        p3.start()
        pam_out.start()

    last = trips - nchunk
    begin = 1
    hooks = [[(0, lambda: send_x(0)), (last, lambda: finish_g1(0))],
             [(begin - 1, begin_chain), (begin, lambda: send_x(1)), (last - 1, last_sums_a), (last - 1, top_rows)]]

    def split_own(m):
        def build(q, _):
            s = pl.ds(pl.multiple_of(q * HALF, HALF), HALF)
            for i, part in enumerate(split3(own[m, :, s])):
                xo[m, i, :, s] = part
            return 0

        own_copies[m].wait()
        loop(rows // HALF, build, 0)

    def panel(m, s0, width):
        return [jnp.concatenate([xo[m, i, :, pl.ds(s0, width)], xs[i, :, 0:width]], 0) for i in SPLITS]

    def head(m, s0, width):
        for q in range(width // HALF):
            d = slice(q * HALF, (q + 1) * HALF)
            for i, part in enumerate(split3(peer[m, :, pl.ds(s0 + q * HALF, HALF)])):
                xs[i, :, d] = part
        x = panel(m, s0, width)
        return dot6(x, x, NT)

    def trip(m, j, slot, s0, width, fresh):
        x = panel(m, s0, width)
        for i in range(CHUNK // PIECE):
            r = dot6(split3(cbuf[slot, i * PIECE:(i + 1) * PIECE, 0:width]), x, NT)
            d = pl.ds(pl.multiple_of(nown + j * CHUNK + i * PIECE, 32), PIECE)
            acc[m, d, :] = jnp.where(fresh, r, acc[m, d, :] + r)

    def products(m, count):
        def span(h, _):
            y_copy(m, h).wait_recv()
            s0 = pl.multiple_of(h * SPAN, SPAN)
            r = head(m, s0, SPAN)
            gacc[m] = jnp.where(h == 0, r, gacc[m] + r)

            if m == 0:
                @pl.when(h == spans - 1)
                def _():
                    g1[0].start()

            def step(j, _):
                t = h * nchunk + j
                slot = lax.rem(m * trips + t, SLOTS)
                c_copy(m, t).wait()
                ahead = t + AHEAD - count * nchunk

                @pl.when(ahead < 0)
                def _():
                    c_copy(m, t + AHEAD).start()

                @pl.when(ahead >= 0)
                def _():
                    (c_copy(1, ahead) if m == 0 else c_half(ahead)).start()

                run = functools.partial(trip, m, j, slot, s0, SPAN, h == 0)
                if m == 0:
                    run()
                else:
                    live = (t >= begin) & (t < begin + NP)

                    @pl.when(live)
                    def _():
                        chain_cols(t - begin, st)
                        run()
                        weave(chain_update(t - begin, st), [])

                    pl.when(~live)(run)
                for at, hook in hooks[m]:
                    pl.when(t == at)(hook)
                return 0

            loop(nchunk, step, 0)
            return 0

        loop(count, span, 0)

    def last_span():
        def span(q, _):
            y_half(q).wait_recv()
            s0 = pl.multiple_of(rows - SPAN + q * HALF, HALF)
            gacc[1] = gacc[1] + head(1, s0, HALF)

            @pl.when(q == 1)
            def _():
                g1[1].start()

            def step(j, _):
                u = q * nchunk + j
                c_half(u).wait()

                @pl.when(u + AHEAD < 2 * nchunk)
                def _():
                    c_half(u + AHEAD).start()

                trip(1, j, half_slot(u), s0, HALF, False)

                @pl.when(u == nchunk)
                def _():
                    finish_g1(1)

                return 0

            loop(nchunk, step, 0)
            return 0

        loop(2, span, 0)

    for m in BOTH:
        split_own(m)
    products(0, spans)
    p1[0].start()
    peer_out[0].start()
    add_half(0)
    p2.start()
    finish_g2(0, gfull)
    products(1, spans - 1)
    last_span()
    p1[1].start()
    peer_out[1].start()
    wait_x(1)
    chain_final(col, st, outs)
    p1[1].wait()
    pbm[...] = r1buf[1] + acc[1, mine, :]
    finish_g2(1, g_out)
    g3[1].wait()

    @pl.when(row == 0)
    def _():
        for c in x_own[0] + x_own[1] + x_peer[0] + x_peer[1] + top_far[0] + top_far[1]:
            c.wait_send()

    @pl.when(row >= 2)
    def _():
        for m in BOTH:
            swap[m].wait()

    for c in peer_out + [p3, pam_out]:
        c.wait()
    for y in ys:
        y.wait_send()


def exchange(ca, cb, own):
    cols, rows = ca.shape
    half = cols // 2
    hbm = pl.BlockSpec(memory_space=pl.ANY)
    vm = pl.BlockSpec(memory_space=pltpu.VMEM)
    dma = pltpu.SemaphoreType.DMA
    pair = (2, N, N)
    ny = 2 * rows // SPAN + 1
    shapes = [(own, rows)] * 2 + [(cols, N)] * 2 + [(half, N)] * 3 + [(N, N), (N, N)] + CHAIN_SHAPES
    scratch = CHAIN_SCRATCH + [(N, N), (2, own, rows), (2, own, rows)]
    after = [(SLOTS, CHUNK, SPAN), (2, cols, N), pair, (2, half, N), (half, N)] + [(2, own, N)] * 3 + [(N, N)]
    return pl.pallas_call(
        exchange_kernel,
        in_specs=[hbm, hbm],
        out_specs=[hbm] * 6 + [vm] * (3 + len(CHAIN_SHAPES)),
        out_shape=[jax.ShapeDtypeStruct(s, F32) for s in shapes],
        scratch_shapes=[pltpu.VMEM(s, F32) for s in scratch] + [pltpu.VMEM((2, 3, own, rows), BF), pltpu.VMEM((3, own, SPAN), BF)]
        + [pltpu.VMEM(s, F32) for s in after]
        + [dma(n) for n in ((SLOTS,), (4,), (4,), (ny,), (ny,), (6, 3), (6,), (2,), (2,), (6,), (6,), (2,), (2,), (2,), (2,))],
        cost_estimate=pl.CostEstimate(flops=24 * cols * rows * N, bytes_accessed=8 * cols * rows, transcendentals=0),
        compiler_params=pltpu.CompilerParams(vmem_limit_bytes=60 * 2**20, collective_id=0, has_side_effects=True))(ca, cb)


def apply_update(ct, peer, psum, poth, c1, small, before, nxt=None, past=()):
    cols, rows = ct.shape
    nb = 512
    mb = 512
    own = peer.shape[0]
    half = cols // 2
    steps = rows // nb
    rinvt, minv, upt, ptt, _, _, bad = small
    no = len(CHAIN_SHAPES)
    extra = list(nxt or ()) + list(past)
    ne = len(extra)

    def body(c_ref, x_ref, p_ref, q_ref, c1_ref, r_ref, m_ref, up_ref, pt_ref, bad_ref, before_ref, *refs):
        ins, (o_ref, f_ref) = refs[:ne], refs[ne:ne + 2]
        outs, (z_ref, rc_ref, *st) = refs[ne + 2:len(refs) - ns], refs[len(refs) - ns:]
        i = pl.program_id(0)
        row = lax.axis_index("row")
        top = row == 0

        @pl.when(i == 0)
        def _():
            zero = jnp.zeros((1, 1), F32)
            for which, src in enumerate((p_ref, q_ref)):
                base = pl.multiple_of((lax.rem(row, 2) ^ which) * half, half)
                for j in range(half // mb):
                    s = slice(j * mb, (j + 1) * mb)
                    d = pl.ds(base + j * mb, mb)
                    rc = hdot(src[s, :], r_ref[...], NT)
                    z = hdot(jnp.where(top, c_ref[d, 0:N], c1_ref[d, :]) - rc, m_ref[...], NT)
                    rc_ref[d, :] = rc
                    z_ref[d, :] = z
                    zero = zero + total(total(z * 0.0, 0), 1)
            f_ref[...] = jnp.where(zero == 0.0, 0.0, 1.0) + bad_ref[...] + before_ref[...]
            if nxt is not None:
                chain_init(lax.axis_index("col"), *ins[:2], st)
                outs[4][0:N, :] = ins[2][...]
                outs[4][2 * N:2 * N + NP, :] = ins[3][...]

        def piece(j):
            x = jnp.concatenate([c_ref[0:own, :], x_ref[...]], 0)
            lo = own if j == 0 else j * mb
            if j == 0:
                o_ref[0:own, :] = hdot(up_ref[...], x)
            s = slice(lo, (j + 1) * mb)
            o_ref[s, :] = c_ref[s, :] - hdot(z_ref[s, :], x)

        pieces = [functools.partial(piece, j) for j in range(cols // mb)]
        if nxt is None:
            weave([], pieces)
        else:
            @pl.when(lax.rem(i, 2) == 0)
            def _():
                chain_cols(lax.div(i, 2), st)
                weave([], pieces)

            @pl.when(lax.rem(i, 2) == 1)
            def _():
                weave(chain_update(lax.div(i, 2), st), pieces)

            @pl.when(i == steps - 1)
            def _():
                tts = (outs[4].at[pl.ds(N, N), :], outs[4].at[pl.ds(2 * N + NP, NP), :])
                chain_final(lax.axis_index("col"), st, (*outs[:4], *tts, outs[6]))

        @pl.when((i == 0) & top)
        def _():
            o_ref[0:own, 0:N] = pt_ref[...]
            o_ref[own:, 0:N] = rc_ref[own:, :]

    blk2 = pl.BlockSpec((cols, nb), lambda i: (0, i))
    fixed = lambda shape: pl.BlockSpec(shape, lambda i: (0, 0))
    consts = [psum, poth, c1, rinvt, minv, upt, ptt, bad, before] + extra
    more = CHAIN_SHAPES[:4] + [(2 * (N + NP), W)] + CHAIN_SHAPES[5:] if nxt is not None else []
    scratch = [(cols, N), (cols, N)] + (CHAIN_SCRATCH if nxt is not None else [])
    ns = len(scratch)
    return pl.pallas_call(
        body, grid=(steps,),
        in_specs=[blk2, pl.BlockSpec((own, nb), lambda i: (0, i))] + [fixed(a.shape) for a in consts],
        out_specs=[blk2, fixed(TILE)] + [fixed(s) for s in more],
        scratch_shapes=[pltpu.VMEM(s, F32) for s in scratch],
        out_shape=[jax.ShapeDtypeStruct(s, F32) for s in [(cols, rows), TILE] + more],
        cost_estimate=pl.CostEstimate(flops=12 * cols * rows * N, bytes_accessed=8 * cols * rows, transcendentals=0),
        compiler_params=pltpu.CompilerParams(vmem_limit_bytes=60 * 2**20))(ct, peer, *consts)


R1 = [(0, 1), (1, 0), (2, 3), (3, 2)]
R2 = [(0, 2), (2, 0), (1, 3), (3, 1)]
CY = [(0, 1), (1, 0)]


def row_major(x):
    def body(i_ref, o_ref):
        o_ref[...] = i_ref[...]

    return pl.pallas_call(body, out_shape=jax.ShapeDtypeStruct(x.shape, F32))(x)


def pick(x, i, axis=0):
    return lax.dynamic_slice_in_dim(x, i, 1, axis)


def row_sum(x):
    x = x + lax.ppermute(x, "row", R1)
    return x + lax.ppermute(x, "row", R2)


def factor_columns(stored):
    local_rows, local_blocks, width = stored.shape
    row_rank = lax.axis_index("row")
    col_rank = lax.axis_index("col")
    row_ids = row_rank * local_rows + jnp.arange(local_rows)
    col_ids = jnp.arange(width)
    edot = functools.partial(jnp.einsum, precision=HI, preferred_element_type=F32)

    def panel_step(panel_idx, state):
        stored, taus, tfs = state
        row_start = panel_idx * width
        local_idx = panel_idx // 2
        is_owner = col_rank == panel_idx % 2
        panel_in = pick(stored, local_idx, 1)[:, 0, :]

        def column_step(col_idx, loop_state):
            work, tau_vec = loop_state
            diag_idx = row_start + col_idx
            column = pick(work, col_idx, 1)[:, 0]
            below = jnp.where(row_ids >= diag_idx, column, 0.0)
            at_diag = (row_ids == diag_idx).astype(F32)
            summed = row_sum(edot("ar,rk->ak", jnp.stack([below, at_diag]), work))
            cross, diag_row = summed[0], summed[1]
            pivot = pick(diag_row, col_idx)[0]
            norm = jnp.sqrt(pick(cross, col_idx)[0])
            beta = -jnp.where(pivot >= 0, 1.0, -1.0) * norm
            tau = (beta - pivot) / beta
            denom = pivot - beta
            proj = jnp.where(col_ids > col_idx, (cross - beta * diag_row) / denom, 0.0)
            refl = jnp.where(row_ids > diag_idx, column / denom, 0.0) + at_diag
            work = work - tau * refl[:, None] * proj[None, :]
            new_col = jnp.where(row_ids < diag_idx, column, jnp.where(row_ids == diag_idx, beta, refl))
            work = lax.dynamic_update_slice_in_dim(work, new_col[:, None], col_idx, 1)
            return work, lax.dynamic_update_slice_in_dim(tau_vec, tau[None], col_idx, 0)

        work, tau_vec = loop(width, column_step, (panel_in, jnp.zeros((width,), F32)))
        diag_ids = row_start + col_ids[None, :]
        v_block = jnp.where(row_ids[:, None] == diag_ids, 1.0, jnp.where(row_ids[:, None] > diag_ids, work, 0.0))

        gram = row_sum(edot("ri,rj->ij", v_block, v_block))

        def t_step(col_idx, tf):
            g = pick(gram, col_idx, 1)[:, 0]
            g = jnp.where(col_ids < col_idx, g, 0.0)
            tau_k = pick(tau_vec, col_idx)[0]
            t_col = -tau_k * edot("ij,j->i", tf, g)
            t_col = jnp.where(col_ids == col_idx, tau_k, t_col)
            return lax.dynamic_update_slice_in_dim(tf, t_col[:, None], col_idx, 1)

        tf = loop(width, t_step, jnp.zeros((width, width), F32))
        v_mine = jnp.where(is_owner, v_block, 0.0)
        t_mine = jnp.where(is_owner, tf, 0.0)
        v_block = v_mine + lax.ppermute(v_mine, "col", CY)
        tf = t_mine + lax.ppermute(t_mine, "col", CY)

        def block_step(b, stored):
            blk = pick(stored, b, 1)[:, 0, :]
            w = edot("ij,ik->jk", tf, row_sum(edot("ri,rk->ik", v_block, blk)))
            upd = blk - edot("ri,ik->rk", v_block, w)
            keep = b * 2 + col_rank > panel_idx
            mine = (b == local_idx) & is_owner
            new = jnp.where(keep, upd, jnp.where(mine, work, blk))
            return lax.dynamic_update_slice_in_dim(stored, new[:, None, :], b, 1)

        stored = loop(local_blocks, block_step, stored)
        taus = lax.dynamic_update_slice_in_dim(taus, jnp.diagonal(tf), row_start, 0)
        return stored, taus, lax.dynamic_update_slice_in_dim(tfs, tf, row_start, 0)

    return loop(PANELS, panel_step, (stored, jnp.zeros((PANELS * width,), F32), jnp.zeros((PANELS * width, width), F32)))


def solution(mesh):
    def factor_both(a_matrix, b_matrix):
        local_rows, local_blocks, width = a_matrix.shape
        cols = local_blocks * width
        own = 2 * width
        col_rank = lax.axis_index("col")
        cts = [m.transpose(1, 2, 0).reshape(cols, local_rows) for m in (a_matrix, b_matrix)]

        pa, pb, c1a, c1b, pam, pao, pbm, g, x1, *first = exchange(*cts, own)
        across = lax.ppermute(pbm, "row", R2)
        out_a, bad_a, *second = apply_update(cts[0], pa, pam, pao, c1a, first, first[6], (g, x1), (first[4], first[5]))
        across, bad_a = lax.optimization_barrier((across, bad_a))
        pbm = pbm + across
        pbo = lax.ppermute(pbm, "row", R1)
        small = lax.ppermute(second[4], "col", [(0, 1)])
        out_b, bad = apply_update(cts[1], pb, pbm, pbo, c1b, second, bad_a)
        small, bad = lax.optimization_barrier((small, bad))
        tt = jnp.where(col_rank == 0, second[4], small)

        def parts(tt):
            return tt[:N], tt[N:2 * N], *(x.reshape(N) for x in jnp.split(tt[2 * N:], 2))

        carry = (bad, lax.ppermute(bad, "col", CY), *parts(tt), out_a, out_b)

        def redo(state):
            def one(i, done):
                st, taus, tfs = factor_columns(jnp.where(i == 0, a_matrix, b_matrix))
                new = (st.transpose(1, 2, 0).reshape(cols, local_rows), jnp.concatenate([tfs, taus.reshape(PANELS, width)], 0))
                return tuple(jnp.where(i == k, n, d) for k, pair in enumerate((done[:2], done[2:])) for n, d in zip(new, pair))

            blank = jnp.zeros((N + PANELS, width), F32)
            st_a, tt_a, st_b, tt_b = loop(2, one, (state[6], blank, state[7], blank))
            tt = row_major(jnp.concatenate([tt_a[:N], tt_b[:N], tt_a[N:], tt_b[N:]], 0))
            return jnp.zeros(TILE, F32), jnp.zeros(TILE, F32), *(row_major(x) for x in parts(tt)), st_a, st_b

        res = lax.while_loop(lambda s: jnp.max(s[0] + s[1]) > 0.5, redo, carry)
        back = lambda x: x.reshape(local_blocks, width, local_rows).transpose(2, 0, 1)
        stack = lambda x: x.reshape(PANELS, width, width)
        return back(res[6]), res[4], stack(res[2]), back(res[7]), res[5], stack(res[3])

    spec_mat = P(("batch", "row"), "col", None)
    spec_out = (spec_mat, P("batch"), P("batch", None, None))
    return jax.shard_map(factor_both, mesh=mesh, in_specs=(spec_mat, spec_mat), out_specs=spec_out + spec_out, check_vma=False)
```

```python
import functools

import jax
import jax.numpy as jnp
from jax import lax
from jax.experimental import pallas as pl
from jax.experimental.pallas import tpu as pltpu
from jax.sharding import PartitionSpec as P

F32 = jnp.float32
BF = jnp.bfloat16
HI = lax.Precision.HIGHEST
PANELS = 4
W = 64
NP = 4
N = 256
NN = (((1,), (0,)), ((), ()))
NT = (((1,), (1,)), ((), ()))
TN = (((0,), (0,)), ((), ()))


BOTH = (0, 1)
total = functools.partial(jnp.sum, keepdims=True)
peak = functools.partial(jnp.max, keepdims=True)
TILE = (8, 128)


def rows_of(shape):
    return lax.broadcasted_iota(jnp.int32, shape, 0)


def lanes_of(shape):
    return lax.broadcasted_iota(jnp.int32, shape, 1)


def hdot(a, b, dn=NN):
    return lax.dot_general(a, b, dn, precision=HI, preferred_element_type=F32)


GROUP = 4
AMPLIFY = 64.0
HUGE = 1e9


def diag_factor(mats):
    tiles = W // 8
    lane8 = lanes_of(TILE)
    sub8 = rows_of(TILE)
    r64 = rows_of((W, W))
    c64 = lanes_of((W, W))
    eye = (r64 == c64).astype(F32)
    full = lambda x: jnp.broadcast_to(x, TILE)
    zeros = jnp.zeros(TILE, F32)
    st = []
    for hpp, ypp in mats:
        he = jnp.concatenate([hpp, eye], 1)
        yw = jnp.concatenate([ypp, eye], 1)
        st.append(dict(he=[he[8 * g:8 * g + 8] for g in range(tiles)], yw=[yw[8 * g:8 * g + 8] for g in range(tiles)],
                       l=[zeros] * tiles, u=[zeros] * tiles, tau=zeros))
    for k0 in range(0, W, GROUP):
        gk = k0 // 8
        for s in st:
            s['bh'] = [[full(s['he'][g][:, k:k + 1]) for g in range(gk, tiles)] for k in range(k0, k0 + GROUP)]
            s['by'] = [[full(s['yw'][g][:, k:k + 1]) for g in range(tiles)] for k in range(k0, k0 + GROUP)]
        for k in range(k0, k0 + GROUP):
            sk = k - 8 * gk
            isk = sub8 == sk
            for s in st:
                ch, cy = s['bh'][k - k0], s['by'][k - k0]
                pick = lambda x: full(x[sk:sk + 1, :])
                h = pick(ch[0])
                a = pick(cy[gk])
                rs = lax.rsqrt(h)
                rinv = jnp.where(a >= 0, -rs, rs)
                ukk = a - h * rinv
                uinv = 1.0 / ukk
                r = pick(s['he'][gk]) * rinv
                u = pick(s['yw'][gk]) - jnp.where((lane8 >= k) & (lane8 < W), r, 0.0)
                un = u * uinv
                rr = r * rinv
                for k2 in range(k + 1, k0 + GROUP):
                    r2 = pick(s['bh'][k2 - k0][0]) * rinv
                    un2 = (pick(s['by'][k2 - k0][gk]) - r2) * uinv
                    rr2 = r2 * rinv
                    s['bh'][k2 - k0] = [x - ch[i] * rr2 for i, x in enumerate(s['bh'][k2 - k0])]
                    nby = [x - cy[i] * un2 for i, x in enumerate(s['by'][k2 - k0])]
                    nby[gk] = jnp.where(isk, un2, nby[gk])
                    s['by'][k2 - k0] = nby
                for g in range(gk, tiles):
                    new = s['he'][g] - ch[g - gk] * rr
                    lc = cy[g] * uinv
                    if g == gk:
                        new = jnp.where(sub8 > sk, new, jnp.where(isk, r, s['he'][g]))
                        lc = jnp.where(sub8 > sk, lc, 0.0)
                    s['he'][g] = new
                    s['l'][g] = jnp.where(lane8 == k, lc, s['l'][g])
                for g in range(tiles):
                    new = s['yw'][g] - cy[g] * un
                    s['yw'][g] = jnp.where(isk, un, new) if g == gk else new
                s['u'][gk] = jnp.where(isk, u, s['u'][gk])
                s['tau'] = jnp.where(lane8 == k, -ukk * rinv, s['tau'])
    out = []
    up = c64 >= r64
    for s in st:
        he = jnp.concatenate(s['he'], 0)
        yw = jnp.concatenate(s['yw'], 0)
        l = jnp.concatenate(s['l'], 0)[:, :W]
        u = jnp.concatenate(s['u'], 0)[:, :W]
        out.append((jnp.where(c64 <= r64, he[:, W:], 0.0), l + eye, jnp.where(up, u, 0.0), yw[:, W:], s['tau'][0:1, :W]))
    return out


def blk(b):
    return slice(b * W, (b + 1) * W)


def order(c):
    return [2 * l + c for l in BOTH] + [2 * l + 1 - c for l in BOTH]


def turn(x):
    return jnp.concatenate([x[:, W:N], x[:, :W], x[:, N:]], 1)


CHAIN_SCRATCH = [(N, 2 * N), (N, 2 * N), (N, N), (NP, 4, W, W), (8, N), (NP, W)]
CHAIN_SHAPES = [(N, N), (N, N), (2 * W, N), (2 * W, N), (N, W), (NP, W), TILE]


def chain_init(col, g, x1, st):
    hs, ys, ls, _, norm, _ = st
    ri, ci = rows_of((N, N)), lanes_of((N, N))
    eye = (ri == ci).astype(F32)
    for c in BOTH:
        @pl.when(col == c)
        def _():
            for i, b in enumerate(order(c)):
                ls[blk(b), :] = x1[blk(i), :]
                for i2, b2 in enumerate(order(c)):
                    hs[blk(b), blk(b2)] = g[blk(i), blk(i2)]
    hs[:, N:] = eye
    ys[:, :N] = ls[...].T
    ys[:, N:] = eye
    dg = jnp.where(ri == ci, hs[:, :N], 0.0)
    norm[...] = jnp.broadcast_to(jnp.sqrt(total(dg, 0)), (8, N))


def chain_cols(p, st):
    hs, ys, _, fac, _, tv = st
    e, l, u, w, tau = diag_factor([(hs[0:W, 0:W], ys[0:W, 0:W])])[0]
    for i, x in enumerate((e, l, u, w)):
        fac[p, i] = x
    tv[pl.ds(p, 1), :] = tau


def chain_update(p, st):
    hs, ys, ls, fac, _, _ = st
    rw = rows_of((W, 2 * N))
    cw = lanes_of((W, 2 * N))
    rl = rows_of((N - W, W))
    live = N - p * W
    e, l, w = fac[p, 0], fac[p, 1], fac[p, 3]
    rall = hdot(e, hs[0:W, :])
    rall = jnp.where((cw >= N) | ((cw >= rw) & (cw < live)), rall, 0.0)
    wl = hdot(w, l)
    yield
    yc = ys[W:, 0:W]
    nrow = hdot(w, ys[0:W, :] - jnp.where(cw < N, rall, 0.0))
    hnew = hs[W:, :] - hdot(rall[:, W:N], rall, TN)
    hs[0:N - W, :] = turn(hnew)
    hs[N - W:, :] = turn(rall)
    lnew = jnp.where(rl < live - W, hdot(yc, wl), 0.0)
    rest = ls[W:, W:]
    first = ls[0:W, W:]
    ls[0:N - W, N - W:] = lnew
    ls[N - W:, N - W:] = l
    ls[0:N - W, 0:N - W] = rest
    ls[N - W:, 0:N - W] = first
    yield
    ynew = ys[W:, :] - hdot(yc, nrow)
    ys[0:N - W, :] = turn(ynew)
    ys[N - W:, :] = turn(nrow)


def weave(stages, pieces):
    stages = iter(stages)
    for piece in pieces:
        next(stages, None)
        piece()
    for _ in stages:
        pass


def chain_final(col, st, outs):
    hs, ys, ls, fac, norm, tv = st
    rinvt, minv, upt, ptt, tfac, tau, bad = outs
    r64 = rows_of((W, W))
    c64 = lanes_of((W, W))
    tau[...] = tv[...]
    for p in range(NP):
        e, _, u, w = [fac[p, i] for i in range(4)]
        t = -hdot(hdot(u, e, NT), hdot(u, w), NT)
        tfac[blk(p), :] = jnp.where(c64 > r64, t, jnp.where(c64 == r64, jnp.broadcast_to(tv[p:p + 1, :], (W, W)), 0.0))
    ri = rows_of((N, N))
    ci = lanes_of((N, N))
    rt, mi = hs[:, N:], ys[:, N:]
    g = norm[0:1, :]
    c1 = peak(total(jnp.abs(rt) * g, 1))
    c2 = peak(hdot(g, jnp.abs(mi)))
    good = (c1 <= AMPLIFY) & (c2 <= AMPLIFY) & (-peak(-g) >= 1 / HUGE) & (peak(g) <= HUGE)
    bad[...] = jnp.broadcast_to(jnp.where(good, 0.0, 1.0), TILE)
    pt = jnp.where(ri > ci, ls[...], hs[:, :N]).T
    ut = lax.dot_general(ls[...], mi, (((0,), (1,)), ((), ())), precision=HI, preferred_element_type=F32)
    hs[:, :N] = pt
    ys[:, :N] = ut
    for c in BOTH:
        @pl.when(col == c)
        def _():
            for i, b in enumerate(order(c)):
                rinvt[:, blk(i)] = hs[:, N + b * W:N + (b + 1) * W]
                minv[blk(i), :] = ys[blk(b), N:]
            for i in BOTH:
                b = order(c)[i]
                ptt[blk(i), :] = hs[blk(b), :N]
                for i2, b2 in enumerate(order(c)):
                    upt[blk(i), blk(i2)] = ys[blk(b), blk(b2)]


SPLITS = range(3)
loop = functools.partial(lax.fori_loop, 0)


def split3(x):
    h = x.astype(BF)
    r = x - h.astype(F32)
    m = r.astype(BF)
    return h, m, (r - m.astype(F32)).astype(BF)


def dot6(a, b, dn):
    d = lambda i, j: lax.dot_general(a[i], b[j], dn, preferred_element_type=F32)
    return (((d(2, 0) + d(0, 2)) + d(1, 1)) + (d(1, 0) + d(0, 1))) + d(0, 0)


CHUNK = 960
PIECE = 480
HALF = 512
SPAN = 1024
SLOTS = 3
AHEAD = SLOTS - 1


def exchange_kernel(ca, cb, peer_a, peer_b, c1a, c1b, pam, pao, pbm, g_out, x1b, *refs):
    outs, refs = refs[:len(CHAIN_SHAPES)], refs[len(CHAIN_SHAPES):]
    st, refs = refs[:len(CHAIN_SCRATCH)], refs[len(CHAIN_SCRATCH):]
    (x1a, peer, own, xo, xs, cbuf, acc, gacc, r1buf, r2buf, gbuf1, gsum, gbuf2, gfull,
     c_sem, own_sem, out_sem, y_send, y_recv, top_send, top_recv, swap_send, swap_recv,
     g_send, g_recv, p_send, p_recv, x_send, x_recv) = refs
    cts, x1 = (ca, cb), (x1a, x1b)
    row = lax.axis_index("row")
    col = lax.axis_index("col")
    core = lax.rem(row, 2)
    mate = row + 1 - 2 * core
    across = lax.rem(row + 2, 4)
    diag = lax.rem(row + 3 - 2 * core, 4)
    cols, rows = ca.shape
    half = cols // 2
    nown = peer.shape[1]
    nchunk = (cols - nown) // CHUNK
    spans = rows // SPAN
    trips = nchunk * spans

    def remote(src, dst, send, recv, **where):
        return pltpu.make_async_remote_copy(src_ref=src, dst_ref=dst, send_sem=send, recv_sem=recv,
                                            device_id=where, device_id_type=pl.DeviceIdType.MESH)

    to_mate = functools.partial(remote, row=mate)
    to_across = functools.partial(remote, row=across)

    def c_copy(m, t):
        slot = lax.rem(m * trips + t, SLOTS)
        h, j = lax.div(t, nchunk), lax.rem(t, nchunk)
        return pltpu.make_async_copy(
            cts[m].at[pl.ds(pl.multiple_of(nown + j * CHUNK, 64), CHUNK), pl.ds(pl.multiple_of(h * SPAN, SPAN), SPAN)],
            cbuf.at[slot], c_sem.at[slot])

    first = pl.ds(0, nown)
    second = pl.ds(nown, nown)
    lanes = pl.ds(0, N)

    def y_copy(m, h):
        s = pl.ds(pl.multiple_of(h * SPAN, SPAN), SPAN)
        i = m * spans + h
        return remote(cts[m].at[first, s], peer.at[m, :, s], y_send.at[i], y_recv.at[i], col=1 - col)

    def half_slot(u):
        return lax.rem(2 * trips - nchunk + u, SLOTS)

    def c_half(u):
        q, j = lax.div(u, nchunk), lax.rem(u, nchunk)
        return pltpu.make_async_copy(
            cb.at[pl.ds(pl.multiple_of(nown + j * CHUNK, 64), CHUNK), pl.ds(pl.multiple_of(rows - SPAN + q * HALF, HALF), HALF)],
            cbuf.at[half_slot(u), :, pl.ds(0, HALF)], c_sem.at[half_slot(u)])

    def y_half(q):
        s = pl.ds(pl.multiple_of(rows - SPAN + q * HALF, HALF), HALF)
        i = 2 * spans - 1 + q
        return remote(cb.at[first, s], peer.at[1, :, s], y_send.at[i], y_recv.at[i], col=1 - col)

    own_copies = [pltpu.make_async_copy(cts[m].at[first, :], own.at[m], own_sem.at[m]) for m in BOTH]
    for o in own_copies:
        o.start()
    for t in range(AHEAD):
        c_copy(0, t).start()

    for m in BOTH:
        acc[m, 0:nown, :] = jnp.zeros((nown, N), F32)
    barrier = pltpu.get_barrier_semaphore()
    for where in (dict(row=mate), dict(row=across), dict(row=diag), dict(col=1 - col)):
        pl.semaphore_signal(barrier, device_id=where, device_id_type=pl.DeviceIdType.MESH)
    pl.semaphore_wait(barrier, 4)

    ys = [y_copy(m, h) for m in BOTH for h in range(spans - m)] + [y_half(q) for q in BOTH]
    for y in ys:
        y.start()

    tops = (c1a, c1b)
    lows = [pl.ds(0, half), pl.ds(half, half)]
    x_local = [pltpu.make_async_copy(cts[m].at[first, lanes], x1[m].at[first, :], own_sem.at[2 + m]) for m in BOTH]
    x_own = [[remote(cts[m].at[first, lanes], x1[m].at[first, :], top_send.at[m, k], top_recv.at[m], row=k + 1)
              for k in SPLITS] for m in BOTH]
    x_peer = [[remote(peer.at[m, :, lanes], x1[m].at[second, :], top_send.at[2 + m, k], top_recv.at[2 + m], row=k + 1)
               for k in SPLITS] for m in BOTH]
    top_far = [[remote(cts[m].at[:, lanes], tops[m], top_send.at[4 + m, 0], top_recv.at[4 + m], row=1)]
               + [remote(cts[m].at[lows[k], lanes], tops[m].at[lows[k], :], top_send.at[4 + m, 1 + k], top_recv.at[4 + m], row=2 + k)
                  for k in BOTH] for m in BOTH]

    @pl.when(row == 0)
    def _():
        for m in BOTH:
            x_local[m].start()
        for c in x_own[0] + x_own[1] + top_far[0] + top_far[1]:
            c.start()

    mine = pl.ds(pl.multiple_of(core * half, half), half)
    others = pl.ds(pl.multiple_of((1 - core) * half, half), half)
    g_mine = pl.ds(pl.multiple_of(core * nown, nown), nown)
    g_theirs = pl.ds(pl.multiple_of((1 - core) * nown, nown), nown)
    p1 = [to_mate(acc.at[m, others, :], r1buf.at[m], p_send.at[m], p_recv.at[m]) for m in BOTH]
    g1 = [to_mate(gacc.at[m, g_theirs, :], gbuf1.at[m], g_send.at[m], g_recv.at[m]) for m in BOTH]
    g2 = [to_across(gsum.at[m], gbuf2.at[m], g_send.at[2 + m], g_recv.at[2 + m]) for m in BOTH]
    g3 = [to_mate(full.at[g_mine, :], full.at[g_mine, :], g_send.at[4 + m], g_recv.at[4 + m]) for m, full in enumerate((gfull, g_out))]
    p2 = to_across(r1buf.at[0], r2buf, x_send.at[0], x_recv.at[0])
    p3 = to_mate(r1buf.at[0], pao, x_send.at[1], x_recv.at[1])
    swap = [to_mate(tops[m].at[mine, :], tops[m].at[mine, :], swap_send.at[m], swap_recv.at[m]) for m in BOTH]
    peer_out = [pltpu.make_async_copy(peer.at[m], (peer_a, peer_b)[m], out_sem.at[m]) for m in BOTH]
    pam_out = pltpu.make_async_copy(r1buf.at[0], pam, out_sem.at[2])

    def add_half(m):
        p1[m].wait()
        r1buf[m] = r1buf[m] + acc[m, mine, :]

    def finish_g1(m):
        g1[m].wait()
        gsum[m] = gacc[m, g_mine, :] + gbuf1[m]
        g2[m].start()

    def finish_g2(m, full):
        g2[m].wait()
        full[g_mine, :] = gsum[m] + gbuf2[m]
        g3[m].start()

    def send_x(m):
        @pl.when(row == 0)
        def _():
            x1[m][nown:, :] = peer[m, :, 0:N]
            for c in x_peer[m]:
                c.start()

    def wait_x(m):
        @pl.when(row == 0)
        def _():
            x_local[m].wait()

        @pl.when(row > 0)
        def _():
            x_own[m][0].wait_recv()
            x_peer[m][0].wait_recv()

    def begin_chain():
        wait_x(0)
        g3[0].wait()
        chain_init(col, gfull, x1a, st)

    def top_rows():
        @pl.when(row == 1)
        def _():
            for m in BOTH:
                top_far[m][0].wait_recv()

        @pl.when(row >= 2)
        def _():
            for m in BOTH:
                top_far[m][1].wait_recv()
                swap[m].start()

    def last_sums_a():
        p2.wait()
        r1buf[0] = r1buf[0] + r2buf[...]
        p3.start()
        pam_out.start()

    last = trips - nchunk
    begin = 1
    hooks = [[(0, lambda: send_x(0)), (last, lambda: finish_g1(0))],
             [(begin - 1, begin_chain), (begin, lambda: send_x(1)), (last - 1, last_sums_a), (last - 1, top_rows)]]

    def split_own(m):
        def build(q, _):
            s = pl.ds(pl.multiple_of(q * HALF, HALF), HALF)
            for i, part in enumerate(split3(own[m, :, s])):
                xo[m, i, :, s] = part
            return 0

        own_copies[m].wait()
        loop(rows // HALF, build, 0)

    def panel(m, s0, width):
        return [jnp.concatenate([xo[m, i, :, pl.ds(s0, width)], xs[i, :, 0:width]], 0) for i in SPLITS]

    def head(m, s0, width):
        for q in range(width // HALF):
            d = slice(q * HALF, (q + 1) * HALF)
            for i, part in enumerate(split3(peer[m, :, pl.ds(s0 + q * HALF, HALF)])):
                xs[i, :, d] = part
        x = panel(m, s0, width)
        return dot6(x, x, NT)

    def trip(m, j, slot, s0, width, fresh):
        x = panel(m, s0, width)
        for i in range(CHUNK // PIECE):
            r = dot6(split3(cbuf[slot, i * PIECE:(i + 1) * PIECE, 0:width]), x, NT)
            d = pl.ds(pl.multiple_of(nown + j * CHUNK + i * PIECE, 32), PIECE)
            acc[m, d, :] = jnp.where(fresh, r, acc[m, d, :] + r)

    def products(m, count):
        def span(h, _):
            y_copy(m, h).wait_recv()
            s0 = pl.multiple_of(h * SPAN, SPAN)
            r = head(m, s0, SPAN)
            gacc[m] = jnp.where(h == 0, r, gacc[m] + r)

            if m == 0:
                @pl.when(h == spans - 1)
                def _():
                    g1[0].start()

            def step(j, _):
                t = h * nchunk + j
                slot = lax.rem(m * trips + t, SLOTS)
                c_copy(m, t).wait()
                ahead = t + AHEAD - count * nchunk

                @pl.when(ahead < 0)
                def _():
                    c_copy(m, t + AHEAD).start()

                @pl.when(ahead >= 0)
                def _():
                    (c_copy(1, ahead) if m == 0 else c_half(ahead)).start()

                run = functools.partial(trip, m, j, slot, s0, SPAN, h == 0)
                if m == 0:
                    run()
                else:
                    live = (t >= begin) & (t < begin + NP)

                    @pl.when(live)
                    def _():
                        chain_cols(t - begin, st)
                        run()
                        weave(chain_update(t - begin, st), [])

                    pl.when(~live)(run)
                for at, hook in hooks[m]:
                    pl.when(t == at)(hook)
                return 0

            loop(nchunk, step, 0)
            return 0

        loop(count, span, 0)

    def last_span():
        def span(q, _):
            y_half(q).wait_recv()
            s0 = pl.multiple_of(rows - SPAN + q * HALF, HALF)
            gacc[1] = gacc[1] + head(1, s0, HALF)

            @pl.when(q == 1)
            def _():
                g1[1].start()

            def step(j, _):
                u = q * nchunk + j
                c_half(u).wait()

                @pl.when(u + AHEAD < 2 * nchunk)
                def _():
                    c_half(u + AHEAD).start()

                trip(1, j, half_slot(u), s0, HALF, False)

                @pl.when(u == nchunk)
                def _():
                    finish_g1(1)

                return 0

            loop(nchunk, step, 0)
            return 0

        loop(2, span, 0)

    for m in BOTH:
        split_own(m)
    products(0, spans)
    p1[0].start()
    peer_out[0].start()
    add_half(0)
    p2.start()
    finish_g2(0, gfull)
    products(1, spans - 1)
    last_span()
    p1[1].start()
    peer_out[1].start()
    wait_x(1)
    chain_final(col, st, outs)
    p1[1].wait()
    pbm[...] = r1buf[1] + acc[1, mine, :]
    finish_g2(1, g_out)
    g3[1].wait()

    @pl.when(row == 0)
    def _():
        for c in x_own[0] + x_own[1] + x_peer[0] + x_peer[1] + top_far[0] + top_far[1]:
            c.wait_send()

    @pl.when(row >= 2)
    def _():
        for m in BOTH:
            swap[m].wait()

    for c in peer_out + [p3, pam_out]:
        c.wait()
    for y in ys:
        y.wait_send()


def exchange(ca, cb, own):
    cols, rows = ca.shape
    half = cols // 2
    hbm = pl.BlockSpec(memory_space=pl.ANY)
    vm = pl.BlockSpec(memory_space=pltpu.VMEM)
    dma = pltpu.SemaphoreType.DMA
    pair = (2, N, N)
    ny = 2 * rows // SPAN + 1
    shapes = [(own, rows)] * 2 + [(cols, N)] * 2 + [(half, N)] * 3 + [(N, N), (N, N)] + CHAIN_SHAPES
    scratch = CHAIN_SCRATCH + [(N, N), (2, own, rows), (2, own, rows)]
    after = [(SLOTS, CHUNK, SPAN), (2, cols, N), pair, (2, half, N), (half, N)] + [(2, own, N)] * 3 + [(N, N)]
    return pl.pallas_call(
        exchange_kernel,
        in_specs=[hbm, hbm],
        out_specs=[hbm] * 6 + [vm] * (3 + len(CHAIN_SHAPES)),
        out_shape=[jax.ShapeDtypeStruct(s, F32) for s in shapes],
        scratch_shapes=[pltpu.VMEM(s, F32) for s in scratch] + [pltpu.VMEM((2, 3, own, rows), BF), pltpu.VMEM((3, own, SPAN), BF)]
        + [pltpu.VMEM(s, F32) for s in after]
        + [dma(n) for n in ((SLOTS,), (4,), (4,), (ny,), (ny,), (6, 3), (6,), (2,), (2,), (6,), (6,), (2,), (2,), (2,), (2,))],
        cost_estimate=pl.CostEstimate(flops=24 * cols * rows * N, bytes_accessed=8 * cols * rows, transcendentals=0),
        compiler_params=pltpu.CompilerParams(vmem_limit_bytes=46 * 2**20, collective_id=0, has_side_effects=True))(ca, cb)


def apply_update(ct, peer, psum, poth, c1, small, before, nxt=None, past=()):
    cols, rows = ct.shape
    nb = 512
    mb = 512
    own = peer.shape[0]
    half = cols // 2
    steps = rows // nb
    rinvt, minv, upt, ptt, _, _, bad = small
    no = len(CHAIN_SHAPES)
    extra = list(nxt or ()) + list(past)
    ne = len(extra)

    def body(c_ref, x_ref, p_ref, q_ref, c1_ref, r_ref, m_ref, up_ref, pt_ref, bad_ref, before_ref, *refs):
        ins, (o_ref, f_ref) = refs[:ne], refs[ne:ne + 2]
        outs, (z_ref, rc_ref, *st) = refs[ne + 2:len(refs) - ns], refs[len(refs) - ns:]
        i = pl.program_id(0)
        row = lax.axis_index("row")
        top = row == 0

        @pl.when(i == 0)
        def _():
            zero = jnp.zeros((1, 1), F32)
            for which, src in enumerate((p_ref, q_ref)):
                base = pl.multiple_of((lax.rem(row, 2) ^ which) * half, half)
                for j in range(half // mb):
                    s = slice(j * mb, (j + 1) * mb)
                    d = pl.ds(base + j * mb, mb)
                    rc = hdot(src[s, :], r_ref[...], NT)
                    z = hdot(jnp.where(top, c_ref[d, 0:N], c1_ref[d, :]) - rc, m_ref[...], NT)
                    rc_ref[d, :] = rc
                    z_ref[d, :] = z
                    zero = zero + total(total(z * 0.0, 0), 1)
            f_ref[...] = jnp.where(zero == 0.0, 0.0, 1.0) + bad_ref[...] + before_ref[...]
            if nxt is not None:
                chain_init(lax.axis_index("col"), *ins[:2], st)
                outs[4][0:N, :] = ins[2][...]
                outs[4][2 * N:2 * N + NP, :] = ins[3][...]

        def piece(j):
            x = jnp.concatenate([c_ref[0:own, :], x_ref[...]], 0)
            lo = own if j == 0 else j * mb
            if j == 0:
                o_ref[0:own, :] = hdot(up_ref[...], x)
            s = slice(lo, (j + 1) * mb)
            o_ref[s, :] = c_ref[s, :] - hdot(z_ref[s, :], x)

        pieces = [functools.partial(piece, j) for j in range(cols // mb)]
        if nxt is None:
            weave([], pieces)
        else:
            @pl.when(lax.rem(i, 2) == 0)
            def _():
                chain_cols(lax.div(i, 2), st)
                weave([], pieces)

            @pl.when(lax.rem(i, 2) == 1)
            def _():
                weave(chain_update(lax.div(i, 2), st), pieces)

            @pl.when(i == steps - 1)
            def _():
                tts = (outs[4].at[pl.ds(N, N), :], outs[4].at[pl.ds(2 * N + NP, NP), :])
                chain_final(lax.axis_index("col"), st, (*outs[:4], *tts, outs[6]))

        @pl.when((i == 0) & top)
        def _():
            o_ref[0:own, 0:N] = pt_ref[...]
            o_ref[own:, 0:N] = rc_ref[own:, :]

    blk2 = pl.BlockSpec((cols, nb), lambda i: (0, i))
    fixed = lambda shape: pl.BlockSpec(shape, lambda i: (0, 0))
    consts = [psum, poth, c1, rinvt, minv, upt, ptt, bad, before] + extra
    more = CHAIN_SHAPES[:4] + [(2 * (N + NP), W)] + CHAIN_SHAPES[5:] if nxt is not None else []
    scratch = [(cols, N), (cols, N)] + (CHAIN_SCRATCH if nxt is not None else [])
    ns = len(scratch)
    return pl.pallas_call(
        body, grid=(steps,),
        in_specs=[blk2, pl.BlockSpec((own, nb), lambda i: (0, i))] + [fixed(a.shape) for a in consts],
        out_specs=[blk2, fixed(TILE)] + [fixed(s) for s in more],
        scratch_shapes=[pltpu.VMEM(s, F32) for s in scratch],
        out_shape=[jax.ShapeDtypeStruct(s, F32) for s in [(cols, rows), TILE] + more],
        cost_estimate=pl.CostEstimate(flops=12 * cols * rows * N, bytes_accessed=8 * cols * rows, transcendentals=0),
        compiler_params=pltpu.CompilerParams(vmem_limit_bytes=40 * 2**20))(ct, peer, *consts)


R1 = [(0, 1), (1, 0), (2, 3), (3, 2)]
R2 = [(0, 2), (2, 0), (1, 3), (3, 1)]
CY = [(0, 1), (1, 0)]


def row_major(x):
    def body(i_ref, o_ref):
        o_ref[...] = i_ref[...]

    return pl.pallas_call(body, out_shape=jax.ShapeDtypeStruct(x.shape, F32))(x)


def pick(x, i, axis=0):
    return lax.dynamic_slice_in_dim(x, i, 1, axis)


def row_sum(x):
    x = x + lax.ppermute(x, "row", R1)
    return x + lax.ppermute(x, "row", R2)


def factor_columns(stored):
    local_rows, local_blocks, width = stored.shape
    row_rank = lax.axis_index("row")
    col_rank = lax.axis_index("col")
    row_ids = row_rank * local_rows + jnp.arange(local_rows)
    col_ids = jnp.arange(width)
    edot = functools.partial(jnp.einsum, precision=HI, preferred_element_type=F32)

    def panel_step(panel_idx, state):
        stored, taus, tfs = state
        row_start = panel_idx * width
        local_idx = panel_idx // 2
        is_owner = col_rank == panel_idx % 2
        panel_in = pick(stored, local_idx, 1)[:, 0, :]

        def column_step(col_idx, loop_state):
            work, tau_vec = loop_state
            diag_idx = row_start + col_idx
            column = pick(work, col_idx, 1)[:, 0]
            below = jnp.where(row_ids >= diag_idx, column, 0.0)
            at_diag = (row_ids == diag_idx).astype(F32)
            summed = row_sum(edot("ar,rk->ak", jnp.stack([below, at_diag]), work))
            cross, diag_row = summed[0], summed[1]
            pivot = pick(diag_row, col_idx)[0]
            norm = jnp.sqrt(pick(cross, col_idx)[0])
            beta = -jnp.where(pivot >= 0, 1.0, -1.0) * norm
            tau = (beta - pivot) / beta
            denom = pivot - beta
            proj = jnp.where(col_ids > col_idx, (cross - beta * diag_row) / denom, 0.0)
            refl = jnp.where(row_ids > diag_idx, column / denom, 0.0) + at_diag
            work = work - tau * refl[:, None] * proj[None, :]
            new_col = jnp.where(row_ids < diag_idx, column, jnp.where(row_ids == diag_idx, beta, refl))
            work = lax.dynamic_update_slice_in_dim(work, new_col[:, None], col_idx, 1)
            return work, lax.dynamic_update_slice_in_dim(tau_vec, tau[None], col_idx, 0)

        work, tau_vec = loop(width, column_step, (panel_in, jnp.zeros((width,), F32)))
        diag_ids = row_start + col_ids[None, :]
        v_block = jnp.where(row_ids[:, None] == diag_ids, 1.0, jnp.where(row_ids[:, None] > diag_ids, work, 0.0))

        gram = row_sum(edot("ri,rj->ij", v_block, v_block))

        def t_step(col_idx, tf):
            g = pick(gram, col_idx, 1)[:, 0]
            g = jnp.where(col_ids < col_idx, g, 0.0)
            tau_k = pick(tau_vec, col_idx)[0]
            t_col = -tau_k * edot("ij,j->i", tf, g)
            t_col = jnp.where(col_ids == col_idx, tau_k, t_col)
            return lax.dynamic_update_slice_in_dim(tf, t_col[:, None], col_idx, 1)

        tf = loop(width, t_step, jnp.zeros((width, width), F32))
        v_mine = jnp.where(is_owner, v_block, 0.0)
        t_mine = jnp.where(is_owner, tf, 0.0)
        v_block = v_mine + lax.ppermute(v_mine, "col", CY)
        tf = t_mine + lax.ppermute(t_mine, "col", CY)

        def block_step(b, stored):
            blk = pick(stored, b, 1)[:, 0, :]
            w = edot("ij,ik->jk", tf, row_sum(edot("ri,rk->ik", v_block, blk)))
            upd = blk - edot("ri,ik->rk", v_block, w)
            keep = b * 2 + col_rank > panel_idx
            mine = (b == local_idx) & is_owner
            new = jnp.where(keep, upd, jnp.where(mine, work, blk))
            return lax.dynamic_update_slice_in_dim(stored, new[:, None, :], b, 1)

        stored = loop(local_blocks, block_step, stored)
        taus = lax.dynamic_update_slice_in_dim(taus, jnp.diagonal(tf), row_start, 0)
        return stored, taus, lax.dynamic_update_slice_in_dim(tfs, tf, row_start, 0)

    return loop(PANELS, panel_step, (stored, jnp.zeros((PANELS * width,), F32), jnp.zeros((PANELS * width, width), F32)))


def solution(mesh):
    def factor_both(a_matrix, b_matrix):
        local_rows, local_blocks, width = a_matrix.shape
        cols = local_blocks * width
        own = 2 * width
        col_rank = lax.axis_index("col")
        cts = [m.transpose(1, 2, 0).reshape(cols, local_rows) for m in (a_matrix, b_matrix)]

        pa, pb, c1a, c1b, pam, pao, pbm, g, x1, *first = exchange(*cts, own)
        c1a, c1b, pb = (pltpu.with_memory_space_constraint(x, pltpu.HBM) for x in (c1a, c1b, pb))
        across = lax.ppermute(pbm, "row", R2)
        out_a, bad_a, *second = apply_update(cts[0], pa, pam, pao, c1a, first, first[6], (g, x1), (first[4], first[5]))
        across, bad_a = lax.optimization_barrier((across, bad_a))
        pbm = pbm + across
        pbo = lax.ppermute(pbm, "row", R1)
        small = lax.ppermute(second[4], "col", [(0, 1)])
        out_b, bad = apply_update(cts[1], pb, pbm, pbo, c1b, second, bad_a)
        small, bad = lax.optimization_barrier((small, bad))
        tt = jnp.where(col_rank == 0, second[4], small)

        def parts(tt):
            return tt[:N], tt[N:2 * N], *(x.reshape(N) for x in jnp.split(tt[2 * N:], 2))

        carry = (bad, lax.ppermute(bad, "col", CY), *parts(tt), out_a, out_b)

        def redo(state):
            def one(i, done):
                st, taus, tfs = factor_columns(jnp.where(i == 0, a_matrix, b_matrix))
                new = (st.transpose(1, 2, 0).reshape(cols, local_rows), jnp.concatenate([tfs, taus.reshape(PANELS, width)], 0))
                return tuple(jnp.where(i == k, n, d) for k, pair in enumerate((done[:2], done[2:])) for n, d in zip(new, pair))

            blank = jnp.zeros((N + PANELS, width), F32)
            st_a, tt_a, st_b, tt_b = loop(2, one, (state[6], blank, state[7], blank))
            tt = row_major(jnp.concatenate([tt_a[:N], tt_b[:N], tt_a[N:], tt_b[N:]], 0))
            return jnp.zeros(TILE, F32), jnp.zeros(TILE, F32), *(row_major(x) for x in parts(tt)), st_a, st_b

        res = lax.while_loop(lambda s: jnp.max(s[0] + s[1]) > 0.5, redo, carry)
        back = lambda x: x.reshape(local_blocks, width, local_rows).transpose(2, 0, 1)
        stack = lambda x: x.reshape(PANELS, width, width)
        return back(res[6]), res[4], stack(res[2]), back(res[7]), res[5], stack(res[3])

    spec_mat = P(("batch", "row"), "col", None)
    spec_out = (spec_mat, P("batch"), P("batch", None, None))
    return jax.shard_map(factor_both, mesh=mesh, in_specs=(spec_mat, spec_mat), out_specs=spec_out + spec_out, check_vma=False)
```

```python
import functools

import jax
import jax.numpy as jnp
from jax import lax
from jax.experimental import pallas as pl
from jax.experimental.pallas import tpu as pltpu
from jax.sharding import PartitionSpec as P

F32 = jnp.float32
BF = jnp.bfloat16
HI = lax.Precision.HIGHEST
PANELS = 4
W = 64
NP = 4
N = 256
NN = (((1,), (0,)), ((), ()))
NT = (((1,), (1,)), ((), ()))
TN = (((0,), (0,)), ((), ()))


BOTH = (0, 1)
total = functools.partial(jnp.sum, keepdims=True)
peak = functools.partial(jnp.max, keepdims=True)
TILE = (8, 128)


def rows_of(shape):
    return lax.broadcasted_iota(jnp.int32, shape, 0)


def lanes_of(shape):
    return lax.broadcasted_iota(jnp.int32, shape, 1)


def hdot(a, b, dn=NN):
    return lax.dot_general(a, b, dn, precision=HI, preferred_element_type=F32)


AMPLIFY = 64.0
HUGE = 1e9


def diag_factor(mats, group):
    tiles = W // 8
    lane8 = lanes_of(TILE)
    sub8 = rows_of(TILE)
    r64 = rows_of((W, W))
    c64 = lanes_of((W, W))
    eye = (r64 == c64).astype(F32)
    full = lambda x: jnp.broadcast_to(x, TILE)
    zeros = jnp.zeros(TILE, F32)
    st = []
    for hpp, ypp in mats:
        he = jnp.concatenate([hpp, eye], 1)
        yw = jnp.concatenate([ypp, eye], 1)
        st.append(dict(he=[he[8 * g:8 * g + 8] for g in range(tiles)], yw=[yw[8 * g:8 * g + 8] for g in range(tiles)],
                       l=[zeros] * tiles, u=[zeros] * tiles, tau=zeros))
    for k0 in range(0, W, group):
        gk = k0 // 8
        for s in st:
            s['bh'] = [[full(s['he'][g][:, k:k + 1]) for g in range(gk, tiles)] for k in range(k0, k0 + group)]
            s['by'] = [[full(s['yw'][g][:, k:k + 1]) for g in range(tiles)] for k in range(k0, k0 + group)]
        for k in range(k0, k0 + group):
            sk = k - 8 * gk
            isk = sub8 == sk
            for s in st:
                ch, cy = s['bh'][k - k0], s['by'][k - k0]
                pick = lambda x: full(x[sk:sk + 1, :])
                h = pick(ch[0])
                a = pick(cy[gk])
                rs = lax.rsqrt(h)
                rinv = jnp.where(a >= 0, -rs, rs)
                ukk = a - h * rinv
                uinv = 1.0 / ukk
                r = pick(s['he'][gk]) * rinv
                u = pick(s['yw'][gk]) - jnp.where((lane8 >= k) & (lane8 < W), r, 0.0)
                un = u * uinv
                rr = r * rinv
                for k2 in range(k + 1, k0 + group):
                    r2 = pick(s['bh'][k2 - k0][0]) * rinv
                    un2 = (pick(s['by'][k2 - k0][gk]) - r2) * uinv
                    rr2 = r2 * rinv
                    s['bh'][k2 - k0] = [x - ch[i] * rr2 for i, x in enumerate(s['bh'][k2 - k0])]
                    nby = [x - cy[i] * un2 for i, x in enumerate(s['by'][k2 - k0])]
                    nby[gk] = jnp.where(isk, un2, nby[gk])
                    s['by'][k2 - k0] = nby
                for g in range(gk, tiles):
                    new = s['he'][g] - ch[g - gk] * rr
                    lc = cy[g] * uinv
                    if g == gk:
                        new = jnp.where(sub8 > sk, new, jnp.where(isk, r, s['he'][g]))
                        lc = jnp.where(sub8 > sk, lc, 0.0)
                    s['he'][g] = new
                    s['l'][g] = jnp.where(lane8 == k, lc, s['l'][g])
                for g in range(tiles):
                    new = s['yw'][g] - cy[g] * un
                    s['yw'][g] = jnp.where(isk, un, new) if g == gk else new
                s['u'][gk] = jnp.where(isk, u, s['u'][gk])
                s['tau'] = jnp.where(lane8 == k, -ukk * rinv, s['tau'])
    out = []
    up = c64 >= r64
    for s in st:
        he = jnp.concatenate(s['he'], 0)
        yw = jnp.concatenate(s['yw'], 0)
        l = jnp.concatenate(s['l'], 0)[:, :W]
        u = jnp.concatenate(s['u'], 0)[:, :W]
        out.append((jnp.where(c64 <= r64, he[:, W:], 0.0), l + eye, jnp.where(up, u, 0.0), yw[:, W:], s['tau'][0:1, :W]))
    return out


def blk(b):
    return slice(b * W, (b + 1) * W)


def order(c):
    return [2 * l + c for l in BOTH] + [2 * l + 1 - c for l in BOTH]


def turn(x):
    return jnp.concatenate([x[:, W:N], x[:, :W], x[:, N:]], 1)


CHAIN_SCRATCH = [(N, 2 * N), (N, 2 * N), (N, N), (NP, 4, W, W), (8, N), (NP, W)]
CHAIN_SHAPES = [(N, N), (N, N), (2 * W, N), (2 * W, N), (N, W), (NP, W), TILE]


def chain_init(col, g, x1, st):
    hs, ys, ls, _, norm, _ = st
    ri, ci = rows_of((N, N)), lanes_of((N, N))
    eye = (ri == ci).astype(F32)
    for c in BOTH:
        @pl.when(col == c)
        def _():
            for i, b in enumerate(order(c)):
                ls[blk(b), :] = x1[blk(i), :]
                for i2, b2 in enumerate(order(c)):
                    hs[blk(b), blk(b2)] = g[blk(i), blk(i2)]
    hs[:, N:] = eye
    ys[:, :N] = ls[...].T
    ys[:, N:] = eye
    dg = jnp.where(ri == ci, hs[:, :N], 0.0)
    norm[...] = jnp.broadcast_to(jnp.sqrt(total(dg, 0)), (8, N))


def chain_cols(p, st, group):
    hs, ys, _, fac, _, tv = st
    e, l, u, w, tau = diag_factor([(hs[0:W, 0:W], ys[0:W, 0:W])], group)[0]
    for i, x in enumerate((e, l, u, w)):
        fac[p, i] = x
    tv[pl.ds(p, 1), :] = tau


def chain_update(p, st):
    hs, ys, ls, fac, _, _ = st
    rw = rows_of((W, 2 * N))
    cw = lanes_of((W, 2 * N))
    rl = rows_of((N - W, W))
    live = N - p * W
    e, l, w = fac[p, 0], fac[p, 1], fac[p, 3]
    rall = hdot(e, hs[0:W, :])
    rall = jnp.where((cw >= N) | ((cw >= rw) & (cw < live)), rall, 0.0)
    wl = hdot(w, l)
    yield
    yc = ys[W:, 0:W]
    nrow = hdot(w, ys[0:W, :] - jnp.where(cw < N, rall, 0.0))
    hnew = hs[W:, :] - hdot(rall[:, W:N], rall, TN)
    hs[0:N - W, :] = turn(hnew)
    hs[N - W:, :] = turn(rall)
    lnew = jnp.where(rl < live - W, hdot(yc, wl), 0.0)
    rest = ls[W:, W:]
    first = ls[0:W, W:]
    ls[0:N - W, N - W:] = lnew
    ls[N - W:, N - W:] = l
    ls[0:N - W, 0:N - W] = rest
    ls[N - W:, 0:N - W] = first
    yield
    ynew = ys[W:, :] - hdot(yc, nrow)
    ys[0:N - W, :] = turn(ynew)
    ys[N - W:, :] = turn(nrow)


def weave(stages, pieces):
    stages = iter(stages)
    for piece in pieces:
        next(stages, None)
        piece()
    for _ in stages:
        pass


def chain_final(col, st, outs):
    hs, ys, ls, fac, norm, tv = st
    rinvt, minv, upt, ptt, tfac, tau, bad = outs
    r64 = rows_of((W, W))
    c64 = lanes_of((W, W))
    tau[...] = tv[...]
    for p in range(NP):
        e, _, u, w = [fac[p, i] for i in range(4)]
        t = -hdot(hdot(u, e, NT), hdot(u, w), NT)
        tfac[blk(p), :] = jnp.where(c64 > r64, t, jnp.where(c64 == r64, jnp.broadcast_to(tv[p:p + 1, :], (W, W)), 0.0))
    ri = rows_of((N, N))
    ci = lanes_of((N, N))
    rt, mi = hs[:, N:], ys[:, N:]
    g = norm[0:1, :]
    c1 = peak(total(jnp.abs(rt) * g, 1))
    c2 = peak(hdot(g, jnp.abs(mi)))
    good = (c1 <= AMPLIFY) & (c2 <= AMPLIFY) & (-peak(-g) >= 1 / HUGE) & (peak(g) <= HUGE)
    bad[...] = jnp.broadcast_to(jnp.where(good, 0.0, 1.0), TILE)
    pt = jnp.where(ri > ci, ls[...], hs[:, :N]).T
    ut = lax.dot_general(ls[...], mi, (((0,), (1,)), ((), ())), precision=HI, preferred_element_type=F32)
    hs[:, :N] = pt
    ys[:, :N] = ut
    for c in BOTH:
        @pl.when(col == c)
        def _():
            for i, b in enumerate(order(c)):
                rinvt[:, blk(i)] = hs[:, N + b * W:N + (b + 1) * W]
                minv[blk(i), :] = ys[blk(b), N:]
            for i in BOTH:
                b = order(c)[i]
                ptt[blk(i), :] = hs[blk(b), :N]
                for i2, b2 in enumerate(order(c)):
                    upt[blk(i), blk(i2)] = ys[blk(b), blk(b2)]


SPLITS = range(3)
loop = functools.partial(lax.fori_loop, 0)


def split3(x):
    h = x.astype(BF)
    r = x - h.astype(F32)
    m = r.astype(BF)
    return h, m, (r - m.astype(F32)).astype(BF)


def dot6(a, b, dn):
    d = lambda i, j: lax.dot_general(a[i], b[j], dn, preferred_element_type=F32)
    return (((d(2, 0) + d(0, 2)) + d(1, 1)) + (d(1, 0) + d(0, 1))) + d(0, 0)


CHUNK = 960
PIECE = 480
HALF = 512
SPAN = 1024
SLOTS = 3
AHEAD = SLOTS - 1


def exchange_kernel(ca, cb, peer_a, peer_b, c1a, c1b, pam, pao, pbm, g_out, x1b, *refs):
    outs, refs = refs[:len(CHAIN_SHAPES)], refs[len(CHAIN_SHAPES):]
    st, refs = refs[:len(CHAIN_SCRATCH)], refs[len(CHAIN_SCRATCH):]
    (x1a, peer, own, xo, xs, cbuf, acc, gacc, r1buf, r2buf, gbuf1, gsum, gbuf2, gfull,
     c_sem, own_sem, out_sem, y_send, y_recv, top_send, top_recv, swap_send, swap_recv,
     g_send, g_recv, p_send, p_recv, x_send, x_recv) = refs
    cts, x1 = (ca, cb), (x1a, x1b)
    row = lax.axis_index("row")
    col = lax.axis_index("col")
    core = lax.rem(row, 2)
    mate = row + 1 - 2 * core
    across = lax.rem(row + 2, 4)
    diag = lax.rem(row + 3 - 2 * core, 4)
    cols, rows = ca.shape
    half = cols // 2
    nown = peer.shape[1]
    nchunk = (cols - nown) // CHUNK
    spans = rows // SPAN
    trips = nchunk * spans

    def remote(src, dst, send, recv, **where):
        return pltpu.make_async_remote_copy(src_ref=src, dst_ref=dst, send_sem=send, recv_sem=recv,
                                            device_id=where, device_id_type=pl.DeviceIdType.MESH)

    to_mate = functools.partial(remote, row=mate)
    to_across = functools.partial(remote, row=across)

    def c_copy(m, t):
        slot = lax.rem(m * trips + t, SLOTS)
        h, j = lax.div(t, nchunk), lax.rem(t, nchunk)
        return pltpu.make_async_copy(
            cts[m].at[pl.ds(pl.multiple_of(nown + j * CHUNK, 64), CHUNK), pl.ds(pl.multiple_of(h * SPAN, SPAN), SPAN)],
            cbuf.at[slot], c_sem.at[slot])

    first = pl.ds(0, nown)
    second = pl.ds(nown, nown)
    lanes = pl.ds(0, N)

    def y_copy(m, h):
        s = pl.ds(pl.multiple_of(h * SPAN, SPAN), SPAN)
        i = m * spans + h
        return remote(cts[m].at[first, s], peer.at[m, :, s], y_send.at[i], y_recv.at[i], col=1 - col)

    def half_slot(u):
        return lax.rem(2 * trips - nchunk + u, SLOTS)

    def c_half(u):
        q, j = lax.div(u, nchunk), lax.rem(u, nchunk)
        return pltpu.make_async_copy(
            cb.at[pl.ds(pl.multiple_of(nown + j * CHUNK, 64), CHUNK), pl.ds(pl.multiple_of(rows - SPAN + q * HALF, HALF), HALF)],
            cbuf.at[half_slot(u), :, pl.ds(0, HALF)], c_sem.at[half_slot(u)])

    def y_half(q):
        s = pl.ds(pl.multiple_of(rows - SPAN + q * HALF, HALF), HALF)
        i = 2 * spans - 1 + q
        return remote(cb.at[first, s], peer.at[1, :, s], y_send.at[i], y_recv.at[i], col=1 - col)

    own_copies = [pltpu.make_async_copy(cts[m].at[first, :], own.at[m], own_sem.at[m]) for m in BOTH]
    for o in own_copies:
        o.start()
    for t in range(AHEAD):
        c_copy(0, t).start()

    for m in BOTH:
        acc[m, 0:nown, :] = jnp.zeros((nown, N), F32)
    barrier = pltpu.get_barrier_semaphore()
    for where in (dict(row=mate), dict(row=across), dict(row=diag), dict(col=1 - col)):
        pl.semaphore_signal(barrier, device_id=where, device_id_type=pl.DeviceIdType.MESH)
    pl.semaphore_wait(barrier, 4)

    ys = [y_copy(m, h) for m in BOTH for h in range(spans - m)] + [y_half(q) for q in BOTH]
    for y in ys:
        y.start()

    tops = (c1a, c1b)
    lows = [pl.ds(0, half), pl.ds(half, half)]
    x_local = [pltpu.make_async_copy(cts[m].at[first, lanes], x1[m].at[first, :], own_sem.at[2 + m]) for m in BOTH]
    x_own = [[remote(cts[m].at[first, lanes], x1[m].at[first, :], top_send.at[m, k], top_recv.at[m], row=k + 1)
              for k in SPLITS] for m in BOTH]
    x_peer = [[remote(peer.at[m, :, lanes], x1[m].at[second, :], top_send.at[2 + m, k], top_recv.at[2 + m], row=k + 1)
               for k in SPLITS] for m in BOTH]
    top_far = [[remote(cts[m].at[:, lanes], tops[m], top_send.at[4 + m, 0], top_recv.at[4 + m], row=1)]
               + [remote(cts[m].at[lows[k], lanes], tops[m].at[lows[k], :], top_send.at[4 + m, 1 + k], top_recv.at[4 + m], row=2 + k)
                  for k in BOTH] for m in BOTH]

    @pl.when(row == 0)
    def _():
        for m in BOTH:
            x_local[m].start()
        for c in x_own[0] + x_own[1] + top_far[0] + top_far[1]:
            c.start()

    mine = pl.ds(pl.multiple_of(core * half, half), half)
    others = pl.ds(pl.multiple_of((1 - core) * half, half), half)
    g_mine = pl.ds(pl.multiple_of(core * nown, nown), nown)
    g_theirs = pl.ds(pl.multiple_of((1 - core) * nown, nown), nown)
    p1 = [to_mate(acc.at[m, others, :], r1buf.at[m], p_send.at[m], p_recv.at[m]) for m in BOTH]
    g1 = [to_mate(gacc.at[m, g_theirs, :], gbuf1.at[m], g_send.at[m], g_recv.at[m]) for m in BOTH]
    g2 = [to_across(gsum.at[m], gbuf2.at[m], g_send.at[2 + m], g_recv.at[2 + m]) for m in BOTH]
    g3 = [to_mate(full.at[g_mine, :], full.at[g_mine, :], g_send.at[4 + m], g_recv.at[4 + m]) for m, full in enumerate((gfull, g_out))]
    p2 = to_across(r1buf.at[0], r2buf, x_send.at[0], x_recv.at[0])
    p3 = to_mate(r1buf.at[0], pao, x_send.at[1], x_recv.at[1])
    swap = [to_mate(tops[m].at[mine, :], tops[m].at[mine, :], swap_send.at[m], swap_recv.at[m]) for m in BOTH]
    peer_out = [pltpu.make_async_copy(peer.at[m], (peer_a, peer_b)[m], out_sem.at[m]) for m in BOTH]
    pam_out = pltpu.make_async_copy(r1buf.at[0], pam, out_sem.at[2])

    def add_half(m):
        p1[m].wait()
        r1buf[m] = r1buf[m] + acc[m, mine, :]

    def finish_g1(m):
        g1[m].wait()
        gsum[m] = gacc[m, g_mine, :] + gbuf1[m]
        g2[m].start()

    def finish_g2(m, full):
        g2[m].wait()
        full[g_mine, :] = gsum[m] + gbuf2[m]
        g3[m].start()

    def send_x(m):
        @pl.when(row == 0)
        def _():
            x1[m][nown:, :] = peer[m, :, 0:N]
            for c in x_peer[m]:
                c.start()

    def wait_x(m):
        @pl.when(row == 0)
        def _():
            x_local[m].wait()

        @pl.when(row > 0)
        def _():
            x_own[m][0].wait_recv()
            x_peer[m][0].wait_recv()

    def begin_chain():
        wait_x(0)
        g3[0].wait()
        chain_init(col, gfull, x1a, st)

    def top_rows():
        @pl.when(row == 1)
        def _():
            for m in BOTH:
                top_far[m][0].wait_recv()

        @pl.when(row >= 2)
        def _():
            for m in BOTH:
                top_far[m][1].wait_recv()
                swap[m].start()

    def last_sums_a():
        p2.wait()
        r1buf[0] = r1buf[0] + r2buf[...]
        p3.start()
        pam_out.start()

    last = trips - nchunk
    begin = 1
    hooks = [[(0, lambda: send_x(0)), (last, lambda: finish_g1(0))],
             [(begin - 1, begin_chain), (begin, lambda: send_x(1)), (last - 1, last_sums_a), (last - 1, top_rows)]]

    def split_own(m):
        def build(q, _):
            s = pl.ds(pl.multiple_of(q * HALF, HALF), HALF)
            for i, part in enumerate(split3(own[m, :, s])):
                xo[m, i, :, s] = part
            return 0

        own_copies[m].wait()
        loop(rows // HALF, build, 0)

    def panel(m, s0, width):
        return [jnp.concatenate([xo[m, i, :, pl.ds(s0, width)], xs[i, :, 0:width]], 0) for i in SPLITS]

    def head(m, s0, width):
        for q in range(width // HALF):
            d = slice(q * HALF, (q + 1) * HALF)
            for i, part in enumerate(split3(peer[m, :, pl.ds(s0 + q * HALF, HALF)])):
                xs[i, :, d] = part
        x = panel(m, s0, width)
        return dot6(x, x, NT)

    def trip(m, j, slot, s0, width, fresh):
        x = panel(m, s0, width)
        for i in range(CHUNK // PIECE):
            r = dot6(split3(cbuf[slot, i * PIECE:(i + 1) * PIECE, 0:width]), x, NT)
            d = pl.ds(pl.multiple_of(nown + j * CHUNK + i * PIECE, 32), PIECE)
            acc[m, d, :] = jnp.where(fresh, r, acc[m, d, :] + r)

    def products(m, count):
        def span(h, _):
            y_copy(m, h).wait_recv()
            s0 = pl.multiple_of(h * SPAN, SPAN)
            r = head(m, s0, SPAN)
            gacc[m] = jnp.where(h == 0, r, gacc[m] + r)

            if m == 0:
                @pl.when(h == spans - 1)
                def _():
                    g1[0].start()

            def step(j, _):
                t = h * nchunk + j
                slot = lax.rem(m * trips + t, SLOTS)
                c_copy(m, t).wait()
                ahead = t + AHEAD - count * nchunk

                @pl.when(ahead < 0)
                def _():
                    c_copy(m, t + AHEAD).start()

                @pl.when(ahead >= 0)
                def _():
                    (c_copy(1, ahead) if m == 0 else c_half(ahead)).start()

                run = functools.partial(trip, m, j, slot, s0, SPAN, h == 0)
                if m == 0:
                    run()
                else:
                    live = (t >= begin) & (t < begin + NP)

                    @pl.when(live)
                    def _():
                        chain_cols(t - begin, st, 8)
                        run()
                        weave(chain_update(t - begin, st), [])

                    pl.when(~live)(run)
                for at, hook in hooks[m]:
                    pl.when(t == at)(hook)
                return 0

            loop(nchunk, step, 0)
            return 0

        loop(count, span, 0)

    def last_span():
        def span(q, _):
            y_half(q).wait_recv()
            s0 = pl.multiple_of(rows - SPAN + q * HALF, HALF)
            gacc[1] = gacc[1] + head(1, s0, HALF)

            @pl.when(q == 1)
            def _():
                g1[1].start()

            def step(j, _):
                u = q * nchunk + j
                c_half(u).wait()

                @pl.when(u + AHEAD < 2 * nchunk)
                def _():
                    c_half(u + AHEAD).start()

                trip(1, j, half_slot(u), s0, HALF, False)

                @pl.when(u == nchunk)
                def _():
                    finish_g1(1)

                return 0

            loop(nchunk, step, 0)
            return 0

        loop(2, span, 0)

    for m in BOTH:
        split_own(m)
    products(0, spans)
    p1[0].start()
    peer_out[0].start()
    add_half(0)
    p2.start()
    finish_g2(0, gfull)
    products(1, spans - 1)
    last_span()
    p1[1].start()
    peer_out[1].start()
    wait_x(1)
    chain_final(col, st, outs)
    p1[1].wait()
    pbm[...] = r1buf[1] + acc[1, mine, :]
    finish_g2(1, g_out)
    g3[1].wait()

    @pl.when(row == 0)
    def _():
        for c in x_own[0] + x_own[1] + x_peer[0] + x_peer[1] + top_far[0] + top_far[1]:
            c.wait_send()

    @pl.when(row >= 2)
    def _():
        for m in BOTH:
            swap[m].wait()

    for c in peer_out + [p3, pam_out]:
        c.wait()
    for y in ys:
        y.wait_send()


def exchange(ca, cb, own):
    cols, rows = ca.shape
    half = cols // 2
    hbm = pl.BlockSpec(memory_space=pl.ANY)
    vm = pl.BlockSpec(memory_space=pltpu.VMEM)
    dma = pltpu.SemaphoreType.DMA
    pair = (2, N, N)
    ny = 2 * rows // SPAN + 1
    shapes = [(own, rows)] * 2 + [(cols, N)] * 2 + [(half, N)] * 3 + [(N, N), (N, N)] + CHAIN_SHAPES
    scratch = CHAIN_SCRATCH + [(N, N), (2, own, rows), (2, own, rows)]
    after = [(SLOTS, CHUNK, SPAN), (2, cols, N), pair, (2, half, N), (half, N)] + [(2, own, N)] * 3 + [(N, N)]
    return pl.pallas_call(
        exchange_kernel,
        in_specs=[hbm, hbm],
        out_specs=[hbm] * 6 + [vm] * (3 + len(CHAIN_SHAPES)),
        out_shape=[jax.ShapeDtypeStruct(s, F32) for s in shapes],
        scratch_shapes=[pltpu.VMEM(s, F32) for s in scratch] + [pltpu.VMEM((2, 3, own, rows), BF), pltpu.VMEM((3, own, SPAN), BF)]
        + [pltpu.VMEM(s, F32) for s in after]
        + [dma(n) for n in ((SLOTS,), (4,), (4,), (ny,), (ny,), (6, 3), (6,), (2,), (2,), (6,), (6,), (2,), (2,), (2,), (2,))],
        cost_estimate=pl.CostEstimate(flops=24 * cols * rows * N, bytes_accessed=8 * cols * rows, transcendentals=0),
        compiler_params=pltpu.CompilerParams(vmem_limit_bytes=46 * 2**20, collective_id=0, has_side_effects=True))(ca, cb)


def apply_update(ct, peer, psum, poth, c1, small, before, nxt=None, past=()):
    cols, rows = ct.shape
    nb = 512
    mb = 512
    own = peer.shape[0]
    half = cols // 2
    steps = rows // nb
    rinvt, minv, upt, ptt, _, _, bad = small
    no = len(CHAIN_SHAPES)
    extra = list(nxt or ()) + list(past)
    ne = len(extra)

    def body(c_ref, x_ref, p_ref, q_ref, c1_ref, r_ref, m_ref, up_ref, pt_ref, bad_ref, before_ref, *refs):
        ins, (o_ref, f_ref) = refs[:ne], refs[ne:ne + 2]
        outs, (z_ref, rc_ref, *st) = refs[ne + 2:len(refs) - ns], refs[len(refs) - ns:]
        i = pl.program_id(0)
        row = lax.axis_index("row")
        top = row == 0

        @pl.when(i == 0)
        def _():
            zero = jnp.zeros((1, 1), F32)
            for which, src in enumerate((p_ref, q_ref)):
                base = pl.multiple_of((lax.rem(row, 2) ^ which) * half, half)
                for j in range(half // mb):
                    s = slice(j * mb, (j + 1) * mb)
                    d = pl.ds(base + j * mb, mb)
                    rc = hdot(src[s, :], r_ref[...], NT)
                    z = hdot(jnp.where(top, c_ref[d, 0:N], c1_ref[d, :]) - rc, m_ref[...], NT)
                    rc_ref[d, :] = rc
                    z_ref[d, :] = z
                    zero = zero + total(total(z * 0.0, 0), 1)
            f_ref[...] = jnp.where(zero == 0.0, 0.0, 1.0) + bad_ref[...] + before_ref[...]
            if nxt is not None:
                chain_init(lax.axis_index("col"), *ins[:2], st)
                outs[4][0:N, :] = ins[2][...]
                outs[4][2 * N:2 * N + NP, :] = ins[3][...]

        def piece(j):
            x = jnp.concatenate([c_ref[0:own, :], x_ref[...]], 0)
            lo = own if j == 0 else j * mb
            if j == 0:
                o_ref[0:own, :] = hdot(up_ref[...], x)
            s = slice(lo, (j + 1) * mb)
            o_ref[s, :] = c_ref[s, :] - hdot(z_ref[s, :], x)

        pieces = [functools.partial(piece, j) for j in range(cols // mb)]
        if nxt is None:
            weave([], pieces)
        else:
            @pl.when(lax.rem(i, 2) == 0)
            def _():
                chain_cols(lax.div(i, 2), st, 4)
                weave([], pieces)

            @pl.when(lax.rem(i, 2) == 1)
            def _():
                weave(chain_update(lax.div(i, 2), st), pieces)

            @pl.when(i == steps - 1)
            def _():
                tts = (outs[4].at[pl.ds(N, N), :], outs[4].at[pl.ds(2 * N + NP, NP), :])
                chain_final(lax.axis_index("col"), st, (*outs[:4], *tts, outs[6]))

        @pl.when((i == 0) & top)
        def _():
            o_ref[0:own, 0:N] = pt_ref[...]
            o_ref[own:, 0:N] = rc_ref[own:, :]

    blk2 = pl.BlockSpec((cols, nb), lambda i: (0, i))
    fixed = lambda shape: pl.BlockSpec(shape, lambda i: (0, 0))
    consts = [psum, poth, c1, rinvt, minv, upt, ptt, bad, before] + extra
    more = CHAIN_SHAPES[:4] + [(2 * (N + NP), W)] + CHAIN_SHAPES[5:] if nxt is not None else []
    scratch = [(cols, N), (cols, N)] + (CHAIN_SCRATCH if nxt is not None else [])
    ns = len(scratch)
    return pl.pallas_call(
        body, grid=(steps,),
        in_specs=[blk2, pl.BlockSpec((own, nb), lambda i: (0, i))] + [fixed(a.shape) for a in consts],
        out_specs=[blk2, fixed(TILE)] + [fixed(s) for s in more],
        scratch_shapes=[pltpu.VMEM(s, F32) for s in scratch],
        out_shape=[jax.ShapeDtypeStruct(s, F32) for s in [(cols, rows), TILE] + more],
        cost_estimate=pl.CostEstimate(flops=12 * cols * rows * N, bytes_accessed=8 * cols * rows, transcendentals=0),
        compiler_params=pltpu.CompilerParams(vmem_limit_bytes=40 * 2**20))(ct, peer, *consts)


R1 = [(0, 1), (1, 0), (2, 3), (3, 2)]
R2 = [(0, 2), (2, 0), (1, 3), (3, 1)]
CY = [(0, 1), (1, 0)]


def row_major(x):
    def body(i_ref, o_ref):
        o_ref[...] = i_ref[...]

    return pl.pallas_call(body, out_shape=jax.ShapeDtypeStruct(x.shape, F32))(x)


def pick(x, i, axis=0):
    return lax.dynamic_slice_in_dim(x, i, 1, axis)


def row_sum(x):
    x = x + lax.ppermute(x, "row", R1)
    return x + lax.ppermute(x, "row", R2)


def factor_columns(stored):
    local_rows, local_blocks, width = stored.shape
    row_rank = lax.axis_index("row")
    col_rank = lax.axis_index("col")
    row_ids = row_rank * local_rows + jnp.arange(local_rows)
    col_ids = jnp.arange(width)
    edot = functools.partial(jnp.einsum, precision=HI, preferred_element_type=F32)

    def panel_step(panel_idx, state):
        stored, taus, tfs = state
        row_start = panel_idx * width
        local_idx = panel_idx // 2
        is_owner = col_rank == panel_idx % 2
        panel_in = pick(stored, local_idx, 1)[:, 0, :]

        def column_step(col_idx, loop_state):
            work, tau_vec = loop_state
            diag_idx = row_start + col_idx
            column = pick(work, col_idx, 1)[:, 0]
            below = jnp.where(row_ids >= diag_idx, column, 0.0)
            at_diag = (row_ids == diag_idx).astype(F32)
            summed = row_sum(edot("ar,rk->ak", jnp.stack([below, at_diag]), work))
            cross, diag_row = summed[0], summed[1]
            pivot = pick(diag_row, col_idx)[0]
            norm = jnp.sqrt(pick(cross, col_idx)[0])
            beta = -jnp.where(pivot >= 0, 1.0, -1.0) * norm
            tau = (beta - pivot) / beta
            denom = pivot - beta
            proj = jnp.where(col_ids > col_idx, (cross - beta * diag_row) / denom, 0.0)
            refl = jnp.where(row_ids > diag_idx, column / denom, 0.0) + at_diag
            work = work - tau * refl[:, None] * proj[None, :]
            new_col = jnp.where(row_ids < diag_idx, column, jnp.where(row_ids == diag_idx, beta, refl))
            work = lax.dynamic_update_slice_in_dim(work, new_col[:, None], col_idx, 1)
            return work, lax.dynamic_update_slice_in_dim(tau_vec, tau[None], col_idx, 0)

        work, tau_vec = loop(width, column_step, (panel_in, jnp.zeros((width,), F32)))
        diag_ids = row_start + col_ids[None, :]
        v_block = jnp.where(row_ids[:, None] == diag_ids, 1.0, jnp.where(row_ids[:, None] > diag_ids, work, 0.0))

        gram = row_sum(edot("ri,rj->ij", v_block, v_block))

        def t_step(col_idx, tf):
            g = pick(gram, col_idx, 1)[:, 0]
            g = jnp.where(col_ids < col_idx, g, 0.0)
            tau_k = pick(tau_vec, col_idx)[0]
            t_col = -tau_k * edot("ij,j->i", tf, g)
            t_col = jnp.where(col_ids == col_idx, tau_k, t_col)
            return lax.dynamic_update_slice_in_dim(tf, t_col[:, None], col_idx, 1)

        tf = loop(width, t_step, jnp.zeros((width, width), F32))
        v_mine = jnp.where(is_owner, v_block, 0.0)
        t_mine = jnp.where(is_owner, tf, 0.0)
        v_block = v_mine + lax.ppermute(v_mine, "col", CY)
        tf = t_mine + lax.ppermute(t_mine, "col", CY)

        def block_step(b, stored):
            blk = pick(stored, b, 1)[:, 0, :]
            w = edot("ij,ik->jk", tf, row_sum(edot("ri,rk->ik", v_block, blk)))
            upd = blk - edot("ri,ik->rk", v_block, w)
            keep = b * 2 + col_rank > panel_idx
            mine = (b == local_idx) & is_owner
            new = jnp.where(keep, upd, jnp.where(mine, work, blk))
            return lax.dynamic_update_slice_in_dim(stored, new[:, None, :], b, 1)

        stored = loop(local_blocks, block_step, stored)
        taus = lax.dynamic_update_slice_in_dim(taus, jnp.diagonal(tf), row_start, 0)
        return stored, taus, lax.dynamic_update_slice_in_dim(tfs, tf, row_start, 0)

    return loop(PANELS, panel_step, (stored, jnp.zeros((PANELS * width,), F32), jnp.zeros((PANELS * width, width), F32)))


def solution(mesh):
    def factor_both(a_matrix, b_matrix):
        local_rows, local_blocks, width = a_matrix.shape
        cols = local_blocks * width
        own = 2 * width
        col_rank = lax.axis_index("col")
        cts = [m.transpose(1, 2, 0).reshape(cols, local_rows) for m in (a_matrix, b_matrix)]

        pa, pb, c1a, c1b, pam, pao, pbm, g, x1, *first = exchange(*cts, own)
        c1a, c1b, pb = (pltpu.with_memory_space_constraint(x, pltpu.HBM) for x in (c1a, c1b, pb))
        across = lax.ppermute(pbm, "row", R2)
        out_a, bad_a, *second = apply_update(cts[0], pa, pam, pao, c1a, first, first[6], (g, x1), (first[4], first[5]))
        across, bad_a = lax.optimization_barrier((across, bad_a))
        pbm = pbm + across
        pbo = lax.ppermute(pbm, "row", R1)
        small = lax.ppermute(second[4], "col", CY)
        out_b, bad = apply_update(cts[1], pb, pbm, pbo, c1b, second, bad_a)
        small, bad = lax.optimization_barrier((small, bad))
        tt = jnp.where(col_rank == 0, second[4], small)

        def parts(tt):
            return tt[:N], tt[N:2 * N], *(x.reshape(N) for x in jnp.split(tt[2 * N:], 2))

        carry = (bad, lax.ppermute(bad, "col", CY), *parts(tt), out_a, out_b)

        def redo(state):
            def one(i, done):
                st, taus, tfs = factor_columns(jnp.where(i == 0, a_matrix, b_matrix))
                new = (st.transpose(1, 2, 0).reshape(cols, local_rows), jnp.concatenate([tfs, taus.reshape(PANELS, width)], 0))
                return tuple(jnp.where(i == k, n, d) for k, pair in enumerate((done[:2], done[2:])) for n, d in zip(new, pair))

            blank = jnp.zeros((N + PANELS, width), F32)
            st_a, tt_a, st_b, tt_b = loop(2, one, (state[6], blank, state[7], blank))
            tt = row_major(jnp.concatenate([tt_a[:N], tt_b[:N], tt_a[N:], tt_b[N:]], 0))
            return jnp.zeros(TILE, F32), jnp.zeros(TILE, F32), *(row_major(x) for x in parts(tt)), st_a, st_b

        res = lax.while_loop(lambda s: jnp.max(s[0] + s[1]) > 0.5, redo, carry)
        back = lambda x: x.reshape(local_blocks, width, local_rows).transpose(2, 0, 1)
        stack = lambda x: x.reshape(PANELS, width, width)
        return back(res[6]), res[4], stack(res[2]), back(res[7]), res[5], stack(res[3])

    spec_mat = P(("batch", "row"), "col", None)
    spec_out = (spec_mat, P("batch"), P("batch", None, None))
    return jax.shard_map(factor_both, mesh=mesh, in_specs=(spec_mat, spec_mat), out_specs=spec_out + spec_out, check_vma=False)
```

```python
import functools

import jax
import jax.numpy as jnp
from jax import lax
from jax.experimental import pallas as pl
from jax.experimental.pallas import tpu as pltpu
from jax.sharding import PartitionSpec as P

F32 = jnp.float32
BF = jnp.bfloat16
HI = lax.Precision.HIGHEST
PANELS = 4
W = 64
NP = 4
N = 256
NN = (((1,), (0,)), ((), ()))
NT = (((1,), (1,)), ((), ()))
TN = (((0,), (0,)), ((), ()))


BOTH = (0, 1)
total = functools.partial(jnp.sum, keepdims=True)
peak = functools.partial(jnp.max, keepdims=True)
TILE = (8, 128)


def rows_of(shape):
    return lax.broadcasted_iota(jnp.int32, shape, 0)


def lanes_of(shape):
    return lax.broadcasted_iota(jnp.int32, shape, 1)


def hdot(a, b, dn=NN):
    return lax.dot_general(a, b, dn, precision=HI, preferred_element_type=F32)


AMPLIFY = 64.0
HUGE = 1e9


def diag_factor(mats, group):
    tiles = W // 8
    lane8 = lanes_of(TILE)
    sub8 = rows_of(TILE)
    r64 = rows_of((W, W))
    c64 = lanes_of((W, W))
    eye = (r64 == c64).astype(F32)
    full = lambda x: jnp.broadcast_to(x, TILE)
    zeros = jnp.zeros(TILE, F32)
    st = []
    for hpp, ypp in mats:
        he = jnp.concatenate([hpp, eye], 1)
        yw = jnp.concatenate([ypp, eye], 1)
        st.append(dict(he=[he[8 * g:8 * g + 8] for g in range(tiles)], yw=[yw[8 * g:8 * g + 8] for g in range(tiles)],
                       l=[zeros] * tiles, u=[zeros] * tiles, tau=zeros))
    for k0 in range(0, W, group):
        gk = k0 // 8
        for s in st:
            s['bh'] = [[full(s['he'][g][:, k:k + 1]) for g in range(gk, tiles)] for k in range(k0, k0 + group)]
            s['by'] = [[full(s['yw'][g][:, k:k + 1]) for g in range(tiles)] for k in range(k0, k0 + group)]
        for k in range(k0, k0 + group):
            sk = k - 8 * gk
            isk = sub8 == sk
            for s in st:
                ch, cy = s['bh'][k - k0], s['by'][k - k0]
                pick = lambda x: full(x[sk:sk + 1, :])
                h = pick(ch[0])
                a = pick(cy[gk])
                rs = lax.rsqrt(h)
                rinv = jnp.where(a >= 0, -rs, rs)
                ukk = a - h * rinv
                uinv = 1.0 / ukk
                r = pick(s['he'][gk]) * rinv
                u = pick(s['yw'][gk]) - jnp.where((lane8 >= k) & (lane8 < W), r, 0.0)
                un = u * uinv
                rr = r * rinv
                for k2 in range(k + 1, k0 + group):
                    r2 = pick(s['bh'][k2 - k0][0]) * rinv
                    un2 = (pick(s['by'][k2 - k0][gk]) - r2) * uinv
                    rr2 = r2 * rinv
                    s['bh'][k2 - k0] = [x - ch[i] * rr2 for i, x in enumerate(s['bh'][k2 - k0])]
                    nby = [x - cy[i] * un2 for i, x in enumerate(s['by'][k2 - k0])]
                    nby[gk] = jnp.where(isk, un2, nby[gk])
                    s['by'][k2 - k0] = nby
                for g in range(gk, tiles):
                    new = s['he'][g] - ch[g - gk] * rr
                    lc = cy[g] * uinv
                    if g == gk:
                        new = jnp.where(sub8 > sk, new, jnp.where(isk, r, s['he'][g]))
                        lc = jnp.where(sub8 > sk, lc, 0.0)
                    s['he'][g] = new
                    s['l'][g] = jnp.where(lane8 == k, lc, s['l'][g])
                for g in range(tiles):
                    new = s['yw'][g] - cy[g] * un
                    s['yw'][g] = jnp.where(isk, un, new) if g == gk else new
                s['u'][gk] = jnp.where(isk, u, s['u'][gk])
                s['tau'] = jnp.where(lane8 == k, -ukk * rinv, s['tau'])
    out = []
    up = c64 >= r64
    for s in st:
        he = jnp.concatenate(s['he'], 0)
        yw = jnp.concatenate(s['yw'], 0)
        l = jnp.concatenate(s['l'], 0)[:, :W]
        u = jnp.concatenate(s['u'], 0)[:, :W]
        out.append((jnp.where(c64 <= r64, he[:, W:], 0.0), l + eye, jnp.where(up, u, 0.0), yw[:, W:], s['tau'][0:1, :W]))
    return out


def blk(b):
    return slice(b * W, (b + 1) * W)


def order(c):
    return [2 * l + c for l in BOTH] + [2 * l + 1 - c for l in BOTH]


def turn(x):
    return jnp.concatenate([x[:, W:N], x[:, :W], x[:, N:]], 1)


CHAIN_SCRATCH = [(N, 2 * N), (N, 2 * N), (N, N), (NP, 4, W, W), (8, N), (NP, W)]
CHAIN_SHAPES = [(N, N), (N, N), (2 * W, N), (2 * W, N), (N, W), (NP, W), TILE]


def chain_init(col, g, x1, st):
    hs, ys, ls, _, norm, _ = st
    ri, ci = rows_of((N, N)), lanes_of((N, N))
    eye = (ri == ci).astype(F32)
    for c in BOTH:
        @pl.when(col == c)
        def _():
            for i, b in enumerate(order(c)):
                ls[blk(b), :] = x1[blk(i), :]
                for i2, b2 in enumerate(order(c)):
                    hs[blk(b), blk(b2)] = g[blk(i), blk(i2)]
    hs[:, N:] = eye
    ys[:, :N] = ls[...].T
    ys[:, N:] = eye
    dg = jnp.where(ri == ci, hs[:, :N], 0.0)
    norm[...] = jnp.broadcast_to(jnp.sqrt(total(dg, 0)), (8, N))


def chain_cols(p, st, group):
    hs, ys, _, fac, _, tv = st
    e, l, u, w, tau = diag_factor([(hs[0:W, 0:W], ys[0:W, 0:W])], group)[0]
    for i, x in enumerate((e, l, u, w)):
        fac[p, i] = x
    tv[pl.ds(p, 1), :] = tau


def chain_update(p, st):
    hs, ys, ls, fac, _, _ = st
    rw = rows_of((W, 2 * N))
    cw = lanes_of((W, 2 * N))
    rl = rows_of((N - W, W))
    live = N - p * W
    e, l, w = fac[p, 0], fac[p, 1], fac[p, 3]
    rall = hdot(e, hs[0:W, :])
    rall = jnp.where((cw >= N) | ((cw >= rw) & (cw < live)), rall, 0.0)
    wl = hdot(w, l)
    yield
    yc = ys[W:, 0:W]
    nrow = hdot(w, ys[0:W, :] - jnp.where(cw < N, rall, 0.0))
    hnew = hs[W:, :] - hdot(rall[:, W:N], rall, TN)
    hs[0:N - W, :] = turn(hnew)
    hs[N - W:, :] = turn(rall)
    lnew = jnp.where(rl < live - W, hdot(yc, wl), 0.0)
    rest = ls[W:, W:]
    first = ls[0:W, W:]
    ls[0:N - W, N - W:] = lnew
    ls[N - W:, N - W:] = l
    ls[0:N - W, 0:N - W] = rest
    ls[N - W:, 0:N - W] = first
    yield
    ynew = ys[W:, :] - hdot(yc, nrow)
    ys[0:N - W, :] = turn(ynew)
    ys[N - W:, :] = turn(nrow)


def weave(stages, pieces):
    stages = iter(stages)
    for piece in pieces:
        next(stages, None)
        piece()
    for _ in stages:
        pass


def chain_final(col, st, outs):
    hs, ys, ls, fac, norm, tv = st
    rinvt, minv, upt, ptt, tfac, tau, bad = outs
    r64 = rows_of((W, W))
    c64 = lanes_of((W, W))
    tau[...] = tv[...]
    for p in range(NP):
        e, _, u, w = [fac[p, i] for i in range(4)]
        t = -hdot(hdot(u, e, NT), hdot(u, w), NT)
        tfac[blk(p), :] = jnp.where(c64 > r64, t, jnp.where(c64 == r64, jnp.broadcast_to(tv[p:p + 1, :], (W, W)), 0.0))
    ri = rows_of((N, N))
    ci = lanes_of((N, N))
    rt, mi = hs[:, N:], ys[:, N:]
    g = norm[0:1, :]
    c1 = peak(total(jnp.abs(rt) * g, 1))
    c2 = peak(hdot(g, jnp.abs(mi)))
    good = (c1 <= AMPLIFY) & (c2 <= AMPLIFY) & (-peak(-g) >= 1 / HUGE) & (peak(g) <= HUGE)
    bad[...] = jnp.broadcast_to(jnp.where(good, 0.0, 1.0), TILE)
    pt = jnp.where(ri > ci, ls[...], hs[:, :N]).T
    ut = lax.dot_general(ls[...], mi, (((0,), (1,)), ((), ())), precision=HI, preferred_element_type=F32)
    hs[:, :N] = pt
    ys[:, :N] = ut
    for c in BOTH:
        @pl.when(col == c)
        def _():
            for i, b in enumerate(order(c)):
                rinvt[:, blk(i)] = hs[:, N + b * W:N + (b + 1) * W]
                minv[blk(i), :] = ys[blk(b), N:]
            for i in BOTH:
                b = order(c)[i]
                ptt[blk(i), :] = hs[blk(b), :N]
                for i2, b2 in enumerate(order(c)):
                    upt[blk(i), blk(i2)] = ys[blk(b), blk(b2)]


SPLITS = range(3)
loop = functools.partial(lax.fori_loop, 0)


def split3(x):
    h = x.astype(BF)
    r = x - h.astype(F32)
    m = r.astype(BF)
    return h, m, (r - m.astype(F32)).astype(BF)


def dot6(a, b, dn):
    d = lambda i, j: lax.dot_general(a[i], b[j], dn, preferred_element_type=F32)
    return (((d(2, 0) + d(0, 2)) + d(1, 1)) + (d(1, 0) + d(0, 1))) + d(0, 0)


CHUNK = 960
PIECE = 480
HALF = 512
SPAN = 1024
SLOTS = 3
AHEAD = SLOTS - 1


def exchange_kernel(ca, cb, peer_a, peer_b, c1a, c1b, pam, pao, pbm, g_out, x1b, *refs):
    outs, refs = refs[:len(CHAIN_SHAPES)], refs[len(CHAIN_SHAPES):]
    st, refs = refs[:len(CHAIN_SCRATCH)], refs[len(CHAIN_SCRATCH):]
    (x1a, peer, own, xo, xs, cbuf, acc, gacc, r1buf, r2buf, gbuf1, gsum, gbuf2, gfull,
     c_sem, own_sem, out_sem, y_send, y_recv, top_send, top_recv, swap_send, swap_recv,
     g_send, g_recv, p_send, p_recv, x_send, x_recv) = refs
    cts, x1 = (ca, cb), (x1a, x1b)
    row = lax.axis_index("row")
    col = lax.axis_index("col")
    core = lax.rem(row, 2)
    mate = row + 1 - 2 * core
    across = lax.rem(row + 2, 4)
    diag = lax.rem(row + 3 - 2 * core, 4)
    cols, rows = ca.shape
    half = cols // 2
    nown = peer.shape[1]
    nchunk = (cols - nown) // CHUNK
    spans = rows // SPAN
    trips = nchunk * spans

    def remote(src, dst, send, recv, **where):
        return pltpu.make_async_remote_copy(src_ref=src, dst_ref=dst, send_sem=send, recv_sem=recv,
                                            device_id=where, device_id_type=pl.DeviceIdType.MESH)

    to_mate = functools.partial(remote, row=mate)
    to_across = functools.partial(remote, row=across)

    def c_copy(m, t):
        slot = lax.rem(m * trips + t, SLOTS)
        h, j = lax.div(t, nchunk), lax.rem(t, nchunk)
        return pltpu.make_async_copy(
            cts[m].at[pl.ds(pl.multiple_of(nown + j * CHUNK, 64), CHUNK), pl.ds(pl.multiple_of(h * SPAN, SPAN), SPAN)],
            cbuf.at[slot], c_sem.at[slot])

    first = pl.ds(0, nown)
    second = pl.ds(nown, nown)
    lanes = pl.ds(0, N)

    def y_copy(m, h):
        s = pl.ds(pl.multiple_of(h * SPAN, SPAN), SPAN)
        i = m * spans + h
        return remote(cts[m].at[first, s], peer.at[m, :, s], y_send.at[i], y_recv.at[i], col=1 - col)

    def half_slot(u):
        return lax.rem(2 * trips - nchunk + u, SLOTS)

    def c_half(u):
        q, j = lax.div(u, nchunk), lax.rem(u, nchunk)
        return pltpu.make_async_copy(
            cb.at[pl.ds(pl.multiple_of(nown + j * CHUNK, 64), CHUNK), pl.ds(pl.multiple_of(rows - SPAN + q * HALF, HALF), HALF)],
            cbuf.at[half_slot(u), :, pl.ds(0, HALF)], c_sem.at[half_slot(u)])

    def y_half(q):
        s = pl.ds(pl.multiple_of(rows - SPAN + q * HALF, HALF), HALF)
        i = 2 * spans - 1 + q
        return remote(cb.at[first, s], peer.at[1, :, s], y_send.at[i], y_recv.at[i], col=1 - col)

    own_copies = [pltpu.make_async_copy(cts[m].at[first, :], own.at[m], own_sem.at[m]) for m in BOTH]
    for o in own_copies:
        o.start()
    for t in range(AHEAD):
        c_copy(0, t).start()

    barrier = pltpu.get_barrier_semaphore()
    for where in (dict(row=mate), dict(row=across), dict(row=diag), dict(col=1 - col)):
        pl.semaphore_signal(barrier, device_id=where, device_id_type=pl.DeviceIdType.MESH)
    pl.semaphore_wait(barrier, 4)

    ys = [y_copy(m, h) for m in BOTH for h in range(spans - m)] + [y_half(q) for q in BOTH]
    for y in ys:
        y.start()

    tops = (c1a, c1b)
    lows = [pl.ds(0, half), pl.ds(half, half)]
    x_local = [pltpu.make_async_copy(cts[m].at[first, lanes], x1[m].at[first, :], own_sem.at[2 + m]) for m in BOTH]
    x_own = [[remote(cts[m].at[first, lanes], x1[m].at[first, :], top_send.at[m, k], top_recv.at[m], row=k + 1)
              for k in SPLITS] for m in BOTH]
    x_peer = [[remote(peer.at[m, :, lanes], x1[m].at[second, :], top_send.at[2 + m, k], top_recv.at[2 + m], row=k + 1)
               for k in SPLITS] for m in BOTH]
    top_far = [[remote(cts[m].at[:, lanes], tops[m], top_send.at[4 + m, 0], top_recv.at[4 + m], row=1)]
               + [remote(cts[m].at[lows[k], lanes], tops[m].at[lows[k], :], top_send.at[4 + m, 1 + k], top_recv.at[4 + m], row=2 + k)
                  for k in BOTH] for m in BOTH]

    @pl.when(row == 0)
    def _():
        for m in BOTH:
            x_local[m].start()
        for c in x_own[0] + x_own[1] + top_far[0] + top_far[1]:
            c.start()

    mine = pl.ds(pl.multiple_of(core * half, half), half)
    others = pl.ds(pl.multiple_of((1 - core) * half, half), half)
    g_mine = pl.ds(pl.multiple_of(core * nown, nown), nown)
    g_theirs = pl.ds(pl.multiple_of((1 - core) * nown, nown), nown)
    p1 = [to_mate(acc.at[m, others, :], r1buf.at[m], p_send.at[m], p_recv.at[m]) for m in BOTH]
    g1 = [to_mate(gacc.at[m, g_theirs, :], gbuf1.at[m], g_send.at[m], g_recv.at[m]) for m in BOTH]
    g2 = [to_across(gsum.at[m], gbuf2.at[m], g_send.at[2 + m], g_recv.at[2 + m]) for m in BOTH]
    g3 = [to_mate(full.at[g_mine, :], full.at[g_mine, :], g_send.at[4 + m], g_recv.at[4 + m]) for m, full in enumerate((gfull, g_out))]
    p2 = to_across(r1buf.at[0], r2buf, x_send.at[0], x_recv.at[0])
    p3 = to_mate(r1buf.at[0], pao, x_send.at[1], x_recv.at[1])
    swap = [to_mate(tops[m].at[mine, :], tops[m].at[mine, :], swap_send.at[m], swap_recv.at[m]) for m in BOTH]
    peer_out = [pltpu.make_async_copy(peer.at[m], (peer_a, peer_b)[m], out_sem.at[m]) for m in BOTH]
    pam_out = pltpu.make_async_copy(r1buf.at[0], pam, out_sem.at[2])

    def add_half(m):
        p1[m].wait()
        r1buf[m] = r1buf[m] + acc[m, mine, :]

    def finish_g1(m):
        g1[m].wait()
        gsum[m] = gacc[m, g_mine, :] + gbuf1[m]
        g2[m].start()

    def finish_g2(m, full):
        g2[m].wait()
        full[g_mine, :] = gsum[m] + gbuf2[m]
        g3[m].start()

    def send_x(m):
        @pl.when(row == 0)
        def _():
            x1[m][nown:, :] = peer[m, :, 0:N]
            for c in x_peer[m]:
                c.start()

    def wait_x(m):
        @pl.when(row == 0)
        def _():
            x_local[m].wait()

        @pl.when(row > 0)
        def _():
            x_own[m][0].wait_recv()
            x_peer[m][0].wait_recv()

    def begin_chain():
        wait_x(0)
        g3[0].wait()
        chain_init(col, gfull, x1a, st)

    def top_rows():
        @pl.when(row == 1)
        def _():
            for m in BOTH:
                top_far[m][0].wait_recv()

        @pl.when(row >= 2)
        def _():
            for m in BOTH:
                top_far[m][1].wait_recv()
                swap[m].start()

    def last_sums_a():
        p2.wait()
        r1buf[0] = r1buf[0] + r2buf[...]
        p3.start()
        pam_out.start()

    last = trips - nchunk
    begin = 1
    hooks = [[(0, lambda: send_x(0)), (last, lambda: finish_g1(0))],
             [(begin - 1, begin_chain), (begin, lambda: send_x(1)), (last - 1, last_sums_a), (last - 1, top_rows)]]

    def split_own(m):
        def build(q, _):
            s = pl.ds(pl.multiple_of(q * HALF, HALF), HALF)
            for i, part in enumerate(split3(own[m, :, s])):
                xo[m, i, :, s] = part
            acc[m, pl.ds(pl.multiple_of(q * N, N), N), :] = jnp.zeros((N, N), F32)
            return 0

        own_copies[m].wait()
        gacc[m] = jnp.zeros((N, N), F32)
        loop(cols // N, build, 0)

    def panel(m, s0, width):
        return [jnp.concatenate([xo[m, i, :, pl.ds(s0, width)], xs[i, :, 0:width]], 0) for i in SPLITS]

    def head(m, s0, width):
        for q in range(width // HALF):
            d = slice(q * HALF, (q + 1) * HALF)
            for i, part in enumerate(split3(peer[m, :, pl.ds(s0 + q * HALF, HALF)])):
                xs[i, :, d] = part
        x = panel(m, s0, width)
        return dot6(x, x, NT)

    def trip(m, j, slot, s0, width):
        x = panel(m, s0, width)
        for i in range(CHUNK // PIECE):
            r = dot6(split3(cbuf[slot, i * PIECE:(i + 1) * PIECE, 0:width]), x, NT)
            d = pl.ds(pl.multiple_of(nown + j * CHUNK + i * PIECE, 32), PIECE)
            acc[m, d, :] = acc[m, d, :] + r

    def products(m, count):
        def span(h, _):
            y_copy(m, h).wait_recv()
            s0 = pl.multiple_of(h * SPAN, SPAN)
            r = head(m, s0, SPAN)
            gacc[m] = gacc[m] + r

            if m == 0:
                @pl.when(h == spans - 1)
                def _():
                    g1[0].start()

            def step(j, _):
                t = h * nchunk + j
                slot = lax.rem(m * trips + t, SLOTS)
                c_copy(m, t).wait()
                ahead = t + AHEAD - count * nchunk

                @pl.when(ahead < 0)
                def _():
                    c_copy(m, t + AHEAD).start()

                @pl.when(ahead >= 0)
                def _():
                    (c_copy(1, ahead) if m == 0 else c_half(ahead)).start()

                run = functools.partial(trip, m, j, slot, s0, SPAN)
                if m == 0:
                    run()
                else:
                    live = (t >= begin) & (t < begin + NP)

                    @pl.when(live)
                    def _():
                        chain_cols(t - begin, st, 8)
                        run()
                        weave(chain_update(t - begin, st), [])

                    pl.when(~live)(run)
                for at, hook in hooks[m]:
                    pl.when(t == at)(hook)
                return 0

            loop(nchunk, step, 0)
            return 0

        loop(count, span, 0)

    def last_span():
        def span(q, _):
            y_half(q).wait_recv()
            s0 = pl.multiple_of(rows - SPAN + q * HALF, HALF)
            gacc[1] = gacc[1] + head(1, s0, HALF)

            @pl.when(q == 1)
            def _():
                g1[1].start()

            def step(j, _):
                u = q * nchunk + j
                c_half(u).wait()

                @pl.when(u + AHEAD < 2 * nchunk)
                def _():
                    c_half(u + AHEAD).start()

                trip(1, j, half_slot(u), s0, HALF)

                @pl.when(u == nchunk)
                def _():
                    finish_g1(1)

                return 0

            loop(nchunk, step, 0)
            return 0

        loop(2, span, 0)

    for m in BOTH:
        split_own(m)
    products(0, spans)
    p1[0].start()
    peer_out[0].start()
    add_half(0)
    p2.start()
    finish_g2(0, gfull)
    products(1, spans - 1)
    last_span()
    p1[1].start()
    peer_out[1].start()
    wait_x(1)
    chain_final(col, st, outs)
    p1[1].wait()
    pbm[...] = r1buf[1] + acc[1, mine, :]
    finish_g2(1, g_out)
    g3[1].wait()

    @pl.when(row == 0)
    def _():
        for c in x_own[0] + x_own[1] + x_peer[0] + x_peer[1] + top_far[0] + top_far[1]:
            c.wait_send()

    @pl.when(row >= 2)
    def _():
        for m in BOTH:
            swap[m].wait()

    for c in peer_out + [p3, pam_out]:
        c.wait()
    for y in ys:
        y.wait_send()


def exchange(ca, cb, own):
    cols, rows = ca.shape
    half = cols // 2
    hbm = pl.BlockSpec(memory_space=pl.ANY)
    vm = pl.BlockSpec(memory_space=pltpu.VMEM)
    dma = pltpu.SemaphoreType.DMA
    pair = (2, N, N)
    ny = 2 * rows // SPAN + 1
    shapes = [(own, rows)] * 2 + [(cols, N)] * 2 + [(half, N)] * 3 + [(N, N), (N, N)] + CHAIN_SHAPES
    scratch = CHAIN_SCRATCH + [(N, N), (2, own, rows), (2, own, rows)]
    after = [(SLOTS, CHUNK, SPAN), (2, cols, N), pair, (2, half, N), (half, N)] + [(2, own, N)] * 3 + [(N, N)]
    return pl.pallas_call(
        exchange_kernel,
        in_specs=[hbm, hbm],
        out_specs=[hbm] * 6 + [vm] * (3 + len(CHAIN_SHAPES)),
        out_shape=[jax.ShapeDtypeStruct(s, F32) for s in shapes],
        scratch_shapes=[pltpu.VMEM(s, F32) for s in scratch] + [pltpu.VMEM((2, 3, own, rows), BF), pltpu.VMEM((3, own, SPAN), BF)]
        + [pltpu.VMEM(s, F32) for s in after]
        + [dma(n) for n in ((SLOTS,), (4,), (4,), (ny,), (ny,), (6, 3), (6,), (2,), (2,), (6,), (6,), (2,), (2,), (2,), (2,))],
        cost_estimate=pl.CostEstimate(flops=24 * cols * rows * N, bytes_accessed=8 * cols * rows, transcendentals=0),
        compiler_params=pltpu.CompilerParams(vmem_limit_bytes=46 * 2**20, collective_id=0, has_side_effects=True))(ca, cb)


def apply_update(ct, peer, psum, poth, c1, small, before, nxt=None, past=()):
    cols, rows = ct.shape
    nb = 512
    mb = 512
    own = peer.shape[0]
    half = cols // 2
    steps = rows // nb
    rinvt, minv, upt, ptt, _, _, bad = small
    no = len(CHAIN_SHAPES)
    extra = list(nxt or ()) + list(past)
    ne = len(extra)

    def body(c_ref, x_ref, p_ref, q_ref, c1_ref, r_ref, m_ref, up_ref, pt_ref, bad_ref, before_ref, *refs):
        ins, (o_ref, f_ref) = refs[:ne], refs[ne:ne + 2]
        outs, (z_ref, rc_ref, *st) = refs[ne + 2:len(refs) - ns], refs[len(refs) - ns:]
        i = pl.program_id(0)
        row = lax.axis_index("row")
        top = row == 0

        @pl.when(i == 0)
        def _():
            zero = jnp.zeros((1, 1), F32)
            for which, src in enumerate((p_ref, q_ref)):
                base = pl.multiple_of((lax.rem(row, 2) ^ which) * half, half)
                for j in range(half // mb):
                    s = slice(j * mb, (j + 1) * mb)
                    d = pl.ds(base + j * mb, mb)
                    rc = hdot(src[s, :], r_ref[...], NT)
                    z = hdot(jnp.where(top, c_ref[d, 0:N], c1_ref[d, :]) - rc, m_ref[...], NT)
                    rc_ref[d, :] = rc
                    z_ref[d, :] = z
                    zero = zero + total(total(z * 0.0, 0), 1)
            f_ref[...] = jnp.where(zero == 0.0, 0.0, 1.0) + bad_ref[...] + before_ref[...]
            if nxt is not None:
                chain_init(lax.axis_index("col"), *ins[:2], st)
                outs[4][0:N, :] = ins[2][...]
                outs[4][2 * N:2 * N + NP, :] = ins[3][...]

        def piece(j):
            x = jnp.concatenate([c_ref[0:own, :], x_ref[...]], 0)
            lo = own if j == 0 else j * mb
            if j == 0:
                o_ref[0:own, :] = hdot(up_ref[...], x)
            s = slice(lo, (j + 1) * mb)
            o_ref[s, :] = c_ref[s, :] - hdot(z_ref[s, :], x)

        pieces = [functools.partial(piece, j) for j in range(cols // mb)]
        if nxt is None:
            weave([], pieces)
        else:
            @pl.when(lax.rem(i, 2) == 0)
            def _():
                chain_cols(lax.div(i, 2), st, 4)
                weave([], pieces)

            @pl.when(lax.rem(i, 2) == 1)
            def _():
                weave(chain_update(lax.div(i, 2), st), pieces)

            @pl.when(i == steps - 1)
            def _():
                tts = (outs[4].at[pl.ds(N, N), :], outs[4].at[pl.ds(2 * N + NP, NP), :])
                chain_final(lax.axis_index("col"), st, (*outs[:4], *tts, outs[6]))

        @pl.when((i == 0) & top)
        def _():
            o_ref[0:own, 0:N] = pt_ref[...]
            o_ref[own:, 0:N] = rc_ref[own:, :]

    blk2 = pl.BlockSpec((cols, nb), lambda i: (0, i))
    fixed = lambda shape: pl.BlockSpec(shape, lambda i: (0, 0))
    consts = [psum, poth, c1, rinvt, minv, upt, ptt, bad, before] + extra
    more = CHAIN_SHAPES[:4] + [(2 * (N + NP), W)] + CHAIN_SHAPES[5:] if nxt is not None else []
    scratch = [(cols, N), (cols, N)] + (CHAIN_SCRATCH if nxt is not None else [])
    ns = len(scratch)
    return pl.pallas_call(
        body, grid=(steps,),
        in_specs=[blk2, pl.BlockSpec((own, nb), lambda i: (0, i))] + [fixed(a.shape) for a in consts],
        out_specs=[blk2, fixed(TILE)] + [fixed(s) for s in more],
        scratch_shapes=[pltpu.VMEM(s, F32) for s in scratch],
        out_shape=[jax.ShapeDtypeStruct(s, F32) for s in [(cols, rows), TILE] + more],
        cost_estimate=pl.CostEstimate(flops=12 * cols * rows * N, bytes_accessed=8 * cols * rows, transcendentals=0),
        compiler_params=pltpu.CompilerParams(vmem_limit_bytes=40 * 2**20))(ct, peer, *consts)


R1 = [(0, 1), (1, 0), (2, 3), (3, 2)]
R2 = [(0, 2), (2, 0), (1, 3), (3, 1)]
CY = [(0, 1), (1, 0)]


def row_major(x):
    def body(i_ref, o_ref):
        o_ref[...] = i_ref[...]

    return pl.pallas_call(body, out_shape=jax.ShapeDtypeStruct(x.shape, F32))(x)


def pick(x, i, axis=0):
    return lax.dynamic_slice_in_dim(x, i, 1, axis)


def row_sum(x):
    x = x + lax.ppermute(x, "row", R1)
    return x + lax.ppermute(x, "row", R2)


def factor_columns(stored):
    local_rows, local_blocks, width = stored.shape
    row_rank = lax.axis_index("row")
    col_rank = lax.axis_index("col")
    row_ids = row_rank * local_rows + jnp.arange(local_rows)
    col_ids = jnp.arange(width)
    edot = functools.partial(jnp.einsum, precision=HI, preferred_element_type=F32)

    def panel_step(panel_idx, state):
        stored, taus, tfs = state
        row_start = panel_idx * width
        local_idx = panel_idx // 2
        is_owner = col_rank == panel_idx % 2
        panel_in = pick(stored, local_idx, 1)[:, 0, :]

        def column_step(col_idx, loop_state):
            work, tau_vec = loop_state
            diag_idx = row_start + col_idx
            column = pick(work, col_idx, 1)[:, 0]
            below = jnp.where(row_ids >= diag_idx, column, 0.0)
            at_diag = (row_ids == diag_idx).astype(F32)
            summed = row_sum(edot("ar,rk->ak", jnp.stack([below, at_diag]), work))
            cross, diag_row = summed[0], summed[1]
            pivot = pick(diag_row, col_idx)[0]
            norm = jnp.sqrt(pick(cross, col_idx)[0])
            beta = -jnp.where(pivot >= 0, 1.0, -1.0) * norm
            tau = (beta - pivot) / beta
            denom = pivot - beta
            proj = jnp.where(col_ids > col_idx, (cross - beta * diag_row) / denom, 0.0)
            refl = jnp.where(row_ids > diag_idx, column / denom, 0.0) + at_diag
            work = work - tau * refl[:, None] * proj[None, :]
            new_col = jnp.where(row_ids < diag_idx, column, jnp.where(row_ids == diag_idx, beta, refl))
            work = lax.dynamic_update_slice_in_dim(work, new_col[:, None], col_idx, 1)
            return work, lax.dynamic_update_slice_in_dim(tau_vec, tau[None], col_idx, 0)

        work, tau_vec = loop(width, column_step, (panel_in, jnp.zeros((width,), F32)))
        diag_ids = row_start + col_ids[None, :]
        v_block = jnp.where(row_ids[:, None] == diag_ids, 1.0, jnp.where(row_ids[:, None] > diag_ids, work, 0.0))

        gram = row_sum(edot("ri,rj->ij", v_block, v_block))

        def t_step(col_idx, tf):
            g = pick(gram, col_idx, 1)[:, 0]
            g = jnp.where(col_ids < col_idx, g, 0.0)
            tau_k = pick(tau_vec, col_idx)[0]
            t_col = -tau_k * edot("ij,j->i", tf, g)
            t_col = jnp.where(col_ids == col_idx, tau_k, t_col)
            return lax.dynamic_update_slice_in_dim(tf, t_col[:, None], col_idx, 1)

        tf = loop(width, t_step, jnp.zeros((width, width), F32))
        v_mine = jnp.where(is_owner, v_block, 0.0)
        t_mine = jnp.where(is_owner, tf, 0.0)
        v_block = v_mine + lax.ppermute(v_mine, "col", CY)
        tf = t_mine + lax.ppermute(t_mine, "col", CY)

        def block_step(b, stored):
            blk = pick(stored, b, 1)[:, 0, :]
            w = edot("ij,ik->jk", tf, row_sum(edot("ri,rk->ik", v_block, blk)))
            upd = blk - edot("ri,ik->rk", v_block, w)
            keep = b * 2 + col_rank > panel_idx
            mine = (b == local_idx) & is_owner
            new = jnp.where(keep, upd, jnp.where(mine, work, blk))
            return lax.dynamic_update_slice_in_dim(stored, new[:, None, :], b, 1)

        stored = loop(local_blocks, block_step, stored)
        taus = lax.dynamic_update_slice_in_dim(taus, jnp.diagonal(tf), row_start, 0)
        return stored, taus, lax.dynamic_update_slice_in_dim(tfs, tf, row_start, 0)

    return loop(PANELS, panel_step, (stored, jnp.zeros((PANELS * width,), F32), jnp.zeros((PANELS * width, width), F32)))


def solution(mesh):
    def factor_both(a_matrix, b_matrix):
        local_rows, local_blocks, width = a_matrix.shape
        cols = local_blocks * width
        own = 2 * width
        col_rank = lax.axis_index("col")
        cts = [m.transpose(1, 2, 0).reshape(cols, local_rows) for m in (a_matrix, b_matrix)]

        pa, pb, c1a, c1b, pam, pao, pbm, g, x1, *first = exchange(*cts, own)
        c1a, c1b, pb = (pltpu.with_memory_space_constraint(x, pltpu.HBM) for x in (c1a, c1b, pb))
        across = lax.ppermute(pbm, "row", R2)
        out_a, bad_a, *second = apply_update(cts[0], pa, pam, pao, c1a, first, first[6], (g, x1), (first[4], first[5]))
        across, bad_a = lax.optimization_barrier((across, bad_a))
        pbm = pbm + across
        pbo = lax.ppermute(pbm, "row", R1)
        small = lax.ppermute(second[4], "col", CY)
        out_b, bad = apply_update(cts[1], pb, pbm, pbo, c1b, second, bad_a)
        small, bad = lax.optimization_barrier((small, bad))
        tt = jnp.where(col_rank == 0, second[4], small)

        def parts(tt):
            return tt[:N], tt[N:2 * N], *(x.reshape(N) for x in jnp.split(tt[2 * N:], 2))

        carry = (bad, lax.ppermute(bad, "col", CY), *parts(tt), out_a, out_b)

        def redo(state):
            def one(i, done):
                st, taus, tfs = factor_columns(jnp.where(i == 0, a_matrix, b_matrix))
                new = (st.transpose(1, 2, 0).reshape(cols, local_rows), jnp.concatenate([tfs, taus.reshape(PANELS, width)], 0))
                return tuple(jnp.where(i == k, n, d) for k, pair in enumerate((done[:2], done[2:])) for n, d in zip(new, pair))

            blank = jnp.zeros((N + PANELS, width), F32)
            st_a, tt_a, st_b, tt_b = loop(2, one, (state[6], blank, state[7], blank))
            tt = row_major(jnp.concatenate([tt_a[:N], tt_b[:N], tt_a[N:], tt_b[N:]], 0))
            return jnp.zeros(TILE, F32), jnp.zeros(TILE, F32), *(row_major(x) for x in parts(tt)), st_a, st_b

        res = lax.while_loop(lambda s: jnp.max(s[0] + s[1]) > 0.5, redo, carry)
        back = lambda x: x.reshape(local_blocks, width, local_rows).transpose(2, 0, 1)
        stack = lambda x: x.reshape(PANELS, width, width)
        return back(res[6]), res[4], stack(res[2]), back(res[7]), res[5], stack(res[3])

    spec_mat = P(("batch", "row"), "col", None)
    spec_out = (spec_mat, P("batch"), P("batch", None, None))
    return jax.shard_map(factor_both, mesh=mesh, in_specs=(spec_mat, spec_mat), out_specs=spec_out + spec_out, check_vma=False)
```
